8 devices in a mesh: batch: 2 (over z, y), seq: 4 (over x, core).
Axes of the slice: x: 2, y: 2, z: 1, core: 2. Of those that a mesh axis runs over, the one named last changes fastest.
Arguments:
- msa_act: bfloat16 [512, 256, 64], P(('batch', 'seq')), parts along dimension 0
- msa_mask: int32 [512, 256], P(('batch', 'seq')), parts along dimension 0
- pair_act: bfloat16 [512, 256, 128], P(('batch', 'seq')), parts along dimension 0
- w_pair_bias: bfloat16 [128, 8], replicated
- w_row_in: bfloat16 [64, 256], replicated
- b_row_gate: bfloat16 [64], replicated
- w_row_out: bfloat16 [64, 64], replicated
- w_col_in: bfloat16 [64, 144], replicated
- b_col_gate: bfloat16 [64], replicated
- w_col_out: bfloat16 [64, 64], replicated
- w_trans_in: bfloat16 [64, 256], replicated
- w_trans_out: bfloat16 [256, 64], replicated
- w_opm_in: bfloat16 [64, 64], replicated
- w_opm_out: bfloat16 [32, 32, 128], replicated
- b_opm_out: bfloat16 [128], replicated
Outputs:
- output 1: bfloat16 [512, 256, 64], P(('batch', 'seq')), parts along dimension 0
- output 2: bfloat16 [512, 256, 128], P(('batch', 'seq')), parts along dimension 0
There are 2 independent parts. The reference program is written for one: setup_inputs(seed, part) draws one part's arguments, and reference() takes and returns one part's arrays. A program takes and returns all parts, laid end to end along the dimension named above; an argument that names none is the same for every part.
All inputs are finite; a program needn't handle non-finite values.
Results may differ from the reference program's by a relative error of at most 0.0116098.
Values are sent between devices in bfloat16 or wider.
A program may use at most 1 GiB of HBM per device.

```python
import jax
import jax.numpy as jnp
from jax import lax

NUM_SEQ = 256
NUM_RES = 256
MSA_DIM = 64
PAIR_DIM = 128
NUM_HEADS = 8
HEAD_DIM = 8
OPM_DIM = 32


def layer_norm(values):
    as_float = values.astype(jnp.float32)
    centered = as_float - jnp.mean(as_float, axis=-1, keepdims=True)
    variance = jnp.mean(centered * centered, axis=-1, keepdims=True)
    return (centered * lax.rsqrt(variance + 1e-5)).astype(jnp.bfloat16)


def project(values, weight):
    lead_shape = values.shape[:-1]
    flat_rows = values.reshape(-1, values.shape[-1])
    return jnp.dot(flat_rows, weight, preferred_element_type=jnp.float32).reshape(lead_shape + (weight.shape[1],))


def draw_mask(mask_key):
    key_set = jax.random.split(mask_key, 3)
    n_valid = jax.random.randint(key_set[0], (), NUM_SEQ // 2, NUM_SEQ + 1)
    starts = jax.random.randint(key_set[1], (NUM_SEQ, 1), 0, NUM_RES // 4)
    lengths = jax.random.randint(key_set[2], (NUM_SEQ, 1), NUM_RES // 2, NUM_RES + 1)
    residue = jnp.arange(NUM_RES)[None, :]
    seq_index = jnp.arange(NUM_SEQ)[:, None]
    covered = (residue >= starts) & (residue < starts + lengths) & (seq_index < n_valid)
    return (covered | (seq_index == 0)).astype(jnp.int32)


def normal_weight(weight_key, weight_shape, factor):
    return (jax.random.normal(weight_key, weight_shape, jnp.float32) * factor).astype(jnp.bfloat16)


def setup_inputs(seed: int = 0, part: int = 0) -> dict:
    part_key = jax.random.fold_in(jax.random.key(seed), part)
    data_keys = jax.random.split(part_key, 5)
    weight_keys = jax.random.split(jax.random.key(seed + 1), 12)
    head_total = NUM_HEADS * HEAD_DIM
    seq_depth = jnp.linspace(-1.5, 1.5, NUM_SEQ, dtype=jnp.float32)
    base_rows = jax.random.normal(data_keys[0], (NUM_RES, MSA_DIM), jnp.float32)
    direction = jax.random.normal(data_keys[1], (NUM_RES, MSA_DIM), jnp.float32)
    msa_noise = jax.random.normal(data_keys[2], (NUM_SEQ, NUM_RES, MSA_DIM), jnp.float32)
    msa_act = base_rows[None] + seq_depth[:, None, None] * direction[None] + 0.8 * msa_noise
    pair_act = jax.random.normal(data_keys[4], (NUM_RES, NUM_RES, PAIR_DIM), jnp.float32)
    return {
        'msa_act': msa_act.astype(jnp.bfloat16),
        'msa_mask': draw_mask(data_keys[3]),
        'pair_act': pair_act.astype(jnp.bfloat16),
        'w_pair_bias': normal_weight(weight_keys[0], (PAIR_DIM, NUM_HEADS), 1.5 * PAIR_DIM ** -0.5),
        'w_row_in': normal_weight(weight_keys[1], (MSA_DIM, 4 * head_total), MSA_DIM ** -0.5),
        'b_row_gate': normal_weight(weight_keys[2], (head_total,), 1.0),
        'w_row_out': normal_weight(weight_keys[3], (head_total, MSA_DIM), 3.0 * head_total ** -0.5),
        'w_col_in': normal_weight(weight_keys[4], (MSA_DIM, 2 * head_total + 2 * HEAD_DIM), MSA_DIM ** -0.5),
        'b_col_gate': normal_weight(weight_keys[5], (head_total,), 1.0),
        'w_col_out': normal_weight(weight_keys[6], (head_total, MSA_DIM), 2.0 * head_total ** -0.5),
        'w_trans_in': normal_weight(weight_keys[7], (MSA_DIM, 4 * MSA_DIM), MSA_DIM ** -0.5),
        'w_trans_out': normal_weight(weight_keys[8], (4 * MSA_DIM, MSA_DIM), 1.5 * (4 * MSA_DIM) ** -0.5),
        'w_opm_in': normal_weight(weight_keys[9], (MSA_DIM, 2 * OPM_DIM), MSA_DIM ** -0.5),
        'w_opm_out': normal_weight(weight_keys[10], (OPM_DIM, OPM_DIM, PAIR_DIM), 2.0 / OPM_DIM),
        'b_opm_out': normal_weight(weight_keys[11], (PAIR_DIM,), 0.5),
    }


def reference(msa_act, msa_mask, pair_act, w_pair_bias, w_row_in, b_row_gate, w_row_out, w_col_in, b_col_gate, w_col_out, w_trans_in, w_trans_out, w_opm_in, w_opm_out, b_opm_out):
    head_total = NUM_HEADS * HEAD_DIM
    attn_scale = HEAD_DIM ** -0.5
    seq_blk = 4
    row_blk = 16
    keep_mask = msa_mask > 0
    mask_float = msa_mask.astype(jnp.float32)

    pair_bias = project(layer_norm(pair_act), w_pair_bias).astype(jnp.bfloat16)
    bias_heads = jnp.transpose(pair_bias, (2, 0, 1)).astype(jnp.float32)
    row_proj = project(layer_norm(msa_act), w_row_in).astype(jnp.bfloat16)
    row_proj = row_proj.reshape(NUM_SEQ // seq_blk, seq_blk, NUM_RES, 4, NUM_HEADS, HEAD_DIM)
    gate_bias = b_row_gate.astype(jnp.float32).reshape(NUM_HEADS, HEAD_DIM)

    def row_block(block_in):
        proj_blk, keep_blk = block_in
        q_blk = proj_blk[:, :, 0].astype(jnp.float32)
        k_blk = proj_blk[:, :, 1].astype(jnp.float32)
        v_blk = proj_blk[:, :, 2].astype(jnp.float32)
        g_blk = proj_blk[:, :, 3].astype(jnp.float32)
        scores = jnp.einsum('sihd,sjhd->shij', q_blk, k_blk) * attn_scale + bias_heads[None]
        scores = jnp.where(keep_blk[:, None, None, :], scores, -1e9)
        attn_probs = jax.nn.softmax(scores, axis=-1).astype(jnp.bfloat16).astype(jnp.float32)
        attended = jnp.einsum('shij,sjhd->sihd', attn_probs, v_blk)
        return (jax.nn.sigmoid(g_blk + gate_bias) * attended).astype(jnp.bfloat16)

    gated_row = lax.map(row_block, (row_proj, keep_mask.reshape(NUM_SEQ // seq_blk, seq_blk, NUM_RES)))
    gated_row = gated_row.reshape(NUM_SEQ, NUM_RES, head_total)
    msa_one = (msa_act.astype(jnp.float32) + project(gated_row, w_row_out)).astype(jnp.bfloat16)

    col_proj = project(layer_norm(msa_one), w_col_in).astype(jnp.bfloat16)
    q_col = col_proj[:, :, :head_total].reshape(NUM_SEQ, NUM_RES, NUM_HEADS, HEAD_DIM).astype(jnp.float32)
    g_col = col_proj[:, :, head_total:2 * head_total].astype(jnp.float32)
    k_col = col_proj[:, :, 2 * head_total:2 * head_total + HEAD_DIM].astype(jnp.float32)
    v_col = col_proj[:, :, 2 * head_total + HEAD_DIM:].astype(jnp.float32)
    q_sum = jnp.einsum('si,sihd->ihd', mask_float, q_col)
    counts = jnp.sum(mask_float, axis=0)
    q_bar = (q_sum / (counts[:, None, None] + 1e-10)).astype(jnp.bfloat16).astype(jnp.float32)
    logits = jnp.einsum('ihd,sid->sih', q_bar, k_col) * attn_scale
    logits = jnp.where(keep_mask[:, :, None], logits, -1e9)
    col_probs = jax.nn.softmax(logits, axis=0)
    col_out = jnp.einsum('sih,sid->ihd', col_probs, v_col).reshape(NUM_RES, head_total)
    col_gate = jax.nn.sigmoid(g_col + b_col_gate.astype(jnp.float32))
    gated_col = (col_gate * col_out[None]).astype(jnp.bfloat16)
    msa_two = (msa_one.astype(jnp.float32) + project(gated_col, w_col_out)).astype(jnp.bfloat16)

    hidden = jnp.maximum(project(layer_norm(msa_two), w_trans_in), 0.0).astype(jnp.bfloat16)
    msa_three = (msa_two.astype(jnp.float32) + project(hidden, w_trans_out)).astype(jnp.bfloat16)

    opm_proj = (project(layer_norm(msa_three), w_opm_in).astype(jnp.bfloat16) * msa_mask[:, :, None].astype(jnp.bfloat16)).astype(jnp.float32)
    left_vec = opm_proj[:, :, :OPM_DIM]
    right_vec = opm_proj[:, :, OPM_DIM:]
    norm_pair = jnp.dot(mask_float.T, mask_float, preferred_element_type=jnp.float32)
    w_opm_float = w_opm_out.astype(jnp.float32)
    left_blocks = jnp.moveaxis(left_vec.reshape(NUM_SEQ, NUM_RES // row_blk, row_blk, OPM_DIM), 1, 0)
    norm_blocks = norm_pair.reshape(NUM_RES // row_blk, row_blk, NUM_RES)

    def outer_block(block_in):
        left_blk, norm_blk = block_in
        outer_sum = jnp.einsum('sic,sjd->ijcd', left_blk, right_vec)
        mean_outer = outer_sum / (norm_blk[:, :, None, None] + 1e-3)
        return jnp.einsum('ijcd,cde->ije', mean_outer, w_opm_float)

    pair_update = lax.map(outer_block, (left_blocks, norm_blocks)).reshape(NUM_RES, NUM_RES, PAIR_DIM)
    pair_out = (pair_act.astype(jnp.float32) + pair_update + b_opm_out.astype(jnp.float32)).astype(jnp.bfloat16)
    return msa_three, pair_out
```

```python
import functools

import jax
import jax.numpy as jnp
from jax import lax
from jax.experimental import pallas as pl
from jax.experimental.pallas import tpu as pltpu
from jax.sharding import PartitionSpec as P

F32, BF16 = jnp.float32, jnp.bfloat16
MESH = pl.DeviceIdType.MESH
LOG2E = 1.4426950408889634
MASK_FILL = -1e9
R256 = 256
C64 = 64
L128 = 128
H8 = 8
W2K = 2048
T16 = 16
O32 = 32
TWO = 2
FOUR = 4
K144 = 144
ALL16K = 16384
THREE = 3
VMEM_LIMIT = 64000 * 1024


def dot(left, right):
    return jnp.dot(left, right, preferred_element_type=F32)


def dot_t(left, right):
    return lax.dot_general(left, right, (((1,), (1,)), ((), ())), preferred_element_type=F32)


def iota(shape, axis):
    return lax.broadcasted_iota(jnp.int32, shape, axis)


def norm_cols(values):
    centered = values - jnp.mean(values, axis=0, keepdims=True)
    variance = jnp.mean(centered * centered, axis=0, keepdims=True)
    return (centered * lax.rsqrt(variance + 1e-5)).astype(BF16)


def eye(size):
    return (iota((size, size), 0) == iota((size, size), 1)).astype(BF16)


def pick(rows, columns, index):
    return (index(iota((rows, columns), 0)) == iota((rows, columns), 1)).astype(BF16)


def swap8(row):
    return (row % H8) * H8 + row // H8


def column(row_vector, index, size):
    hit = index(iota((size, size), 0)) == iota((size, size), 1)
    wide = jnp.broadcast_to(row_vector.astype(F32), (size, size))
    return jnp.sum(jnp.where(hit, wide, 0.0), axis=1, keepdims=True)


def place():
    me = lax.axis_index('seq')
    batch = lax.axis_index('batch')
    mate = me + 1 - TWO * lax.rem(me, TWO)
    cross = lax.rem(me + TWO, FOUR)
    return me, batch, mate, cross


def meet(batch, peers):
    barrier = pltpu.get_barrier_semaphore()
    for peer in peers:
        pl.semaphore_signal(barrier, inc=1, device_id=(batch, peer), device_id_type=MESH)
    pl.semaphore_wait(barrier, len(peers))


def rows64(index):
    return pl.ds(pl.multiple_of(index * C64, C64), C64)


def row_kernel(e_hbm, z_hbm, mask_ref, wpb_ref, wri_ref, brg_ref, wro_ref, wci_ref,
               e1_ref, g1_ref, kv_ref, qs_ref,
               z_buf, e_buf, tmp, own, full, bias, q_s, k_s, v_s, g_s, x_s, rhs, att, w_big, w_ci,
               z_sem, e_sem, send_sem, recv_sem):
    me, batch, mate, cross = place()
    for part in range(H8):
        pltpu.make_async_copy(z_hbm.at[pl.ds(part * H8, H8)], z_buf.at[pl.ds(part * H8, H8)], z_sem.at[part]).start()
    for part in range(H8):
        pltpu.make_async_copy(e_hbm.at[pl.ds(part * H8, H8)], e_buf.at[pl.ds(part * H8, H8)], e_sem.at[part]).start()
    meet(batch, (mate, cross))

    def big_index(row):
        in_k, in_v = row - C64, row - 192
        head_k = C64 + (in_k // T16) * H8 + in_k % H8
        head_v = jnp.where(in_v % T16 < H8, L128 + (in_v // T16) * H8 + in_v % H8, -1)
        return jnp.where(row < C64, row, jnp.where(row < 192, head_k, jnp.where(row < 320, head_v, row - L128)))

    w_big[...] = dot_t(pick(384, R256, big_index), wri_ref[...]).astype(BF16)
    w_ci[...] = dot_t(
        pick(K144, K144, lambda row: jnp.where(row < C64, swap8(row), jnp.where(row < L128, C64 + swap8(row - C64), row))),
        wci_ref[...]).astype(BF16)
    w_pb = wpb_ref[...]
    rhs[...] = jnp.broadcast_to((iota((K144, R256), 0) == L128).astype(BF16)[None], (H8, K144, R256))

    def bias_part(part, carry):
        pltpu.make_async_copy(z_hbm.at[pl.ds(part * H8, H8)], z_buf.at[pl.ds(part * H8, H8)], z_sem.at[part]).wait()
        z_t = jnp.transpose(z_buf[pl.ds(part * H8, H8)].reshape(W2K, L128).astype(F32))
        heads = dot(w_pb, norm_cols(z_t))
        for t in range(H8):
            for lane in range(TWO):
                at = t * R256 + lane * L128
                tmp[lane, t * H8:(t + 1) * H8, :] = heads[:, at:at + L128]
        for h in range(H8):
            for lane in range(TWO):
                own[h, pl.ds(pl.multiple_of(part * H8, H8), H8), lane * L128:(lane + 1) * L128] = tmp[lane, pl.ds(h, H8, stride=H8), :]
        return carry

    lax.fori_loop(0, H8, bias_part, 0)
    full[:, rows64(me), :] = own[...].astype(BF16)

    def ship(block, slot, peer):
        view = full.at[:, rows64(block), :]
        return pltpu.make_async_remote_copy(
            src_ref=view, dst_ref=view, send_sem=send_sem.at[slot], recv_sem=recv_sem.at[slot],
            device_id=(batch, peer), device_id_type=MESH)

    to_cross, to_mate, relay = ship(me, 0, cross), ship(me, 1, mate), ship(cross, TWO, mate)
    to_cross.start()
    to_mate.start()

    ones = ((iota((L128, W2K), 0) % T16) == H8).astype(F32)

    def project_part(part, carry):
        pltpu.make_async_copy(e_hbm.at[pl.ds(part * H8, H8)], e_buf.at[pl.ds(part * H8, H8)], e_sem.at[part]).wait()
        lanes = pl.ds(pl.multiple_of(part * W2K, W2K), W2K)
        x_raw = jnp.concatenate([e_buf[part * H8 + t] for t in range(H8)], axis=1)
        x_s[:, lanes] = x_raw
        x_t = x_raw.astype(F32)
        proj = dot(w_big[...], norm_cols(x_t))
        q_val = proj[0:C64].astype(BF16).astype(F32) * (H8 ** -0.5 * LOG2E)
        q_hi = q_val.astype(BF16).astype(F32)
        q_lo = q_val - q_hi
        for h in range(H8):
            pair = jnp.concatenate([q_hi[h * H8:h * H8 + H8], q_lo[h * H8:h * H8 + H8]], axis=0)
            q_s[h * T16:(h + 1) * T16, lanes] = pair.astype(BF16)
        keep = mask_ref[pl.ds(pl.multiple_of(part * H8, H8), H8), :].astype(F32)
        keep_row = jnp.concatenate([keep[t:t + 1] for t in range(H8)], axis=1)
        k_s[lanes, 0:L128] = jnp.transpose(proj[C64:192] * keep_row).astype(BF16)
        fill = jnp.where(iota((T16, W2K), 0) == 0, (1.0 - keep_row) * (MASK_FILL * LOG2E), 0.0)
        k_s[lanes, L128:K144] = jnp.transpose(fill).astype(BF16)
        v_s[:, lanes] = (proj[192:320] + ones).astype(BF16)
        g_s[:, lanes] = proj[320:384].astype(BF16)
        return carry

    lax.fori_loop(0, 6, project_part, 0)
    to_cross.wait_recv()
    relay.start()
    lax.fori_loop(6, H8, project_part, 0)
    to_mate.wait_recv()
    relay.wait_recv()
    to_cross.wait_send()
    to_mate.wait_send()
    relay.wait_send()
    for h in range(H8):
        bias[h] = jnp.transpose(full[h].astype(F32)) * LOG2E

    def attend(s, carry):
        lanes = pl.ds(pl.multiple_of(s * R256, R256), R256)
        k_blk = k_s[lanes, :]
        some = jnp.max(mask_ref[pl.ds(s, 1), :].astype(F32), axis=1, keepdims=True) > 0.0
        for h in range(H8):
            sub = slice(h * T16, (h + 1) * T16)
            rhs[h, sub, :] = q_s[sub, lanes]
            logits = dot(k_blk, rhs[h]) + bias[h]
            top = jnp.max(logits, axis=0, keepdims=True)
            probs = jnp.exp2(logits - top).astype(BF16)
            v_blk = v_s[sub, lanes]
            out = dot(v_blk, probs)
            mean = jnp.sum(v_blk.astype(F32)[0:H8], axis=1, keepdims=True) * (1.0 / 256.0)
            att[h * H8:(h + 1) * H8, lanes] = jnp.where(some, out[0:H8] * (1.0 / out[H8:9]), mean)
        return carry

    lax.fori_loop(0, C64, attend, 0)

    w_ro = dot_t(eye(C64), wro_ref[...]).astype(BF16)
    gate_bias = column(brg_ref[...], lambda row: row, C64)
    qs_ref[0:C64, :] = jnp.zeros((C64, R256), F32)
    qs_ref[C64:72, :] = jnp.broadcast_to(jnp.sum(mask_ref[...].astype(F32), axis=0, keepdims=True), (H8, R256))

    def finish_part(part, carry):
        lanes = pl.ds(pl.multiple_of(part * W2K, W2K), W2K)
        gate = jax.nn.sigmoid(g_s[:, lanes].astype(F32) + gate_bias)
        gated = (gate * att[:, lanes]).astype(BF16)
        e_one = (x_s[:, lanes].astype(F32) + dot(w_ro, gated)).astype(BF16)
        e1_ref[:, lanes] = e_one
        proj = dot(w_ci[...], norm_cols(e_one.astype(F32))).astype(BF16)
        g1_ref[:, lanes] = proj[C64:L128]
        keep = mask_ref[pl.ds(pl.multiple_of(part * H8, H8), H8), :].astype(F32)
        q_sum = jnp.zeros((C64, R256), F32)
        for t in range(H8):
            cut = slice(t * R256, (t + 1) * R256)
            kv_ref[part * H8 + t] = proj[L128:K144, cut].astype(F32)
            q_sum += proj[0:C64, cut].astype(F32) * keep[t:t + 1]
        qs_ref[0:C64, :] += q_sum
        return carry

    lax.fori_loop(0, H8, finish_part, 0)


def row_stage(msa, pair, mask, wpb, wri, brg, wro, wci):
    any_spec = pl.BlockSpec(memory_space=pl.ANY)
    vmem = pl.BlockSpec(memory_space=pltpu.VMEM)
    return pl.pallas_call(
        row_kernel,
        name='row_stage',
        out_shape=(
            jax.ShapeDtypeStruct((C64, ALL16K), BF16),
            jax.ShapeDtypeStruct((C64, ALL16K), BF16),
            jax.ShapeDtypeStruct((C64, T16, R256), F32),
            jax.ShapeDtypeStruct((72, R256), F32),
        ),
        in_specs=[any_spec, any_spec] + [vmem] * 6,
        out_specs=(vmem,) * FOUR,
        scratch_shapes=[
            pltpu.VMEM((C64, R256, L128), BF16),
            pltpu.VMEM((C64, C64, R256), BF16),
            pltpu.VMEM((TWO, C64, L128), F32),
            pltpu.VMEM((H8, C64, R256), F32),
            pltpu.VMEM((H8, R256, R256), BF16),
            pltpu.VMEM((H8, R256, R256), F32),
            pltpu.VMEM((L128, ALL16K), BF16),
            pltpu.VMEM((ALL16K, K144), BF16),
            pltpu.VMEM((L128, ALL16K), BF16),
            pltpu.VMEM((C64, ALL16K), BF16),
            pltpu.VMEM((C64, ALL16K), BF16),
            pltpu.VMEM((H8, K144, R256), BF16),
            pltpu.VMEM((C64, ALL16K), F32),
            pltpu.VMEM((384, C64), BF16),
            pltpu.VMEM((K144, C64), BF16),
            pltpu.SemaphoreType.DMA((H8,)),
            pltpu.SemaphoreType.DMA((H8,)),
            pltpu.SemaphoreType.DMA((THREE,)),
            pltpu.SemaphoreType.DMA((THREE,)),
        ],
        compiler_params=pltpu.CompilerParams(collective_id=0, has_side_effects=True, vmem_limit_bytes=VMEM_LIMIT),
    )(msa, pair, mask, wpb, wri, brg, wro, wci)


def column_kernel(qs_ref, kv_ref, mask_ref, out_ref, first, second, stat, logit_s, send_sem, recv_sem):
    me, batch, mate, cross = place()
    peers = [lax.rem(me + step, FOUR) for step in (1, TWO, THREE)]
    meet(batch, peers)

    def share(src, slots, base):
        copies = []
        for n, peer in enumerate(peers):
            copies.append(pltpu.make_async_remote_copy(
                src_ref=src, dst_ref=slots.at[me], send_sem=send_sem.at[base + n], recv_sem=recv_sem.at[base + n],
                device_id=(batch, peer), device_id_type=MESH))
        for copy in copies:
            copy.start()
        return copies

    copies = share(qs_ref, first, 0)
    first[me] = qs_ref[...]
    for copy in copies:
        copy.wait()
    total = first[0] + first[1] + first[TWO] + first[THREE]
    count = total[C64:72] + 1e-10
    q_bar = [(total[d * H8:(d + 1) * H8] / count).astype(BF16).astype(F32) for d in range(H8)]

    def scores(s, top):
        kv = kv_ref[s]
        value = q_bar[0] * kv[0:1]
        for d in range(1, H8):
            value += q_bar[d] * kv[d:d + 1]
        value = jnp.where(mask_ref[pl.ds(s, 1), :] > 0, value * (H8 ** -0.5), MASK_FILL)
        logit_s[s] = value
        return jnp.maximum(top, value)

    top = lax.fori_loop(0, C64, scores, jnp.full((H8, R256), -3e38, F32), unroll=FOUR)

    def gather(s, sums):
        kv = kv_ref[s]
        weight = jnp.exp(logit_s[s] - top)
        return (sums[0] + weight,) + tuple(sums[d + 1] + weight * kv[H8 + d:9 + d] for d in range(H8))

    sums = lax.fori_loop(0, C64, gather, (jnp.zeros((H8, R256), F32),) * 9, unroll=FOUR)
    stat[0:H8, :] = top
    for n in range(9):
        stat[H8 + n * H8:T16 + n * H8, :] = sums[n]
    copies = share(stat, second, THREE)
    second[me] = stat[...]
    for copy in copies:
        copy.wait()
    tops = [second[n, 0:H8, :] for n in range(FOUR)]
    best = jnp.maximum(jnp.maximum(tops[0], tops[1]), jnp.maximum(tops[TWO], tops[THREE]))
    scale = [jnp.exp(value - best) for value in tops]

    def merge(at):
        return sum(second[n, at:at + H8, :] * scale[n] for n in range(FOUR))

    den = merge(H8)
    for d in range(H8):
        out_ref[d * H8:(d + 1) * H8, :] = merge(T16 + d * H8) / den


def column_stage(qs, kv, mask):
    vmem = pl.BlockSpec(memory_space=pltpu.VMEM)
    return pl.pallas_call(
        column_kernel,
        name='column_stage',
        out_shape=jax.ShapeDtypeStruct((C64, R256), F32),
        in_specs=[vmem] * THREE,
        out_specs=vmem,
        scratch_shapes=[
            pltpu.VMEM((FOUR, 72, R256), F32),
            pltpu.VMEM((FOUR, 80, R256), F32),
            pltpu.VMEM((80, R256), F32),
            pltpu.VMEM((C64, H8, R256), F32),
            pltpu.SemaphoreType.DMA((6,)),
            pltpu.SemaphoreType.DMA((6,)),
        ],
        compiler_params=pltpu.CompilerParams(collective_id=1, has_side_effects=True, vmem_limit_bytes=VMEM_LIMIT),
    )(qs, kv, mask)


def transition_kernel(e1_ref, g1_ref, col_ref, mask_ref, bcg_ref, wco_ref, wti_ref, wto_ref, wom_ref,
                      e3_ref, ab_ref, w_co, w_ti, w_to, w_om, ab_s):
    @pl.when(pl.program_id(0) == 0)
    def _():
        w_co[...] = dot(dot_t(eye(C64), wco_ref[...]).astype(BF16),
                        (swap8(iota((C64, C64), 1)) == iota((C64, C64), 0)).astype(BF16)).astype(BF16)
        w_ti[...] = dot_t(eye(R256), wti_ref[...]).astype(BF16)
        w_to[...] = wto_ref[...]
        w_om[...] = dot_t(eye(C64), wom_ref[...]).astype(BF16)

    gate_bias = column(bcg_ref[...], swap8, C64)
    col = jnp.concatenate([col_ref[...]] * H8, axis=1)

    def half(part, carry):
        lanes = pl.ds(pl.multiple_of(part * W2K, W2K), W2K)
        gate = jax.nn.sigmoid(g1_ref[:, lanes].astype(F32) + gate_bias)
        gated = (gate * col).astype(BF16)
        e_two = (e1_ref[:, lanes].astype(F32) + dot(w_co[...], gated)).astype(BF16).astype(F32)
        hidden = jnp.maximum(dot(w_ti[...], norm_cols(e_two)), 0.0).astype(BF16)
        e_three = (e_two + dot(w_to[...], hidden)).astype(BF16).astype(F32)
        for t in range(H8):
            e3_ref[part * H8 + t] = e_three[:, t * R256:(t + 1) * R256].astype(BF16)
        proj = dot(w_om[...], norm_cols(e_three)).astype(BF16).astype(F32)
        keep = mask_ref[pl.ds(pl.multiple_of(part * H8, H8), H8), :].astype(F32)
        for t in range(H8):
            at = pl.ds(pl.multiple_of((part * H8 + t) * C64, C64), C64)
            for lane in range(TWO):
                cut = slice(lane * L128, (lane + 1) * L128)
                ab_s[lane, at, :] = proj[:, t * R256 + lane * L128:t * R256 + (lane + 1) * L128] * keep[t:t + 1, cut]
        return carry

    lax.fori_loop(0, TWO, half, 0)
    for f in range(C64):
        for lane in range(TWO):
            ab_ref[f, :, lane * L128:(lane + 1) * L128] = ab_s[lane, pl.ds(f, T16, stride=C64), :].astype(BF16)


def transition_stage(e1, g1, col, mask, bcg, wco, wti, wto, wom):
    vmem = pl.BlockSpec(memory_space=pltpu.VMEM)
    wide = pl.BlockSpec((C64, 4096), lambda n: (0, n))
    return pl.pallas_call(
        transition_kernel,
        name='transition_stage',
        grid=(FOUR,),
        out_shape=(jax.ShapeDtypeStruct((C64, C64, R256), BF16), jax.ShapeDtypeStruct((C64, C64, R256), BF16)),
        in_specs=[wide, wide, vmem, pl.BlockSpec((T16, R256), lambda n: (n, 0))] + [vmem] * 5,
        out_specs=(pl.BlockSpec((T16, C64, R256), lambda n: (n, 0, 0)), pl.BlockSpec((C64, T16, R256), lambda n: (0, n, 0))),
        scratch_shapes=[
            pltpu.VMEM((C64, C64), BF16),
            pltpu.VMEM((R256, C64), BF16),
            pltpu.VMEM((C64, R256), BF16),
            pltpu.VMEM((C64, C64), BF16),
            pltpu.VMEM((TWO, 1024, L128), F32),
        ],
        compiler_params=pltpu.CompilerParams(dimension_semantics=('arbitrary',), vmem_limit_bytes=VMEM_LIMIT),
    )(e1, g1, col, mask, bcg, wco, wti, wto, wom)


def outer_kernel(ab_ref, mask_ref, z_hbm, w_ref, b_ref, out_ref,
                 z_buf, a_half, b_full, m_full, a_tmp, a_s, acc, p_hi, p_lo, w_tmp, w_t, inv_s,
                 z_sem, send_sem, recv_sem):
    me, batch, mate, cross = place()
    third = lax.rem(mate + TWO, FOUR)
    z_copy = pltpu.make_async_copy(z_hbm, z_buf, z_sem)
    z_copy.start()
    meet(batch, (mate, cross, third))

    def send(src, dst, slot, peer):
        return pltpu.make_async_remote_copy(
            src_ref=src, dst_ref=dst, send_sem=send_sem.at[slot], recv_sem=recv_sem.at[slot],
            device_id=(batch, peer), device_id_type=MESH)

    def lanes_of(device):
        return pl.ds(pl.multiple_of((device // TWO) * L128, L128), L128)

    a_own = ab_ref.at[pl.ds(0, O32), :, :]
    a_dst = a_half.at[:, rows64(me), :]
    a_cross = send(a_own.at[:, :, lanes_of(cross)], a_dst, 0, cross)
    a_mate = send(a_own.at[:, :, lanes_of(me)], a_dst, 1, mate)
    a_relay = send(a_half.at[:, rows64(cross), :], a_half.at[:, rows64(cross), :], TWO, mate)
    b_cross, b_mate, b_relay = [], [], []
    for k in range(FOUR):
        src = ab_ref.at[pl.ds(O32 + k * H8, H8), :, :]
        dst = b_full.at[pl.ds(k * H8, H8), rows64(me), :]
        far = b_full.at[pl.ds(k * H8, H8), rows64(cross), :]
        b_cross.append(send(src, dst, THREE + k, cross))
        b_mate.append(send(src, dst, 7 + k, mate))
        b_relay.append(send(far, far, 11 + k, mate))
    m_full[rows64(me), :] = mask_ref[...].astype(F32).astype(BF16)
    a_cross.start()
    a_mate.start()
    for k in range(FOUR):
        b_cross[k].start()
        b_mate[k].start()
    m_view = m_full.at[rows64(me), :]
    m_copies = [send(m_view, m_view, 15 + n, peer) for n, peer in enumerate((mate, cross, third))]
    for copy in m_copies:
        copy.start()

    a_half[:, rows64(me), :] = ab_ref[pl.ds(0, O32), :, lanes_of(me)]
    b_full[:, rows64(me), :] = ab_ref[pl.ds(O32, O32), :, :]

    w_tmp[...] = w_ref[...].astype(F32)
    for d in range(O32):
        w_t[:, d * O32:(d + 1) * O32] = jnp.transpose(w_tmp[pl.ds(d, O32, stride=O32), :]).astype(BF16)

    a_cross.wait_recv()
    a_relay.start()
    for copy in m_copies:
        copy.wait()
    keep = m_full[...]
    count = dot(jnp.transpose(keep.astype(F32)).astype(BF16), keep)
    inv_s[...] = 1.0 / (count + 1e-3)
    a_mate.wait_recv()
    a_relay.wait_recv()

    def turn(c, carry):
        turned = jnp.transpose(a_half[c].astype(F32))
        for lane in range(TWO):
            a_tmp[lane, pl.ds(pl.multiple_of(c * L128, L128), L128), :] = turned[:, lane * L128:(lane + 1) * L128]
        return carry

    lax.fori_loop(0, O32, turn, 0)
    offset = lax.rem(me, TWO) * C64

    def line_up(i, carry):
        at = pl.ds(pl.multiple_of(i * O32, O32), O32)
        for lane in range(TWO):
            a_s[at, lane * L128:(lane + 1) * L128] = a_tmp[lane, pl.ds(offset + i, O32, stride=L128), :].astype(BF16)
        return carry

    lax.fori_loop(0, C64, line_up, 0)
    b_cross[0].wait_recv()
    b_relay[0].start()
    z_copy.wait()
    e_bias = b_ref[...].astype(F32)

    for k in range(FOUR):
        b_mate[k].wait_recv()
        b_relay[k].wait_recv()
        w_k = w_t[:, k * R256:(k + 1) * R256]

        def block(n, carry):
            a_blk = a_s[pl.ds(pl.multiple_of(n * R256, R256), R256), :]
            for d in range(H8):
                outer = dot(a_blk, b_full[k * H8 + d])
                high = outer.astype(BF16)
                low = (outer - high.astype(F32)).astype(BF16)
                for i in range(H8):
                    p_hi[i, d * O32:(d + 1) * O32, :] = high[i * O32:(i + 1) * O32]
                    p_lo[i, d * O32:(d + 1) * O32, :] = low[i * O32:(i + 1) * O32]
            for i in range(H8):
                at = n * H8 + i
                part = dot(w_k, p_hi[i]) + dot(w_k, p_lo[i])
                if k == 0:
                    acc[at] = part
                elif k < THREE:
                    acc[at] += part
                else:
                    update = (acc[at] + part) * inv_s[pl.ds(me * C64 + at, 1), :]
                    out_ref[at] = (z_buf[at].astype(F32) + jnp.transpose(update) + e_bias).astype(BF16)
            return carry

        lax.fori_loop(0, FOUR, block, 0)
        if k < THREE:
            b_cross[k + 1].wait_recv()
            b_relay[k + 1].start()
        lax.fori_loop(FOUR, H8, block, 0)

    for copy in [a_cross, a_mate, a_relay] + b_cross + b_mate + b_relay:
        copy.wait_send()


def outer_stage(ab, mask, pair, weight, bias):
    any_spec = pl.BlockSpec(memory_space=pl.ANY)
    vmem = pl.BlockSpec(memory_space=pltpu.VMEM)
    return pl.pallas_call(
        outer_kernel,
        name='outer_stage',
        out_shape=jax.ShapeDtypeStruct((C64, R256, L128), BF16),
        in_specs=[vmem, vmem, any_spec, vmem, vmem],
        out_specs=vmem,
        scratch_shapes=[
            pltpu.VMEM((C64, R256, L128), BF16),
            pltpu.VMEM((O32, R256, L128), BF16),
            pltpu.VMEM((O32, R256, R256), BF16),
            pltpu.VMEM((R256, R256), BF16),
            pltpu.VMEM((TWO, 4096, L128), F32),
            pltpu.VMEM((W2K, R256), BF16),
            pltpu.VMEM((C64, L128, R256), F32),
            pltpu.VMEM((H8, R256, R256), BF16),
            pltpu.VMEM((H8, R256, R256), BF16),
            pltpu.VMEM((1024, L128), F32),
            pltpu.VMEM((L128, 1024), BF16),
            pltpu.VMEM((R256, R256), F32),
            pltpu.SemaphoreType.DMA(()),
            pltpu.SemaphoreType.DMA((18,)),
            pltpu.SemaphoreType.DMA((18,)),
        ],
        compiler_params=pltpu.CompilerParams(collective_id=TWO, has_side_effects=True, vmem_limit_bytes=VMEM_LIMIT),
    )(ab, mask, pair, weight, bias)


def solution(mesh):
    row_spec = P(('batch', 'seq'))
    rep_spec = P()

    def local_block(msa, mask, pair, w_pair_bias, w_row_in, b_row_gate, w_row_out, w_col_in, b_col_gate, w_col_out, w_trans_in, w_trans_out, w_opm_in, w_opm_out, b_opm_out):
        e1, g1, kv, qs = row_stage(jnp.swapaxes(msa, 1, TWO), pair, mask, w_pair_bias.T, w_row_in, b_row_gate.reshape(1, C64), w_row_out, w_col_in)
        col = column_stage(qs, kv, mask)
        e3, ab = transition_stage(e1, g1, col, mask, b_col_gate.reshape(1, C64), w_col_out, w_trans_in, w_trans_out.T, w_opm_in)
        pair_out = outer_stage(ab, mask, pair, w_opm_out.reshape(1024, L128), b_opm_out.reshape(1, L128))
        return jnp.swapaxes(e3, 1, TWO), pair_out

    return jax.shard_map(local_block, mesh=mesh, in_specs=(row_spec, row_spec, row_spec) + (rep_spec,) * 12, out_specs=(row_spec, row_spec), check_vma=False)
```

```python
import functools

import jax
import jax.numpy as jnp
from jax import lax
from jax.experimental import pallas as pl
from jax.experimental.pallas import tpu as pltpu
from jax.sharding import PartitionSpec as P

F32, BF16 = jnp.float32, jnp.bfloat16
MESH = pl.DeviceIdType.MESH
LOG2E = 1.4426950408889634
MASK_FILL = -1e9
R256 = 256
C64 = 64
L128 = 128
H8 = 8
W2K = 2048
T16 = 16
O32 = 32
TWO = 2
FOUR = 4
K144 = 144
ALL16K = 16384
THREE = 3
VMEM_LIMIT = 64000 * 1024


def dot(left, right):
    return jnp.dot(left, right, preferred_element_type=F32)


def dot_t(left, right):
    return lax.dot_general(left, right, (((1,), (1,)), ((), ())), preferred_element_type=F32)


def iota(shape, axis):
    return lax.broadcasted_iota(jnp.int32, shape, axis)


def norm_cols(values):
    centered = values - jnp.mean(values, axis=0, keepdims=True)
    variance = jnp.mean(centered * centered, axis=0, keepdims=True)
    return (centered * lax.rsqrt(variance + 1e-5)).astype(BF16)


def eye(size):
    return (iota((size, size), 0) == iota((size, size), 1)).astype(BF16)


def pick(rows, columns, index):
    return (index(iota((rows, columns), 0)) == iota((rows, columns), 1)).astype(BF16)


def swap8(row):
    return (row % H8) * H8 + row // H8


def column(row_vector, index, size):
    hit = index(iota((size, size), 0)) == iota((size, size), 1)
    wide = jnp.broadcast_to(row_vector.astype(F32), (size, size))
    return jnp.sum(jnp.where(hit, wide, 0.0), axis=1, keepdims=True)


def place():
    me = lax.axis_index('seq')
    batch = lax.axis_index('batch')
    mate = me + 1 - TWO * lax.rem(me, TWO)
    cross = lax.rem(me + TWO, FOUR)
    return me, batch, mate, cross


def meet(batch, peers):
    barrier = pltpu.get_barrier_semaphore()
    for peer in peers:
        pl.semaphore_signal(barrier, inc=1, device_id=(batch, peer), device_id_type=MESH)
    pl.semaphore_wait(barrier, len(peers))


def rows64(index):
    return pl.ds(pl.multiple_of(index * C64, C64), C64)


def row_kernel(e_hbm, z_hbm, mask_ref, wpb_ref, wri_ref, brg_ref, wro_ref, wci_ref,
               e1_ref, g1_ref, kv_ref, qs_ref,
               z_buf, e_buf, tmp, own, full, bias, q_s, k_s, v_s, g_s, x_s, rhs, att, w_big, w_ci,
               logit_0, logit_1, top_0, top_1, prob_0, prob_1, z_sem, e_sem, send_sem, recv_sem):
    logit_s, top_s, prob_s = (logit_0, logit_1), (top_0, top_1), (prob_0, prob_1)
    me, batch, mate, cross = place()
    for part in range(H8):
        pltpu.make_async_copy(z_hbm.at[pl.ds(part * H8, H8)], z_buf.at[pl.ds(part * H8, H8)], z_sem.at[part]).start()
    for part in range(H8):
        pltpu.make_async_copy(e_hbm.at[pl.ds(part * H8, H8)], e_buf.at[pl.ds(part * H8, H8)], e_sem.at[part]).start()
    meet(batch, (mate, cross))

    def big_index(row):
        in_k, in_v = row - C64, row - 192
        head_k = C64 + (in_k // T16) * H8 + in_k % H8
        head_v = jnp.where(in_v % T16 < H8, L128 + (in_v // T16) * H8 + in_v % H8, -1)
        return jnp.where(row < C64, row, jnp.where(row < 192, head_k, jnp.where(row < 320, head_v, row - L128)))

    w_big[...] = dot_t(pick(384, R256, big_index), wri_ref[...]).astype(BF16)
    w_ci[...] = dot_t(
        pick(K144, K144, lambda row: jnp.where(row < C64, swap8(row), jnp.where(row < L128, C64 + swap8(row - C64), row))),
        wci_ref[...]).astype(BF16)
    w_pb = wpb_ref[...]
    rhs[...] = jnp.broadcast_to((iota((K144, R256), 0) == L128).astype(BF16)[None], (T16, K144, R256))

    def bias_part(part, carry):
        pltpu.make_async_copy(z_hbm.at[pl.ds(part * H8, H8)], z_buf.at[pl.ds(part * H8, H8)], z_sem.at[part]).wait()
        z_t = jnp.transpose(z_buf[pl.ds(part * H8, H8)].reshape(W2K, L128).astype(F32))
        heads = dot(w_pb, norm_cols(z_t))
        for t in range(H8):
            for lane in range(TWO):
                at = t * R256 + lane * L128
                tmp[lane, t * H8:(t + 1) * H8, :] = heads[:, at:at + L128]
        for h in range(H8):
            for lane in range(TWO):
                own[h, pl.ds(pl.multiple_of(part * H8, H8), H8), lane * L128:(lane + 1) * L128] = tmp[lane, pl.ds(h, H8, stride=H8), :]
        return carry

    lax.fori_loop(0, H8, bias_part, 0)
    full[:, rows64(me), :] = own[...].astype(BF16)

    def ship(block, slot, peer):
        view = full.at[:, rows64(block), :]
        return pltpu.make_async_remote_copy(
            src_ref=view, dst_ref=view, send_sem=send_sem.at[slot], recv_sem=recv_sem.at[slot],
            device_id=(batch, peer), device_id_type=MESH)

    to_cross, to_mate, relay = ship(me, 0, cross), ship(me, 1, mate), ship(cross, TWO, mate)
    to_cross.start()
    to_mate.start()

    ones = ((iota((L128, W2K), 0) % T16) == H8).astype(F32)

    def project_part(part, carry):
        pltpu.make_async_copy(e_hbm.at[pl.ds(part * H8, H8)], e_buf.at[pl.ds(part * H8, H8)], e_sem.at[part]).wait()
        lanes = pl.ds(pl.multiple_of(part * W2K, W2K), W2K)
        x_raw = jnp.concatenate([e_buf[part * H8 + t] for t in range(H8)], axis=1)
        x_s[:, lanes] = x_raw
        x_t = x_raw.astype(F32)
        proj = dot(w_big[...], norm_cols(x_t))
        q_val = proj[0:C64].astype(BF16).astype(F32) * (H8 ** -0.5 * LOG2E)
        q_hi = q_val.astype(BF16).astype(F32)
        q_lo = q_val - q_hi
        for h in range(H8):
            pair = jnp.concatenate([q_hi[h * H8:h * H8 + H8], q_lo[h * H8:h * H8 + H8]], axis=0)
            q_s[h * T16:(h + 1) * T16, lanes] = pair.astype(BF16)
        keep = mask_ref[pl.ds(pl.multiple_of(part * H8, H8), H8), :].astype(F32)
        keep_row = jnp.concatenate([keep[t:t + 1] for t in range(H8)], axis=1)
        k_s[lanes, 0:L128] = jnp.transpose(proj[C64:192] * keep_row).astype(BF16)
        fill = jnp.where(iota((T16, W2K), 0) == 0, (1.0 - keep_row) * (MASK_FILL * LOG2E), 0.0)
        k_s[lanes, L128:K144] = jnp.transpose(fill).astype(BF16)
        v_s[:, lanes] = (proj[192:320] + ones).astype(BF16)
        g_s[:, lanes] = proj[320:384].astype(BF16)
        return carry

    lax.fori_loop(0, 6, project_part, 0)
    to_cross.wait_recv()
    relay.start()
    lax.fori_loop(6, H8, project_part, 0)
    to_mate.wait_recv()
    relay.wait_recv()
    to_cross.wait_send()
    to_mate.wait_send()
    relay.wait_send()
    for h in range(H8):
        bias[h] = jnp.transpose(full[h].astype(F32)) * LOG2E

    def at_seq(s):
        s = jnp.clip(s, 0, 63)
        return s, pl.ds(pl.multiple_of(s * R256, R256), R256)

    def load_q(slot, s):
        lanes = at_seq(s)[1]
        for h in range(H8):
            sub = slice(h * T16, (h + 1) * T16)
            rhs[slot * H8 + h, sub, :] = q_s[sub, lanes]

    def score(slot, s, h):
        lanes = at_seq(s)[1]
        logits = dot(k_s[lanes, :], rhs[slot * H8 + h]) + bias[h]
        logit_s[slot][h] = logits
        tops = jnp.max(logits.reshape(FOUR, H8, H8, R256), axis=1)
        tops = jnp.maximum(jnp.maximum(tops[0], tops[1]), jnp.maximum(tops[TWO], tops[THREE]))
        top_s[slot][h] = jnp.broadcast_to(jnp.max(tops, axis=0, keepdims=True), (H8, R256))

    def soften(slot, h):
        shifted = logit_s[slot][h].reshape(O32, H8, R256) - top_s[slot][h][None]
        prob_s[slot][h] = jnp.exp2(shifted).reshape(R256, R256).astype(BF16)

    def combine(slot, s, h):
        s, lanes = at_seq(s)
        some = jnp.max(mask_ref[pl.ds(s, 1), :].astype(F32), axis=1, keepdims=True) > 0.0
        v_blk = v_s[h * T16:(h + 1) * T16, lanes]
        out = dot(v_blk, prob_s[slot][h])
        mean = jnp.sum(v_blk.astype(F32)[0:H8], axis=1, keepdims=True) * (1.0 / 256.0)
        att[h * H8:(h + 1) * H8, lanes] = jnp.where(some, out[0:H8] * (1.0 / out[H8:9]), mean)

    load_q(0, 0)
    load_q(1, 1)

    def attend(t, carry):
        for half in range(TWO):
            s = TWO * t + half
            for h in range(H8):
                score(half, s, h)
                soften(1 - half, h)
                combine(half, s - TWO, h)
            load_q(half, s + TWO)
        return carry

    lax.fori_loop(0, 33, attend, 0)

    w_ro = dot_t(eye(C64), wro_ref[...]).astype(BF16)
    gate_bias = column(brg_ref[...], lambda row: row, C64)
    qs_ref[0:C64, :] = jnp.zeros((C64, R256), F32)
    qs_ref[C64:72, :] = jnp.broadcast_to(jnp.sum(mask_ref[...].astype(F32), axis=0, keepdims=True), (H8, R256))

    def finish_part(part, carry):
        lanes = pl.ds(pl.multiple_of(part * W2K, W2K), W2K)
        gate = jax.nn.sigmoid(g_s[:, lanes].astype(F32) + gate_bias)
        gated = (gate * att[:, lanes]).astype(BF16)
        e_one = (x_s[:, lanes].astype(F32) + dot(w_ro, gated)).astype(BF16)
        e1_ref[:, lanes] = e_one
        proj = dot(w_ci[...], norm_cols(e_one.astype(F32))).astype(BF16)
        g1_ref[:, lanes] = proj[C64:L128]
        keep = mask_ref[pl.ds(pl.multiple_of(part * H8, H8), H8), :].astype(F32)
        q_sum = jnp.zeros((C64, R256), F32)
        for t in range(H8):
            cut = slice(t * R256, (t + 1) * R256)
            kv_ref[part * H8 + t] = proj[L128:K144, cut].astype(F32)
            q_sum += proj[0:C64, cut].astype(F32) * keep[t:t + 1]
        qs_ref[0:C64, :] += q_sum
        return carry

    lax.fori_loop(0, H8, finish_part, 0)


def row_stage(msa, pair, mask, wpb, wri, brg, wro, wci):
    any_spec = pl.BlockSpec(memory_space=pl.ANY)
    vmem = pl.BlockSpec(memory_space=pltpu.VMEM)
    return pl.pallas_call(
        row_kernel,
        name='row_stage',
        out_shape=(
            jax.ShapeDtypeStruct((C64, ALL16K), BF16),
            jax.ShapeDtypeStruct((C64, ALL16K), BF16),
            jax.ShapeDtypeStruct((C64, T16, R256), F32),
            jax.ShapeDtypeStruct((72, R256), F32),
        ),
        in_specs=[any_spec, any_spec] + [vmem] * 6,
        out_specs=(vmem,) * FOUR,
        scratch_shapes=[
            pltpu.VMEM((C64, R256, L128), BF16),
            pltpu.VMEM((C64, C64, R256), BF16),
            pltpu.VMEM((TWO, C64, L128), F32),
            pltpu.VMEM((H8, C64, R256), F32),
            pltpu.VMEM((H8, R256, R256), BF16),
            pltpu.VMEM((H8, R256, R256), F32),
            pltpu.VMEM((L128, ALL16K), BF16),
            pltpu.VMEM((ALL16K, K144), BF16),
            pltpu.VMEM((L128, ALL16K), BF16),
            pltpu.VMEM((C64, ALL16K), BF16),
            pltpu.VMEM((C64, ALL16K), BF16),
            pltpu.VMEM((T16, K144, R256), BF16),
            pltpu.VMEM((C64, ALL16K), F32),
            pltpu.VMEM((384, C64), BF16),
            pltpu.VMEM((K144, C64), BF16),
            pltpu.VMEM((H8, R256, R256), F32),
            pltpu.VMEM((H8, R256, R256), F32),
            pltpu.VMEM((H8, H8, R256), F32),
            pltpu.VMEM((H8, H8, R256), F32),
            pltpu.VMEM((H8, R256, R256), BF16),
            pltpu.VMEM((H8, R256, R256), BF16),
            pltpu.SemaphoreType.DMA((H8,)),
            pltpu.SemaphoreType.DMA((H8,)),
            pltpu.SemaphoreType.DMA((THREE,)),
            pltpu.SemaphoreType.DMA((THREE,)),
        ],
        compiler_params=pltpu.CompilerParams(collective_id=0, has_side_effects=True, vmem_limit_bytes=VMEM_LIMIT),
    )(msa, pair, mask, wpb, wri, brg, wro, wci)


def column_kernel(qs_ref, kv_ref, mask_ref, out_ref, first, second, stat, logit_s, send_sem, recv_sem):
    me, batch, mate, cross = place()
    peers = [lax.rem(me + step, FOUR) for step in (1, TWO, THREE)]
    meet(batch, peers)

    def share(src, slots, base):
        copies = []
        for n, peer in enumerate(peers):
            copies.append(pltpu.make_async_remote_copy(
                src_ref=src, dst_ref=slots.at[me], send_sem=send_sem.at[base + n], recv_sem=recv_sem.at[base + n],
                device_id=(batch, peer), device_id_type=MESH))
        for copy in copies:
            copy.start()
        return copies

    copies = share(qs_ref, first, 0)
    first[me] = qs_ref[...]
    for copy in copies:
        copy.wait()
    total = first[0] + first[1] + first[TWO] + first[THREE]
    count = total[C64:72] + 1e-10
    q_bar = [(total[d * H8:(d + 1) * H8] / count).astype(BF16).astype(F32) for d in range(H8)]

    def scores(s, top):
        kv = kv_ref[s]
        value = q_bar[0] * kv[0:1]
        for d in range(1, H8):
            value += q_bar[d] * kv[d:d + 1]
        value = jnp.where(mask_ref[pl.ds(s, 1), :] > 0, value * (H8 ** -0.5), MASK_FILL)
        logit_s[s] = value
        return jnp.maximum(top, value)

    top = lax.fori_loop(0, C64, scores, jnp.full((H8, R256), -3e38, F32), unroll=FOUR)

    def gather(s, sums):
        kv = kv_ref[s]
        weight = jnp.exp(logit_s[s] - top)
        return (sums[0] + weight,) + tuple(sums[d + 1] + weight * kv[H8 + d:9 + d] for d in range(H8))

    sums = lax.fori_loop(0, C64, gather, (jnp.zeros((H8, R256), F32),) * 9, unroll=FOUR)
    stat[0:H8, :] = top
    for n in range(9):
        stat[H8 + n * H8:T16 + n * H8, :] = sums[n]
    copies = share(stat, second, THREE)
    second[me] = stat[...]
    for copy in copies:
        copy.wait()
    tops = [second[n, 0:H8, :] for n in range(FOUR)]
    best = jnp.maximum(jnp.maximum(tops[0], tops[1]), jnp.maximum(tops[TWO], tops[THREE]))
    scale = [jnp.exp(value - best) for value in tops]

    def merge(at):
        return sum(second[n, at:at + H8, :] * scale[n] for n in range(FOUR))

    den = merge(H8)
    for d in range(H8):
        out_ref[d * H8:(d + 1) * H8, :] = merge(T16 + d * H8) / den


def column_stage(qs, kv, mask):
    vmem = pl.BlockSpec(memory_space=pltpu.VMEM)
    return pl.pallas_call(
        column_kernel,
        name='column_stage',
        out_shape=jax.ShapeDtypeStruct((C64, R256), F32),
        in_specs=[vmem] * THREE,
        out_specs=vmem,
        scratch_shapes=[
            pltpu.VMEM((FOUR, 72, R256), F32),
            pltpu.VMEM((FOUR, 80, R256), F32),
            pltpu.VMEM((80, R256), F32),
            pltpu.VMEM((C64, H8, R256), F32),
            pltpu.SemaphoreType.DMA((6,)),
            pltpu.SemaphoreType.DMA((6,)),
        ],
        compiler_params=pltpu.CompilerParams(collective_id=1, has_side_effects=True, vmem_limit_bytes=VMEM_LIMIT),
    )(qs, kv, mask)


def transition_kernel(e1_ref, g1_ref, col_ref, mask_ref, bcg_ref, wco_ref, wti_ref, wto_ref, wom_ref,
                      e3_ref, ab_ref, w_co, w_ti, w_to, w_om, ab_s):
    @pl.when(pl.program_id(0) == 0)
    def _():
        w_co[...] = dot(dot_t(eye(C64), wco_ref[...]).astype(BF16),
                        (swap8(iota((C64, C64), 1)) == iota((C64, C64), 0)).astype(BF16)).astype(BF16)
        w_ti[...] = dot_t(eye(R256), wti_ref[...]).astype(BF16)
        w_to[...] = wto_ref[...]
        w_om[...] = dot_t(eye(C64), wom_ref[...]).astype(BF16)

    gate_bias = column(bcg_ref[...], swap8, C64)
    col = jnp.concatenate([col_ref[...]] * H8, axis=1)

    def half(part, carry):
        lanes = pl.ds(pl.multiple_of(part * W2K, W2K), W2K)
        gate = jax.nn.sigmoid(g1_ref[:, lanes].astype(F32) + gate_bias)
        gated = (gate * col).astype(BF16)
        e_two = (e1_ref[:, lanes].astype(F32) + dot(w_co[...], gated)).astype(BF16).astype(F32)
        hidden = jnp.maximum(dot(w_ti[...], norm_cols(e_two)), 0.0).astype(BF16)
        e_three = (e_two + dot(w_to[...], hidden)).astype(BF16).astype(F32)
        for t in range(H8):
            e3_ref[part * H8 + t] = e_three[:, t * R256:(t + 1) * R256].astype(BF16)
        proj = dot(w_om[...], norm_cols(e_three)).astype(BF16).astype(F32)
        keep = mask_ref[pl.ds(pl.multiple_of(part * H8, H8), H8), :].astype(F32)
        for t in range(H8):
            at = pl.ds(pl.multiple_of((part * H8 + t) * C64, C64), C64)
            for lane in range(TWO):
                cut = slice(lane * L128, (lane + 1) * L128)
                ab_s[lane, at, :] = proj[:, t * R256 + lane * L128:t * R256 + (lane + 1) * L128] * keep[t:t + 1, cut]
        return carry

    lax.fori_loop(0, TWO, half, 0)
    for f in range(C64):
        for lane in range(TWO):
            ab_ref[f, :, lane * L128:(lane + 1) * L128] = ab_s[lane, pl.ds(f, T16, stride=C64), :].astype(BF16)


def transition_stage(e1, g1, col, mask, bcg, wco, wti, wto, wom):
    vmem = pl.BlockSpec(memory_space=pltpu.VMEM)
    wide = pl.BlockSpec((C64, 4096), lambda n: (0, n))
    return pl.pallas_call(
        transition_kernel,
        name='transition_stage',
        grid=(FOUR,),
        out_shape=(jax.ShapeDtypeStruct((C64, C64, R256), BF16), jax.ShapeDtypeStruct((C64, C64, R256), BF16)),
        in_specs=[wide, wide, vmem, pl.BlockSpec((T16, R256), lambda n: (n, 0))] + [vmem] * 5,
        out_specs=(pl.BlockSpec((T16, C64, R256), lambda n: (n, 0, 0)), pl.BlockSpec((C64, T16, R256), lambda n: (0, n, 0))),
        scratch_shapes=[
            pltpu.VMEM((C64, C64), BF16),
            pltpu.VMEM((R256, C64), BF16),
            pltpu.VMEM((C64, R256), BF16),
            pltpu.VMEM((C64, C64), BF16),
            pltpu.VMEM((TWO, 1024, L128), F32),
        ],
        compiler_params=pltpu.CompilerParams(dimension_semantics=('arbitrary',), vmem_limit_bytes=VMEM_LIMIT),
    )(e1, g1, col, mask, bcg, wco, wti, wto, wom)


def outer_kernel(ab_ref, mask_ref, z_hbm, w_ref, b_ref, out_ref,
                 z_buf, a_half, b_full, m_full, a_tmp, a_s, acc, p_hi, p_lo, w_tmp, w_t, inv_s,
                 z_sem, send_sem, recv_sem):
    me, batch, mate, cross = place()
    third = lax.rem(mate + TWO, FOUR)
    z_copy = pltpu.make_async_copy(z_hbm, z_buf, z_sem)
    z_copy.start()
    meet(batch, (mate, cross, third))

    def send(src, dst, slot, peer):
        return pltpu.make_async_remote_copy(
            src_ref=src, dst_ref=dst, send_sem=send_sem.at[slot], recv_sem=recv_sem.at[slot],
            device_id=(batch, peer), device_id_type=MESH)

    def lanes_of(device):
        return pl.ds(pl.multiple_of((device // TWO) * L128, L128), L128)

    a_own = ab_ref.at[pl.ds(0, O32), :, :]
    a_dst = a_half.at[:, rows64(me), :]
    a_cross = send(a_own.at[:, :, lanes_of(cross)], a_dst, 0, cross)
    a_mate = send(a_own.at[:, :, lanes_of(me)], a_dst, 1, mate)
    a_relay = send(a_half.at[:, rows64(cross), :], a_half.at[:, rows64(cross), :], TWO, mate)
    b_cross, b_mate, b_relay = [], [], []
    for k in range(FOUR):
        src = ab_ref.at[pl.ds(O32 + k * H8, H8), :, :]
        dst = b_full.at[pl.ds(k * H8, H8), rows64(me), :]
        far = b_full.at[pl.ds(k * H8, H8), rows64(cross), :]
        b_cross.append(send(src, dst, THREE + k, cross))
        b_mate.append(send(src, dst, 7 + k, mate))
        b_relay.append(send(far, far, 11 + k, mate))
    m_full[rows64(me), :] = mask_ref[...].astype(F32).astype(BF16)
    a_cross.start()
    a_mate.start()
    for k in range(FOUR):
        b_cross[k].start()
        b_mate[k].start()
    m_view = m_full.at[rows64(me), :]
    m_copies = [send(m_view, m_view, 15 + n, peer) for n, peer in enumerate((mate, cross, third))]
    for copy in m_copies:
        copy.start()

    a_half[:, rows64(me), :] = ab_ref[pl.ds(0, O32), :, lanes_of(me)]
    b_full[:, rows64(me), :] = ab_ref[pl.ds(O32, O32), :, :]

    w_tmp[...] = w_ref[...].astype(F32)
    for d in range(O32):
        w_t[:, d * O32:(d + 1) * O32] = jnp.transpose(w_tmp[pl.ds(d, O32, stride=O32), :]).astype(BF16)

    a_cross.wait_recv()
    a_relay.start()
    for copy in m_copies:
        copy.wait()
    keep = m_full[...]
    count = dot(jnp.transpose(keep.astype(F32)).astype(BF16), keep)
    inv_s[...] = 1.0 / (count + 1e-3)
    a_mate.wait_recv()
    a_relay.wait_recv()

    def turn(c, carry):
        turned = jnp.transpose(a_half[c].astype(F32))
        for lane in range(TWO):
            a_tmp[lane, pl.ds(pl.multiple_of(c * L128, L128), L128), :] = turned[:, lane * L128:(lane + 1) * L128]
        return carry

    lax.fori_loop(0, O32, turn, 0)
    offset = lax.rem(me, TWO) * C64

    def line_up(i, carry):
        at = pl.ds(pl.multiple_of(i * O32, O32), O32)
        for lane in range(TWO):
            a_s[at, lane * L128:(lane + 1) * L128] = a_tmp[lane, pl.ds(offset + i, O32, stride=L128), :].astype(BF16)
        return carry

    lax.fori_loop(0, C64, line_up, 0)
    b_cross[0].wait_recv()
    b_relay[0].start()
    z_copy.wait()
    e_bias = b_ref[...].astype(F32)

    for k in range(FOUR):
        b_mate[k].wait_recv()
        b_relay[k].wait_recv()
        w_k = w_t[:, k * R256:(k + 1) * R256]

        def block(n, carry):
            a_blk = a_s[pl.ds(pl.multiple_of(n * R256, R256), R256), :]
            for d in range(H8):
                outer = dot(a_blk, b_full[k * H8 + d])
                high = outer.astype(BF16)
                low = (outer - high.astype(F32)).astype(BF16)
                for i in range(H8):
                    p_hi[i, d * O32:(d + 1) * O32, :] = high[i * O32:(i + 1) * O32]
                    p_lo[i, d * O32:(d + 1) * O32, :] = low[i * O32:(i + 1) * O32]
            for i in range(H8):
                at = n * H8 + i
                part = dot(w_k, p_hi[i]) + dot(w_k, p_lo[i])
                if k == 0:
                    acc[at] = part
                elif k < THREE:
                    acc[at] += part
                else:
                    update = (acc[at] + part) * inv_s[pl.ds(me * C64 + at, 1), :]
                    out_ref[at] = (z_buf[at].astype(F32) + jnp.transpose(update) + e_bias).astype(BF16)
            return carry

        lax.fori_loop(0, FOUR, block, 0)
        if k < THREE:
            b_cross[k + 1].wait_recv()
            b_relay[k + 1].start()
        lax.fori_loop(FOUR, H8, block, 0)

    for copy in [a_cross, a_mate, a_relay] + b_cross + b_mate + b_relay:
        copy.wait_send()


def outer_stage(ab, mask, pair, weight, bias):
    any_spec = pl.BlockSpec(memory_space=pl.ANY)
    vmem = pl.BlockSpec(memory_space=pltpu.VMEM)
    return pl.pallas_call(
        outer_kernel,
        name='outer_stage',
        out_shape=jax.ShapeDtypeStruct((C64, R256, L128), BF16),
        in_specs=[vmem, vmem, any_spec, vmem, vmem],
        out_specs=vmem,
        scratch_shapes=[
            pltpu.VMEM((C64, R256, L128), BF16),
            pltpu.VMEM((O32, R256, L128), BF16),
            pltpu.VMEM((O32, R256, R256), BF16),
            pltpu.VMEM((R256, R256), BF16),
            pltpu.VMEM((TWO, 4096, L128), F32),
            pltpu.VMEM((W2K, R256), BF16),
            pltpu.VMEM((C64, L128, R256), F32),
            pltpu.VMEM((H8, R256, R256), BF16),
            pltpu.VMEM((H8, R256, R256), BF16),
            pltpu.VMEM((1024, L128), F32),
            pltpu.VMEM((L128, 1024), BF16),
            pltpu.VMEM((R256, R256), F32),
            pltpu.SemaphoreType.DMA(()),
            pltpu.SemaphoreType.DMA((18,)),
            pltpu.SemaphoreType.DMA((18,)),
        ],
        compiler_params=pltpu.CompilerParams(collective_id=TWO, has_side_effects=True, vmem_limit_bytes=VMEM_LIMIT),
    )(ab, mask, pair, weight, bias)


def solution(mesh):
    row_spec = P(('batch', 'seq'))
    rep_spec = P()

    def local_block(msa, mask, pair, w_pair_bias, w_row_in, b_row_gate, w_row_out, w_col_in, b_col_gate, w_col_out, w_trans_in, w_trans_out, w_opm_in, w_opm_out, b_opm_out):
        e1, g1, kv, qs = row_stage(jnp.swapaxes(msa, 1, TWO), pair, mask, w_pair_bias.T, w_row_in, b_row_gate.reshape(1, C64), w_row_out, w_col_in)
        col = column_stage(qs, kv, mask)
        e3, ab = transition_stage(e1, g1, col, mask, b_col_gate.reshape(1, C64), w_col_out, w_trans_in, w_trans_out.T, w_opm_in)
        pair_out = outer_stage(ab, mask, pair, w_opm_out.reshape(1024, L128), b_opm_out.reshape(1, L128))
        return jnp.swapaxes(e3, 1, TWO), pair_out

    return jax.shard_map(local_block, mesh=mesh, in_specs=(row_spec, row_spec, row_spec) + (rep_spec,) * 12, out_specs=(row_spec, row_spec), check_vma=False)
```

```python
import functools

import jax
import jax.numpy as jnp
from jax import lax
from jax.experimental import pallas as pl
from jax.experimental.pallas import tpu as pltpu
from jax.sharding import PartitionSpec as P

F32, BF16 = jnp.float32, jnp.bfloat16
MESH = pl.DeviceIdType.MESH
LOG2E = 1.4426950408889634
MASK_FILL = -1e9
R256 = 256
C64 = 64
L128 = 128
H8 = 8
W2K = 2048
T16 = 16
O32 = 32
TWO = 2
FOUR = 4
K144 = 144
ALL16K = 16384
THREE = 3
VMEM_LIMIT = 64000 * 1024


def dot(left, right):
    return jnp.dot(left, right, preferred_element_type=F32)


def dot_t(left, right):
    return lax.dot_general(left, right, (((1,), (1,)), ((), ())), preferred_element_type=F32)


def iota(shape, axis):
    return lax.broadcasted_iota(jnp.int32, shape, axis)


def norm_cols(values):
    centered = values - jnp.mean(values, axis=0, keepdims=True)
    variance = jnp.mean(centered * centered, axis=0, keepdims=True)
    return (centered * lax.rsqrt(variance + 1e-5)).astype(BF16)


def eye(size):
    return (iota((size, size), 0) == iota((size, size), 1)).astype(BF16)


def pick(rows, columns, index):
    return (index(iota((rows, columns), 0)) == iota((rows, columns), 1)).astype(BF16)


def swap8(row):
    return (row % H8) * H8 + row // H8


def column(row_vector, index, size):
    hit = index(iota((size, size), 0)) == iota((size, size), 1)
    wide = jnp.broadcast_to(row_vector.astype(F32), (size, size))
    return jnp.sum(jnp.where(hit, wide, 0.0), axis=1, keepdims=True)


def place():
    me = lax.axis_index('seq')
    batch = lax.axis_index('batch')
    mate = me + 1 - TWO * lax.rem(me, TWO)
    cross = lax.rem(me + TWO, FOUR)
    return me, batch, mate, cross


def meet(batch, peers):
    barrier = pltpu.get_barrier_semaphore()
    for peer in peers:
        pl.semaphore_signal(barrier, inc=1, device_id=(batch, peer), device_id_type=MESH)
    pl.semaphore_wait(barrier, len(peers))


def rows64(index):
    return pl.ds(pl.multiple_of(index * C64, C64), C64)


def row_kernel(e_hbm, z_hbm, mask_ref, wpb_ref, wri_ref, brg_ref, wro_ref, wci_ref,
               e1_ref, g1_ref, kv_ref, qs_ref,
               z_buf, e_buf, tmp, own, full, bias, q_s, k_s, v_s, g_s, x_s, rhs, att, w_big, w_ci,
               logit_0, logit_1, top_0, top_1, prob_0, prob_1, z_sem, e_sem, send_sem, recv_sem):
    logit_s, top_s, prob_s = (logit_0, logit_1), (top_0, top_1), (prob_0, prob_1)
    me, batch, mate, cross = place()
    for part in range(H8):
        pltpu.make_async_copy(z_hbm.at[pl.ds(part * H8, H8)], z_buf.at[pl.ds(part * H8, H8)], z_sem.at[part]).start()
    for part in range(H8):
        pltpu.make_async_copy(e_hbm.at[pl.ds(part * H8, H8)], e_buf.at[pl.ds(part * H8, H8)], e_sem.at[part]).start()
    meet(batch, (mate, cross))

    def big_index(row):
        in_k, in_v = row - C64, row - 192
        head_k = C64 + (in_k // T16) * H8 + in_k % H8
        head_v = jnp.where(in_v % T16 < H8, L128 + (in_v // T16) * H8 + in_v % H8, -1)
        return jnp.where(row < C64, row, jnp.where(row < 192, head_k, jnp.where(row < 320, head_v, row - L128)))

    w_big[...] = dot_t(pick(384, R256, big_index), wri_ref[...]).astype(BF16)
    w_ci[...] = dot_t(
        pick(K144, K144, lambda row: jnp.where(row < C64, swap8(row), jnp.where(row < L128, C64 + swap8(row - C64), row))),
        wci_ref[...]).astype(BF16)
    w_pb = wpb_ref[...]
    rhs[...] = jnp.broadcast_to((iota((K144, R256), 0) == L128).astype(BF16)[None], (T16, K144, R256))

    def bias_part(part, carry):
        pltpu.make_async_copy(z_hbm.at[pl.ds(part * H8, H8)], z_buf.at[pl.ds(part * H8, H8)], z_sem.at[part]).wait()
        z_t = jnp.transpose(z_buf[pl.ds(part * H8, H8)].reshape(W2K, L128).astype(F32))
        heads = dot(w_pb, norm_cols(z_t))
        for t in range(H8):
            for lane in range(TWO):
                at = t * R256 + lane * L128
                tmp[lane, t * H8:(t + 1) * H8, :] = heads[:, at:at + L128]
        for h in range(H8):
            for lane in range(TWO):
                own[h, pl.ds(pl.multiple_of(part * H8, H8), H8), lane * L128:(lane + 1) * L128] = tmp[lane, pl.ds(h, H8, stride=H8), :]
        return carry

    lax.fori_loop(0, H8, bias_part, 0)
    full[:, rows64(me), :] = own[...].astype(BF16)

    def ship(block, slot, peer):
        view = full.at[:, rows64(block), :]
        return pltpu.make_async_remote_copy(
            src_ref=view, dst_ref=view, send_sem=send_sem.at[slot], recv_sem=recv_sem.at[slot],
            device_id=(batch, peer), device_id_type=MESH)

    to_cross, to_mate, relay = ship(me, 0, cross), ship(me, 1, mate), ship(cross, TWO, mate)
    to_cross.start()
    to_mate.start()

    ones = ((iota((L128, W2K), 0) % T16) == H8).astype(F32)

    def project_part(part, carry):
        pltpu.make_async_copy(e_hbm.at[pl.ds(part * H8, H8)], e_buf.at[pl.ds(part * H8, H8)], e_sem.at[part]).wait()
        lanes = pl.ds(pl.multiple_of(part * W2K, W2K), W2K)
        x_raw = jnp.concatenate([e_buf[part * H8 + t] for t in range(H8)], axis=1)
        x_s[:, lanes] = x_raw
        x_t = x_raw.astype(F32)
        proj = dot(w_big[...], norm_cols(x_t))
        q_val = proj[0:C64].astype(BF16).astype(F32) * (H8 ** -0.5 * LOG2E)
        q_hi = q_val.astype(BF16).astype(F32)
        q_lo = q_val - q_hi
        for h in range(H8):
            pair = jnp.concatenate([q_hi[h * H8:h * H8 + H8], q_lo[h * H8:h * H8 + H8]], axis=0)
            q_s[h * T16:(h + 1) * T16, lanes] = pair.astype(BF16)
        keep = mask_ref[pl.ds(pl.multiple_of(part * H8, H8), H8), :].astype(F32)
        keep_row = jnp.concatenate([keep[t:t + 1] for t in range(H8)], axis=1)
        k_s[lanes, 0:L128] = jnp.transpose(proj[C64:192] * keep_row).astype(BF16)
        fill = jnp.where(iota((T16, W2K), 0) == 0, (1.0 - keep_row) * (MASK_FILL * LOG2E), 0.0)
        k_s[lanes, L128:K144] = jnp.transpose(fill).astype(BF16)
        v_s[:, lanes] = (proj[192:320] + ones).astype(BF16)
        g_s[:, lanes] = proj[320:384].astype(BF16)
        return carry

    lax.fori_loop(0, 6, project_part, 0)
    to_cross.wait_recv()
    relay.start()
    lax.fori_loop(6, H8, project_part, 0)
    to_mate.wait_recv()
    relay.wait_recv()
    to_cross.wait_send()
    to_mate.wait_send()
    relay.wait_send()
    for h in range(H8):
        bias[h] = jnp.transpose(full[h].astype(F32)) * LOG2E

    def at_seq(s):
        s = jnp.clip(s, 0, 63)
        return s, pl.ds(pl.multiple_of(s * R256, R256), R256)

    def load_q(slot, s):
        lanes = at_seq(s)[1]
        for h in range(H8):
            sub = slice(h * T16, (h + 1) * T16)
            rhs[slot * H8 + h, sub, :] = q_s[sub, lanes]

    def score(slot, s, h):
        lanes = at_seq(s)[1]
        logits = dot(k_s[lanes, :], rhs[slot * H8 + h]) + bias[h]
        logit_s[slot][h] = logits
        tops = jnp.max(logits.reshape(FOUR, H8, H8, R256), axis=1)
        tops = jnp.maximum(jnp.maximum(tops[0], tops[1]), jnp.maximum(tops[TWO], tops[THREE]))
        top_s[slot][h] = jnp.broadcast_to(jnp.max(tops, axis=0, keepdims=True), (H8, R256))

    def soften(slot, h):
        shifted = logit_s[slot][h].reshape(O32, H8, R256) - top_s[slot][h][None]
        prob_s[slot][h] = jnp.exp2(shifted).reshape(R256, R256).astype(BF16)

    def combine(slot, s, h):
        s, lanes = at_seq(s)
        some = jnp.max(mask_ref[pl.ds(s, 1), :].astype(F32), axis=1, keepdims=True) > 0.0
        v_blk = v_s[h * T16:(h + 1) * T16, lanes]
        out = dot(v_blk, prob_s[slot][h])
        mean = jnp.sum(v_blk.astype(F32)[0:H8], axis=1, keepdims=True) * (1.0 / 256.0)
        att[h * H8:(h + 1) * H8, lanes] = jnp.where(some, out[0:H8] * (1.0 / out[H8:9]), mean)

    load_q(0, 0)
    load_q(1, 1)

    def attend(t, carry):
        for half in range(TWO):
            s = TWO * t + half
            for h in range(H8):
                score(half, s, h)
                soften(1 - half, h)
                combine(half, s - TWO, h)
            load_q(half, s + TWO)
        return carry

    lax.fori_loop(0, 33, attend, 0)

    w_ro = dot_t(eye(C64), wro_ref[...]).astype(BF16)
    gate_bias = column(brg_ref[...], lambda row: row, C64)
    qs_ref[0:C64, :] = jnp.zeros((C64, R256), F32)
    qs_ref[C64:72, :] = jnp.broadcast_to(jnp.sum(mask_ref[...].astype(F32), axis=0, keepdims=True), (H8, R256))

    def finish_part(part, carry):
        lanes = pl.ds(pl.multiple_of(part * W2K, W2K), W2K)
        gate = jax.nn.sigmoid(g_s[:, lanes].astype(F32) + gate_bias)
        gated = (gate * att[:, lanes]).astype(BF16)
        e_one = (x_s[:, lanes].astype(F32) + dot(w_ro, gated)).astype(BF16)
        e1_ref[:, lanes] = e_one
        proj = dot(w_ci[...], norm_cols(e_one.astype(F32))).astype(BF16)
        g1_ref[:, lanes] = proj[C64:L128]
        keep = mask_ref[pl.ds(pl.multiple_of(part * H8, H8), H8), :].astype(F32)
        q_sum = jnp.zeros((C64, R256), F32)
        for t in range(H8):
            cut = slice(t * R256, (t + 1) * R256)
            kv_ref[part * H8 + t] = proj[L128:K144, cut].astype(F32)
            q_sum += proj[0:C64, cut].astype(F32) * keep[t:t + 1]
        qs_ref[0:C64, :] += q_sum
        return carry

    lax.fori_loop(0, H8, finish_part, 0)


def row_stage(msa, pair, mask, wpb, wri, brg, wro, wci):
    any_spec = pl.BlockSpec(memory_space=pl.ANY)
    vmem = pl.BlockSpec(memory_space=pltpu.VMEM)
    return pl.pallas_call(
        row_kernel,
        name='row_stage',
        out_shape=(
            jax.ShapeDtypeStruct((C64, ALL16K), BF16),
            jax.ShapeDtypeStruct((C64, ALL16K), BF16),
            jax.ShapeDtypeStruct((C64, T16, R256), F32),
            jax.ShapeDtypeStruct((72, R256), F32),
        ),
        in_specs=[any_spec, any_spec] + [vmem] * 6,
        out_specs=(vmem,) * FOUR,
        scratch_shapes=[
            pltpu.VMEM((C64, R256, L128), BF16),
            pltpu.VMEM((C64, C64, R256), BF16),
            pltpu.VMEM((TWO, C64, L128), F32),
            pltpu.VMEM((H8, C64, R256), F32),
            pltpu.VMEM((H8, R256, R256), BF16),
            pltpu.VMEM((H8, R256, R256), F32),
            pltpu.VMEM((L128, ALL16K), BF16),
            pltpu.VMEM((ALL16K, K144), BF16),
            pltpu.VMEM((L128, ALL16K), BF16),
            pltpu.VMEM((C64, ALL16K), BF16),
            pltpu.VMEM((C64, ALL16K), BF16),
            pltpu.VMEM((T16, K144, R256), BF16),
            pltpu.VMEM((C64, ALL16K), F32),
            pltpu.VMEM((384, C64), BF16),
            pltpu.VMEM((K144, C64), BF16),
            pltpu.VMEM((H8, R256, R256), F32),
            pltpu.VMEM((H8, R256, R256), F32),
            pltpu.VMEM((H8, H8, R256), F32),
            pltpu.VMEM((H8, H8, R256), F32),
            pltpu.VMEM((H8, R256, R256), BF16),
            pltpu.VMEM((H8, R256, R256), BF16),
            pltpu.SemaphoreType.DMA((H8,)),
            pltpu.SemaphoreType.DMA((H8,)),
            pltpu.SemaphoreType.DMA((THREE,)),
            pltpu.SemaphoreType.DMA((THREE,)),
        ],
        compiler_params=pltpu.CompilerParams(collective_id=0, has_side_effects=True, vmem_limit_bytes=VMEM_LIMIT),
    )(msa, pair, mask, wpb, wri, brg, wro, wci)


def tail_kernel(qs_ref, kv_ref, mask_ref, e1_hbm, g1_hbm, z_hbm, bcg_ref, wco_ref, wti_ref, wto_ref, wom_ref, w_ref, b_ref,
                e3_ref, out_ref,
                first, second, stat, logit_s, e_buf, g_buf, z_buf,
                w_co, w_ti, w_to, w_om, ab_s, ab,
                a_half, b_full, m_full, turn_s, a_tmp, a_s, acc, p_hi0, p_lo0, p_hi1, p_lo1, w_tmp, w_t, inv_s,
                load_sem, stat_send, stat_recv, send_sem, recv_sem):
    me, batch, mate, cross = place()
    loads = [pltpu.make_async_copy(src, dst, load_sem.at[n])
             for n, (src, dst) in enumerate(((e1_hbm, e_buf), (g1_hbm, g_buf), (z_hbm, z_buf)))]
    for load in loads:
        load.start()
    peers = [lax.rem(me + step, FOUR) for step in (1, TWO, THREE)]
    meet(batch, peers)

    def share(src, slots, base):
        copies = []
        for n, peer in enumerate(peers):
            copies.append(pltpu.make_async_remote_copy(
                src_ref=src, dst_ref=slots, send_sem=stat_send.at[base + n], recv_sem=stat_recv.at[base + n],
                device_id=(batch, peer), device_id_type=MESH))
        for copy in copies:
            copy.start()
        return copies

    query_copies = share(qs_ref, first.at[me], 0)
    first[me] = qs_ref[...]
    m_full[rows64(me), :] = mask_ref[...].astype(F32).astype(BF16)
    mask_copies = share(m_full.at[rows64(me), :], m_full.at[rows64(me), :], 6)

    w_co[...] = dot(dot_t(eye(C64), wco_ref[...]).astype(BF16),
                    (swap8(iota((C64, C64), 1)) == iota((C64, C64), 0)).astype(BF16)).astype(BF16)
    w_ti[...] = dot_t(eye(R256), wti_ref[...]).astype(BF16)
    w_to[...] = wto_ref[...]
    w_om[...] = dot_t(eye(C64), wom_ref[...]).astype(BF16)
    for c in range(O32):
        w_tmp[c * 40:c * 40 + O32, :] = w_ref[c * O32:(c + 1) * O32, :].astype(F32)
    for k in range(FOUR):
        for d in range(H8):
            w_t[k, :, d * O32:(d + 1) * O32] = jnp.transpose(w_tmp[pl.ds(k * H8 + d, O32, stride=40), :]).astype(BF16)

    for copy in query_copies:
        copy.wait()
    total = first[0] + first[1] + first[TWO] + first[THREE]
    population = total[C64:72] + 1e-10
    q_bar = [(total[d * H8:(d + 1) * H8] / population).astype(BF16).astype(F32) for d in range(H8)]

    def scores(s, top):
        kv = kv_ref[s]
        value = q_bar[0] * kv[0:1]
        for d in range(1, H8):
            value += q_bar[d] * kv[d:d + 1]
        value = jnp.where(mask_ref[pl.ds(s, 1), :] > 0, value * (H8 ** -0.5), MASK_FILL)
        logit_s[s] = value
        return jnp.maximum(top, value)

    top = lax.fori_loop(0, C64, scores, jnp.full((H8, R256), -3e38, F32), unroll=FOUR)

    def gather(s, sums):
        kv = kv_ref[s]
        weight = jnp.exp(logit_s[s] - top)
        return (sums[0] + weight,) + tuple(sums[d + 1] + weight * kv[H8 + d:9 + d] for d in range(H8))

    sums = lax.fori_loop(0, C64, gather, (jnp.zeros((H8, R256), F32),) * 9, unroll=FOUR)
    stat[0:H8, :] = top
    for n in range(9):
        stat[H8 + n * H8:T16 + n * H8, :] = sums[n]
    stat_copies = share(stat, second.at[me], THREE)
    second[me] = stat[...]
    for copy in stat_copies:
        copy.wait()
    tops = [second[n, 0:H8, :] for n in range(FOUR)]
    best = jnp.maximum(jnp.maximum(tops[0], tops[1]), jnp.maximum(tops[TWO], tops[THREE]))
    scale = [jnp.exp(value - best) for value in tops]

    def merge(at):
        return sum(second[n, at:at + H8, :] * scale[n] for n in range(FOUR))

    den = merge(H8)
    column_out = jnp.concatenate([merge(T16 + d * H8) / den for d in range(H8)], axis=0)
    col = jnp.concatenate([column_out] * H8, axis=1)
    gate_bias = column(bcg_ref[...], swap8, C64)

    def send(src, dst, slot, peer):
        return pltpu.make_async_remote_copy(
            src_ref=src, dst_ref=dst, send_sem=send_sem.at[slot], recv_sem=recv_sem.at[slot],
            device_id=(batch, peer), device_id_type=MESH)

    def lanes_of(device):
        return pl.ds(pl.multiple_of((device // TWO) * L128, L128), L128)

    def rows16(device, block):
        return pl.ds(pl.multiple_of(device * C64 + block * T16, T16), T16)

    def b_piece(k, src_rows, dst_rows, slot, peer):
        return send(ab.at[pl.ds(O32 + k * H8, H8), src_rows, :], b_full.at[pl.ds(k * H8, H8), dst_rows, :], slot, peer)

    whole = pl.ds(0, C64)

    def a_cross(n):
        return send(ab.at[pl.ds(0, O32), rows16(0, n), lanes_of(cross)], a_half.at[:, rows16(me, n), :], n, cross)

    def first_cross(n):
        return b_piece(0, rows16(0, n), rows16(me, n), FOUR + n, cross)

    def late_cross(k):
        return b_piece(k, whole, rows64(me), 7 + k, cross)

    def b_mate(k):
        return b_piece(k, whole, rows64(me), 12 + k, mate)

    def b_relay(k):
        far_b = b_full.at[pl.ds(k * H8, H8), rows64(cross), :]
        return send(far_b, far_b, 17 + k, mate)

    a_mate = send(ab.at[pl.ds(0, O32), :, lanes_of(me)], a_half.at[:, rows64(me), :], 11, mate)
    far_a = a_half.at[:, rows64(cross), :]
    a_relay = send(far_a, far_a, T16, mate)

    loads[0].wait()
    loads[1].wait()

    def sixteen(block, done):
        def half(part, carry):
            where = block * TWO + part
            lanes = pl.ds(pl.multiple_of(where * W2K, W2K), W2K)
            gate = jax.nn.sigmoid(g_buf[:, lanes].astype(F32) + gate_bias)
            gated = (gate * col).astype(BF16)
            e_two = (e_buf[:, lanes].astype(F32) + dot(w_co[...], gated)).astype(BF16).astype(F32)
            hidden = jnp.maximum(dot(w_ti[...], norm_cols(e_two)), 0.0).astype(BF16)
            e_three = (e_two + dot(w_to[...], hidden)).astype(BF16).astype(F32)
            for t in range(H8):
                e3_ref[where * H8 + t] = e_three[:, t * R256:(t + 1) * R256].astype(BF16)
            proj = dot(w_om[...], norm_cols(e_three)).astype(BF16).astype(F32)
            keep = mask_ref[pl.ds(pl.multiple_of(where * H8, H8), H8), :].astype(F32)
            for t in range(H8):
                at = pl.ds(pl.multiple_of((part * H8 + t) * 72, H8), C64)
                for lane in range(TWO):
                    cut = slice(lane * L128, (lane + 1) * L128)
                    ab_s[lane, at, :] = proj[:, t * R256 + lane * L128:t * R256 + (lane + 1) * L128] * keep[t:t + 1, cut]
            return carry

        lax.fori_loop(0, TWO, half, 0)
        for f in range(C64):
            for lane in range(TWO):
                ab[f, rows16(0, block), lane * L128:(lane + 1) * L128] = (
                    ab_s[lane, pl.ds(f, T16, stride=72), :].astype(BF16))
        a_cross(block).start()
        first_cross(block).start()
        return done

    lax.fori_loop(0, FOUR, sixteen, 0)
    for k in range(1, FOUR):
        late_cross(k).start()
    a_mate.start()
    for k in range(FOUR):
        b_mate(k).start()

    a_half[:, rows64(me), :] = ab[0:O32, :, lanes_of(me)]
    b_full[:, rows64(me), :] = ab[O32:C64, :, :]
    for copy in mask_copies:
        copy.wait()
    keep_all = m_full[...]
    inv_s[...] = 1.0 / (dot(jnp.transpose(keep_all.astype(F32)).astype(BF16), keep_all) + 1e-3)
    loads[TWO].wait()
    e_bias = b_ref[...].astype(F32)

    for n in range(FOUR):
        a_cross(n).wait_recv()
    a_relay.start()
    for n in range(FOUR):
        first_cross(n).wait_recv()
    b_relay(0).start()
    a_mate.wait_recv()
    a_relay.wait_recv()
    offset = pl.multiple_of(lax.rem(me, TWO) * C64, C64)

    def turn(c, carry):
        turn_s[...] = jnp.transpose(a_half[c].astype(F32))
        mine = turn_s[pl.ds(offset, C64), :]
        for lane in range(TWO):
            a_tmp[lane, pl.ds(pl.multiple_of(c * 72, H8), C64), :] = mine[:, lane * L128:(lane + 1) * L128]
        return carry

    lax.fori_loop(0, O32, turn, 0)
    for i in range(C64):
        for lane in range(TWO):
            a_s[i * O32:(i + 1) * O32, lane * L128:(lane + 1) * L128] = a_tmp[lane, pl.ds(i, O32, stride=72), :].astype(BF16)

    slots = ((p_hi0, p_lo0), (p_hi1, p_lo1))

    def outer(slot, index, d):
        p_hi, p_lo = slots[slot]
        k, n = index // H8, lax.rem(index, H8)
        value = dot(a_s[pl.ds(pl.multiple_of(n * R256, R256), R256), :], b_full[k * H8 + d])
        high = value.astype(BF16)
        low = (value - high.astype(F32)).astype(BF16)
        for i in range(H8):
            p_hi[i, d * O32:(d + 1) * O32, :] = high[i * O32:(i + 1) * O32]
            p_lo[i, d * O32:(d + 1) * O32, :] = low[i * O32:(i + 1) * O32]

    def project(slot, index, i):
        p_hi, p_lo = slots[slot]
        index = jnp.maximum(index, 0)
        k, at = index // H8, lax.rem(index, H8) * H8 + i
        part = dot(w_t[k], p_hi[i]) + dot(w_t[k], p_lo[i])
        acc[at] = jnp.where(k == 0, part, acc[at] + part)

    def settle(index, i):
        at = jnp.maximum(index - 24, 0) * H8 + i
        update = acc[at] * inv_s[pl.ds(me * C64 + at, 1), :]
        out_ref[at] = (z_buf[at].astype(F32) + jnp.transpose(update) + e_bias).astype(BF16)

    def pair(last, t, carry):
        k = t // FOUR

        @pl.when(lax.rem(t, FOUR) == 0)
        def _():
            b_mate(k).wait_recv()
            b_relay(k).wait_recv()

        if not last:
            @pl.when(lax.rem(t, FOUR) == TWO)
            def _():
                late_cross(k + 1).wait_recv()
                b_relay(k + 1).start()

        for slot in range(TWO):
            index = TWO * t + slot
            for n in range(H8):
                outer(slot, index, n)
                project(1 - slot, index - 1, n)
                if last:
                    settle(index - TWO, n)
        return carry

    lax.fori_loop(0, 12, functools.partial(pair, False), 0)
    lax.fori_loop(12, T16, functools.partial(pair, True), 0)
    for n in range(H8):
        project(1, 31, n)
        settle(30, n)
    for n in range(H8):
        settle(31, n)
    a_mate.wait_send()
    a_relay.wait_send()
    for n in range(FOUR):
        a_cross(n).wait_send()
        first_cross(n).wait_send()
        b_mate(n).wait_send()
        b_relay(n).wait_send()
    for k in range(1, FOUR):
        late_cross(k).wait_send()


def tail_stage(qs, kv, mask, e1, g1, pair, bcg, wco, wti, wto, wom, weight, bias):
    any_spec = pl.BlockSpec(memory_space=pl.ANY)
    vmem = pl.BlockSpec(memory_space=pltpu.VMEM)
    return pl.pallas_call(
        tail_kernel,
        name='tail_stage',
        out_shape=(jax.ShapeDtypeStruct((C64, C64, R256), BF16), jax.ShapeDtypeStruct((C64, R256, L128), BF16)),
        in_specs=[vmem] * THREE + [any_spec] * THREE + [vmem] * 7,
        out_specs=(vmem, vmem),
        scratch_shapes=[
            pltpu.VMEM((FOUR, 72, R256), F32),
            pltpu.VMEM((FOUR, 80, R256), F32),
            pltpu.VMEM((80, R256), F32),
            pltpu.VMEM((C64, H8, R256), F32),
            pltpu.VMEM((C64, ALL16K), BF16),
            pltpu.VMEM((C64, ALL16K), BF16),
            pltpu.VMEM((C64, R256, L128), BF16),
            pltpu.VMEM((C64, C64), BF16),
            pltpu.VMEM((R256, C64), BF16),
            pltpu.VMEM((C64, R256), BF16),
            pltpu.VMEM((C64, C64), BF16),
            pltpu.VMEM((TWO, 1152, L128), F32),
            pltpu.VMEM((C64, C64, R256), BF16),
            pltpu.VMEM((O32, R256, L128), BF16),
            pltpu.VMEM((O32, R256, R256), BF16),
            pltpu.VMEM((R256, R256), BF16),
            pltpu.VMEM((L128, R256), F32),
            pltpu.VMEM((TWO, 2304, L128), F32),
            pltpu.VMEM((W2K, R256), BF16),
            pltpu.VMEM((C64, L128, R256), F32),
        ] + [pltpu.VMEM((H8, R256, R256), BF16)] * FOUR + [
            pltpu.VMEM((1280, L128), F32),
            pltpu.VMEM((FOUR, L128, R256), BF16),
            pltpu.VMEM((R256, R256), F32),
            pltpu.SemaphoreType.DMA((THREE,)),
            pltpu.SemaphoreType.DMA((9,)),
            pltpu.SemaphoreType.DMA((9,)),
            pltpu.SemaphoreType.DMA((21,)),
            pltpu.SemaphoreType.DMA((21,)),
        ],
        compiler_params=pltpu.CompilerParams(collective_id=1, has_side_effects=True, vmem_limit_bytes=VMEM_LIMIT),
    )(qs, kv, mask, e1, g1, pair, bcg, wco, wti, wto, wom, weight, bias)


def solution(mesh):
    row_spec = P(('batch', 'seq'))
    rep_spec = P()

    def local_block(msa, mask, pair, w_pair_bias, w_row_in, b_row_gate, w_row_out, w_col_in, b_col_gate, w_col_out, w_trans_in, w_trans_out, w_opm_in, w_opm_out, b_opm_out):
        e1, g1, kv, qs = row_stage(jnp.swapaxes(msa, 1, TWO), pair, mask, w_pair_bias.T, w_row_in, b_row_gate.reshape(1, C64), w_row_out, w_col_in)
        e3, pair_out = tail_stage(qs, kv, mask, e1, g1, pair, b_col_gate.reshape(1, C64), w_col_out, w_trans_in, w_trans_out.T, w_opm_in, w_opm_out.reshape(1024, L128), b_opm_out.reshape(1, L128))
        return jnp.swapaxes(e3, 1, TWO), pair_out

    return jax.shard_map(local_block, mesh=mesh, in_specs=(row_spec, row_spec, row_spec) + (rep_spec,) * 12, out_specs=(row_spec, row_spec), check_vma=False)
```

```python
import functools

import jax
import jax.numpy as jnp
from jax import lax
from jax.experimental import pallas as pl
from jax.experimental.pallas import tpu as pltpu
from jax.sharding import PartitionSpec as P

F32, BF16 = jnp.float32, jnp.bfloat16
MESH = pl.DeviceIdType.MESH
LOG2E = 1.4426950408889634
MASK_FILL = -1e9
R256 = 256
C64 = 64
L128 = 128
H8 = 8
W2K = 2048
T16 = 16
O32 = 32
TWO = 2
FOUR = 4
K144 = 144
ALL16K = 16384
THREE = 3
VMEM_LIMIT = 46000 * 1024
TAIL_LIMIT = 40000 * 1024


def dot(left, right):
    return jnp.dot(left, right, preferred_element_type=F32)


def dot_t(left, right):
    return lax.dot_general(left, right, (((1,), (1,)), ((), ())), preferred_element_type=F32)


def iota(shape, axis):
    return lax.broadcasted_iota(jnp.int32, shape, axis)


def norm_cols(values):
    centered = values - jnp.mean(values, axis=0, keepdims=True)
    variance = jnp.mean(centered * centered, axis=0, keepdims=True)
    return (centered * lax.rsqrt(variance + 1e-5)).astype(BF16)


def eye(size):
    return (iota((size, size), 0) == iota((size, size), 1)).astype(BF16)


def pick(rows, columns, index):
    return (index(iota((rows, columns), 0)) == iota((rows, columns), 1)).astype(BF16)


def swap8(row):
    return (row % H8) * H8 + row // H8


def column(row_vector, index, size):
    hit = index(iota((size, size), 0)) == iota((size, size), 1)
    wide = jnp.broadcast_to(row_vector.astype(F32), (size, size))
    return jnp.sum(jnp.where(hit, wide, 0.0), axis=1, keepdims=True)


def place():
    me = lax.axis_index('seq')
    batch = lax.axis_index('batch')
    mate = me + 1 - TWO * lax.rem(me, TWO)
    cross = lax.rem(me + TWO, FOUR)
    return me, batch, mate, cross


def meet(batch, peers):
    barrier = pltpu.get_barrier_semaphore()
    for peer in peers:
        pl.semaphore_signal(barrier, inc=1, device_id=(batch, peer), device_id_type=MESH)
    pl.semaphore_wait(barrier, len(peers))


def rows64(index):
    return pl.ds(pl.multiple_of(index * C64, C64), C64)


def row_kernel(e_hbm, z_hbm, mask_ref, wpb_ref, wri_ref, brg_ref, wro_ref, wci_ref,
               e1_ref, g1_ref, kv_ref, qs_ref,
               z_buf, e_buf, tmp, own, full, bias, q_s, k_s, v_s, g_s, x_s, rhs, att, w_big, w_ci,
               logit_0, logit_1, top_0, top_1, out_0, out_1, z_sem, e_sem, send_sem, recv_sem):
    logit_s, top_s, out_s = (logit_0, logit_1), (top_0, top_1), (out_0, out_1)
    me, batch, mate, cross = place()
    for part in range(H8):
        pltpu.make_async_copy(z_hbm.at[pl.ds(part * H8, H8)], z_buf.at[pl.ds(part * H8, H8)], z_sem.at[part]).start()
    for part in range(H8):
        pltpu.make_async_copy(e_hbm.at[pl.ds(part * H8, H8)], e_buf.at[pl.ds(part * H8, H8)], e_sem.at[part]).start()
    meet(batch, (mate, cross))

    def big_index(row):
        in_k, in_v = row - C64, row - 192
        head_k = C64 + (in_k // T16) * H8 + in_k % H8
        head_v = jnp.where(in_v % T16 < H8, L128 + (in_v // T16) * H8 + in_v % H8, -1)
        return jnp.where(row < C64, row, jnp.where(row < 192, head_k, jnp.where(row < 320, head_v, row - L128)))

    w_big[...] = dot_t(pick(384, R256, big_index), wri_ref[...]).astype(BF16)
    w_ci[...] = dot_t(
        pick(K144, K144, lambda row: jnp.where(row < C64, swap8(row), jnp.where(row < L128, C64 + swap8(row - C64), row))),
        wci_ref[...]).astype(BF16)
    w_pb = wpb_ref[...]
    rhs[...] = jnp.broadcast_to((iota((K144, R256), 0) == L128).astype(BF16)[None], (T16, K144, R256))

    def bias_part(part, carry):
        pltpu.make_async_copy(z_hbm.at[pl.ds(part * H8, H8)], z_buf.at[pl.ds(part * H8, H8)], z_sem.at[part]).wait()
        z_t = jnp.transpose(z_buf[pl.ds(part * H8, H8)].reshape(W2K, L128).astype(F32))
        heads = dot(w_pb, norm_cols(z_t))
        for t in range(H8):
            for lane in range(TWO):
                at = t * R256 + lane * L128
                tmp[lane, t * H8:(t + 1) * H8, :] = heads[:, at:at + L128]
        for h in range(H8):
            for lane in range(TWO):
                own[h, pl.ds(pl.multiple_of(part * H8, H8), H8), lane * L128:(lane + 1) * L128] = tmp[lane, pl.ds(h, H8, stride=H8), :]
        return carry

    lax.fori_loop(0, H8, bias_part, 0)
    full[:, rows64(me), :] = own[...].astype(BF16)

    def ship(block, slot, peer):
        view = full.at[:, rows64(block), :]
        return pltpu.make_async_remote_copy(
            src_ref=view, dst_ref=view, send_sem=send_sem.at[slot], recv_sem=recv_sem.at[slot],
            device_id=(batch, peer), device_id_type=MESH)

    to_cross, to_mate, relay = ship(me, 0, cross), ship(me, 1, mate), ship(cross, TWO, mate)
    to_cross.start()
    to_mate.start()

    ones = ((iota((L128, W2K), 0) % T16) == H8).astype(F32)

    def project_part(part, carry):
        pltpu.make_async_copy(e_hbm.at[pl.ds(part * H8, H8)], e_buf.at[pl.ds(part * H8, H8)], e_sem.at[part]).wait()
        lanes = pl.ds(pl.multiple_of(part * W2K, W2K), W2K)
        x_raw = jnp.concatenate([e_buf[part * H8 + t] for t in range(H8)], axis=1)
        x_s[:, lanes] = x_raw
        x_t = x_raw.astype(F32)
        proj = dot(w_big[...], norm_cols(x_t))
        q_val = proj[0:C64].astype(BF16).astype(F32) * (H8 ** -0.5 * LOG2E)
        q_hi = q_val.astype(BF16).astype(F32)
        q_lo = q_val - q_hi
        for h in range(H8):
            pair = jnp.concatenate([q_hi[h * H8:h * H8 + H8], q_lo[h * H8:h * H8 + H8]], axis=0)
            q_s[h * T16:(h + 1) * T16, lanes] = pair.astype(BF16)
        keep = mask_ref[pl.ds(pl.multiple_of(part * H8, H8), H8), :].astype(F32)
        keep_row = jnp.concatenate([keep[t:t + 1] for t in range(H8)], axis=1)
        k_s[lanes, 0:L128] = jnp.transpose(proj[C64:192] * keep_row).astype(BF16)
        fill = jnp.where(iota((T16, W2K), 0) == 0, (1.0 - keep_row) * (MASK_FILL * LOG2E), 0.0)
        k_s[lanes, L128:K144] = jnp.transpose(fill).astype(BF16)
        v_s[:, lanes] = (proj[192:320] + ones).astype(BF16)
        g_s[:, lanes] = proj[320:384].astype(BF16)
        return carry

    lax.fori_loop(0, 6, project_part, 0)
    to_cross.wait_recv()
    relay.start()
    lax.fori_loop(6, H8, project_part, 0)
    to_mate.wait_recv()
    relay.wait_recv()
    to_cross.wait_send()
    to_mate.wait_send()
    relay.wait_send()
    for h in range(H8):
        bias[h] = jnp.transpose(full[h].astype(F32)) * LOG2E

    def at_seq(s):
        s = jnp.clip(s, 0, 63)
        return s, pl.ds(pl.multiple_of(s * R256, R256), R256)

    def load_q(slot, s):
        lanes = at_seq(s)[1]
        for h in range(H8):
            sub = slice(h * T16, (h + 1) * T16)
            rhs[slot * H8 + h, sub, :] = q_s[sub, lanes]

    def score(slot, s, h):
        lanes = at_seq(s)[1]
        logits = dot(k_s[lanes, :], rhs[slot * H8 + h]) + bias[h]
        logit_s[slot][h] = logits
        tops = jnp.max(logits.reshape(FOUR, H8, H8, R256), axis=1)
        tops = jnp.maximum(jnp.maximum(tops[0], tops[1]), jnp.maximum(tops[TWO], tops[THREE]))
        top_s[slot][h] = jnp.broadcast_to(jnp.max(tops, axis=0, keepdims=True), (H8, R256))

    def soften(slot, s, h):
        lanes = at_seq(s)[1]
        shifted = logit_s[slot][h].reshape(O32, H8, R256) - top_s[slot][h][None]
        probs = jnp.exp2(shifted).reshape(R256, R256).astype(BF16)
        out_s[slot][h] = dot(v_s[h * T16:(h + 1) * T16, lanes], probs)

    def combine(slot, s, h):
        s, lanes = at_seq(s)
        some = jnp.max(mask_ref[pl.ds(s, 1), :].astype(F32), axis=1, keepdims=True) > 0.0
        values = v_s[h * T16:(h + 1) * T16, lanes].astype(F32)[0:H8]
        mean = jnp.sum(values, axis=1, keepdims=True) * (1.0 / 256.0)
        out = out_s[slot][h]
        att[h * H8:(h + 1) * H8, lanes] = jnp.where(some, out[0:H8] * (1.0 / out[H8:9]), mean)

    load_q(0, 0)
    load_q(1, 1)

    def attend(t, carry):
        for step in range(6):
            s, slot = 6 * t + step, step % TWO
            for h in range(H8):
                score(slot, s, h)
                combine(slot, s - TWO, h)
                soften(1 - slot, s - 1, h)
            load_q(slot, s + TWO)
        return carry

    lax.fori_loop(0, 11, attend, 0)

    w_ro = dot_t(eye(C64), wro_ref[...]).astype(BF16)
    gate_bias = column(brg_ref[...], lambda row: row, C64)
    qs_ref[0:C64, :] = jnp.zeros((C64, R256), F32)
    qs_ref[C64:72, :] = jnp.broadcast_to(jnp.sum(mask_ref[...].astype(F32), axis=0, keepdims=True), (H8, R256))

    def finish_part(part, carry):
        lanes = pl.ds(pl.multiple_of(part * W2K, W2K), W2K)
        gate = jax.nn.sigmoid(g_s[:, lanes].astype(F32) + gate_bias)
        gated = (gate * att[:, lanes]).astype(BF16)
        e_one = (x_s[:, lanes].astype(F32) + dot(w_ro, gated)).astype(BF16)
        e1_ref[:, lanes] = e_one
        proj = dot(w_ci[...], norm_cols(e_one.astype(F32))).astype(BF16)
        g1_ref[:, lanes] = proj[C64:L128]
        keep = mask_ref[pl.ds(pl.multiple_of(part * H8, H8), H8), :].astype(F32)
        q_sum = jnp.zeros((C64, R256), F32)
        for t in range(H8):
            cut = slice(t * R256, (t + 1) * R256)
            kv_ref[part * H8 + t] = proj[L128:K144, cut].astype(F32)
            q_sum += proj[0:C64, cut].astype(F32) * keep[t:t + 1]
        qs_ref[0:C64, :] += q_sum
        return carry

    lax.fori_loop(0, H8, finish_part, 0)


def row_stage(msa, pair, mask, wpb, wri, brg, wro, wci):
    any_spec = pl.BlockSpec(memory_space=pl.ANY)
    vmem = pl.BlockSpec(memory_space=pltpu.VMEM)
    return pl.pallas_call(
        row_kernel,
        name='row_stage',
        out_shape=(
            jax.ShapeDtypeStruct((C64, ALL16K), BF16),
            jax.ShapeDtypeStruct((C64, ALL16K), BF16),
            jax.ShapeDtypeStruct((C64, T16, R256), F32),
            jax.ShapeDtypeStruct((72, R256), F32),
        ),
        in_specs=[any_spec, any_spec] + [vmem] * 6,
        out_specs=(vmem,) * FOUR,
        scratch_shapes=[
            pltpu.VMEM((C64, R256, L128), BF16),
            pltpu.VMEM((C64, C64, R256), BF16),
            pltpu.VMEM((TWO, C64, L128), F32),
            pltpu.VMEM((H8, C64, R256), F32),
            pltpu.VMEM((H8, R256, R256), BF16),
            pltpu.VMEM((H8, R256, R256), F32),
            pltpu.VMEM((L128, ALL16K), BF16),
            pltpu.VMEM((ALL16K, K144), BF16),
            pltpu.VMEM((L128, ALL16K), BF16),
            pltpu.VMEM((C64, ALL16K), BF16),
            pltpu.VMEM((C64, ALL16K), BF16),
            pltpu.VMEM((T16, K144, R256), BF16),
            pltpu.VMEM((C64, ALL16K), F32),
            pltpu.VMEM((384, C64), BF16),
            pltpu.VMEM((K144, C64), BF16),
            pltpu.VMEM((H8, R256, R256), F32),
            pltpu.VMEM((H8, R256, R256), F32),
            pltpu.VMEM((H8, H8, R256), F32),
            pltpu.VMEM((H8, H8, R256), F32),
            pltpu.VMEM((H8, T16, R256), F32),
            pltpu.VMEM((H8, T16, R256), F32),
            pltpu.SemaphoreType.DMA((H8,)),
            pltpu.SemaphoreType.DMA((H8,)),
            pltpu.SemaphoreType.DMA((THREE,)),
            pltpu.SemaphoreType.DMA((THREE,)),
        ],
        compiler_params=pltpu.CompilerParams(collective_id=0, has_side_effects=True, vmem_limit_bytes=VMEM_LIMIT),
    )(msa, pair, mask, wpb, wri, brg, wro, wci)


def tail_kernel(qs_ref, kv_ref, mask_ref, e_buf, g_buf, z_hbm, bcg_ref, wco_ref, wti_ref, wto_ref, wom_ref, w_ref, b_ref,
                e3_ref, out_ref,
                first, second, stat, logit_s, z_buf,
                w_co, w_ti, w_to, w_om, ab_s, ab,
                a_half, b_full, m_full, turn_s, a_tmp, a_s, acc, p_hi0, p_lo0, p_hi1, p_lo1, w_tmp, w_t, inv_s,
                load_sem, stat_send, stat_recv, send_sem, recv_sem):
    me, batch, mate, cross = place()
    z_load = pltpu.make_async_copy(z_hbm, z_buf, load_sem)
    z_load.start()
    peers = [lax.rem(me + step, FOUR) for step in (1, TWO, THREE)]
    meet(batch, peers)

    def share(src, slots, base):
        copies = []
        for n, peer in enumerate(peers):
            copies.append(pltpu.make_async_remote_copy(
                src_ref=src, dst_ref=slots, send_sem=stat_send.at[base + n], recv_sem=stat_recv.at[base + n],
                device_id=(batch, peer), device_id_type=MESH))
        for copy in copies:
            copy.start()
        return copies

    query_copies = share(qs_ref, first.at[me], 0)
    first[me] = qs_ref[...]
    m_full[rows64(me), :] = mask_ref[...].astype(F32).astype(BF16)
    mask_copies = share(m_full.at[rows64(me), :], m_full.at[rows64(me), :], 6)

    w_co[...] = dot(dot_t(eye(C64), wco_ref[...]).astype(BF16),
                    (swap8(iota((C64, C64), 1)) == iota((C64, C64), 0)).astype(BF16)).astype(BF16)
    w_ti[...] = dot_t(eye(R256), wti_ref[...]).astype(BF16)
    w_to[...] = wto_ref[...]
    w_om[...] = dot_t(eye(C64), wom_ref[...]).astype(BF16)
    for c in range(O32):
        w_tmp[c * 40:c * 40 + O32, :] = w_ref[c * O32:(c + 1) * O32, :].astype(F32)
    for k in range(FOUR):
        for d in range(H8):
            w_t[k, :, d * O32:(d + 1) * O32] = jnp.transpose(w_tmp[pl.ds(k * H8 + d, O32, stride=40), :]).astype(BF16)

    for copy in query_copies:
        copy.wait()
    total = first[0] + first[1] + first[TWO] + first[THREE]
    population = total[C64:72] + 1e-10
    q_bar = [(total[d * H8:(d + 1) * H8] / population).astype(BF16).astype(F32) for d in range(H8)]

    def scores(s, top):
        kv = kv_ref[s]
        value = q_bar[0] * kv[0:1]
        for d in range(1, H8):
            value += q_bar[d] * kv[d:d + 1]
        value = jnp.where(mask_ref[pl.ds(s, 1), :] > 0, value * (H8 ** -0.5), MASK_FILL)
        logit_s[s] = value
        return jnp.maximum(top, value)

    top = lax.fori_loop(0, C64, scores, jnp.full((H8, R256), -3e38, F32), unroll=FOUR)

    def gather(s, sums):
        kv = kv_ref[s]
        weight = jnp.exp(logit_s[s] - top)
        return (sums[0] + weight,) + tuple(sums[d + 1] + weight * kv[H8 + d:9 + d] for d in range(H8))

    sums = lax.fori_loop(0, C64, gather, (jnp.zeros((H8, R256), F32),) * 9, unroll=FOUR)
    stat[0:H8, :] = top
    for n in range(9):
        stat[H8 + n * H8:T16 + n * H8, :] = sums[n]
    stat_copies = share(stat, second.at[me], THREE)
    second[me] = stat[...]
    for copy in stat_copies:
        copy.wait()
    tops = [second[n, 0:H8, :] for n in range(FOUR)]
    best = jnp.maximum(jnp.maximum(tops[0], tops[1]), jnp.maximum(tops[TWO], tops[THREE]))
    scale = [jnp.exp(value - best) for value in tops]

    def merge(at):
        return sum(second[n, at:at + H8, :] * scale[n] for n in range(FOUR))

    den = merge(H8)
    column_out = jnp.concatenate([merge(T16 + d * H8) / den for d in range(H8)], axis=0)
    col = jnp.concatenate([column_out] * H8, axis=1)
    gate_bias = column(bcg_ref[...], swap8, C64)

    def send(src, dst, slot, peer):
        return pltpu.make_async_remote_copy(
            src_ref=src, dst_ref=dst, send_sem=send_sem.at[slot], recv_sem=recv_sem.at[slot],
            device_id=(batch, peer), device_id_type=MESH)

    def lanes_of(device):
        return pl.ds(pl.multiple_of((device // TWO) * L128, L128), L128)

    def rows16(device, block):
        return pl.ds(pl.multiple_of(device * C64 + block * T16, T16), T16)

    def b_piece(k, src_rows, dst_rows, slot, peer):
        return send(ab.at[pl.ds(O32 + k * H8, H8), src_rows, :], b_full.at[pl.ds(k * H8, H8), dst_rows, :], slot, peer)

    whole = pl.ds(0, C64)

    def a_cross(n):
        return send(ab.at[pl.ds(0, O32), rows16(0, n), lanes_of(cross)], a_half.at[:, rows16(me, n), :], n, cross)

    def first_cross(n):
        return b_piece(0, rows16(0, n), rows16(me, n), FOUR + n, cross)

    def late_cross(k):
        return b_piece(k, whole, rows64(me), 7 + k, cross)

    def b_mate(k):
        return b_piece(k, whole, rows64(me), 12 + k, mate)

    def b_relay(k):
        far_b = b_full.at[pl.ds(k * H8, H8), rows64(cross), :]
        return send(far_b, far_b, 17 + k, mate)

    a_mate = send(ab.at[pl.ds(0, O32), :, lanes_of(me)], a_half.at[:, rows64(me), :], 11, mate)
    far_a = a_half.at[:, rows64(cross), :]
    a_relay = send(far_a, far_a, T16, mate)


    def sixteen(block, done):
        def half(part, carry):
            where = block * TWO + part
            lanes = pl.ds(pl.multiple_of(where * W2K, W2K), W2K)
            gate = jax.nn.sigmoid(g_buf[:, lanes].astype(F32) + gate_bias)
            gated = (gate * col).astype(BF16)
            e_two = (e_buf[:, lanes].astype(F32) + dot(w_co[...], gated)).astype(BF16).astype(F32)
            hidden = jnp.maximum(dot(w_ti[...], norm_cols(e_two)), 0.0).astype(BF16)
            e_three = (e_two + dot(w_to[...], hidden)).astype(BF16).astype(F32)
            for t in range(H8):
                e3_ref[where * H8 + t] = e_three[:, t * R256:(t + 1) * R256].astype(BF16)
            proj = dot(w_om[...], norm_cols(e_three)).astype(BF16).astype(F32)
            keep = mask_ref[pl.ds(pl.multiple_of(where * H8, H8), H8), :].astype(F32)
            for t in range(H8):
                at = pl.ds(pl.multiple_of((part * H8 + t) * 72, H8), C64)
                for lane in range(TWO):
                    cut = slice(lane * L128, (lane + 1) * L128)
                    ab_s[lane, at, :] = proj[:, t * R256 + lane * L128:t * R256 + (lane + 1) * L128] * keep[t:t + 1, cut]
            return carry

        lax.fori_loop(0, TWO, half, 0)
        for f in range(C64):
            for lane in range(TWO):
                ab[f, rows16(0, block), lane * L128:(lane + 1) * L128] = (
                    ab_s[lane, pl.ds(f, T16, stride=72), :].astype(BF16))
        a_cross(block).start()
        first_cross(block).start()
        return done

    lax.fori_loop(0, FOUR, sixteen, 0)
    for k in range(1, FOUR):
        late_cross(k).start()
    a_mate.start()
    for k in range(FOUR):
        b_mate(k).start()

    a_half[:, rows64(me), :] = ab[0:O32, :, lanes_of(me)]
    b_full[:, rows64(me), :] = ab[O32:C64, :, :]
    for copy in mask_copies:
        copy.wait()
    keep_all = m_full[...]
    inv_s[...] = 1.0 / (dot(jnp.transpose(keep_all.astype(F32)).astype(BF16), keep_all) + 1e-3)
    z_load.wait()
    e_bias = b_ref[...].astype(F32)

    for n in range(FOUR):
        a_cross(n).wait_recv()
    a_relay.start()
    for n in range(FOUR):
        first_cross(n).wait_recv()
    b_relay(0).start()
    a_mate.wait_recv()
    a_relay.wait_recv()
    offset = pl.multiple_of(lax.rem(me, TWO) * C64, C64)

    def turn(c, carry):
        turn_s[...] = jnp.transpose(a_half[c].astype(F32))
        mine = turn_s[pl.ds(offset, C64), :]
        for lane in range(TWO):
            a_tmp[lane, pl.ds(pl.multiple_of(c * 72, H8), C64), :] = mine[:, lane * L128:(lane + 1) * L128]
        return carry

    lax.fori_loop(0, O32, turn, 0)
    for i in range(C64):
        for lane in range(TWO):
            a_s[i * O32:(i + 1) * O32, lane * L128:(lane + 1) * L128] = a_tmp[lane, pl.ds(i, O32, stride=72), :].astype(BF16)

    slots = ((p_hi0, p_lo0), (p_hi1, p_lo1))

    def outer(slot, index, d):
        p_hi, p_lo = slots[slot]
        k, n = index // H8, lax.rem(index, H8)
        value = dot(a_s[pl.ds(pl.multiple_of(n * R256, R256), R256), :], b_full[k * H8 + d])
        high = value.astype(BF16)
        low = (value - high.astype(F32)).astype(BF16)
        for i in range(H8):
            p_hi[i, d * O32:(d + 1) * O32, :] = high[i * O32:(i + 1) * O32]
            p_lo[i, d * O32:(d + 1) * O32, :] = low[i * O32:(i + 1) * O32]

    def project(slot, index, i):
        p_hi, p_lo = slots[slot]
        index = jnp.maximum(index, 0)
        k, at = index // H8, lax.rem(index, H8) * H8 + i
        part = dot(w_t[k], p_hi[i]) + dot(w_t[k], p_lo[i])
        acc[at] = jnp.where(k == 0, part, acc[at] + part)

    def settle(index, i):
        at = jnp.maximum(index - 24, 0) * H8 + i
        update = acc[at] * inv_s[pl.ds(me * C64 + at, 1), :]
        out_ref[at] = (z_buf[at].astype(F32) + jnp.transpose(update) + e_bias).astype(BF16)

    def pair(last, t, carry):
        k = t // FOUR

        @pl.when(lax.rem(t, FOUR) == 0)
        def _():
            b_mate(k).wait_recv()
            b_relay(k).wait_recv()

        if not last:
            @pl.when(lax.rem(t, FOUR) == TWO)
            def _():
                late_cross(k + 1).wait_recv()
                b_relay(k + 1).start()

        for slot in range(TWO):
            index = TWO * t + slot
            for n in range(H8):
                outer(slot, index, n)
                project(1 - slot, index - 1, n)
                if last:
                    settle(index - TWO, n)
        return carry

    lax.fori_loop(0, 12, functools.partial(pair, False), 0)
    lax.fori_loop(12, T16, functools.partial(pair, True), 0)
    for n in range(H8):
        project(1, 31, n)
        settle(30, n)
    for n in range(H8):
        settle(31, n)
    a_mate.wait_send()
    a_relay.wait_send()
    for n in range(FOUR):
        a_cross(n).wait_send()
        first_cross(n).wait_send()
        b_mate(n).wait_send()
        b_relay(n).wait_send()
    for k in range(1, FOUR):
        late_cross(k).wait_send()


def tail_stage(qs, kv, mask, e1, g1, pair, bcg, wco, wti, wto, wom, weight, bias):
    any_spec = pl.BlockSpec(memory_space=pl.ANY)
    vmem = pl.BlockSpec(memory_space=pltpu.VMEM)
    return pl.pallas_call(
        tail_kernel,
        name='tail_stage',
        out_shape=(jax.ShapeDtypeStruct((C64, C64, R256), BF16), jax.ShapeDtypeStruct((C64, R256, L128), BF16)),
        in_specs=[vmem] * 5 + [any_spec] + [vmem] * 7,
        out_specs=(vmem, vmem),
        scratch_shapes=[
            pltpu.VMEM((FOUR, 72, R256), F32),
            pltpu.VMEM((FOUR, 80, R256), F32),
            pltpu.VMEM((80, R256), F32),
            pltpu.VMEM((C64, H8, R256), F32),
            pltpu.VMEM((C64, R256, L128), BF16),
            pltpu.VMEM((C64, C64), BF16),
            pltpu.VMEM((R256, C64), BF16),
            pltpu.VMEM((C64, R256), BF16),
            pltpu.VMEM((C64, C64), BF16),
            pltpu.VMEM((TWO, 1152, L128), F32),
            pltpu.VMEM((C64, C64, R256), BF16),
            pltpu.VMEM((O32, R256, L128), BF16),
            pltpu.VMEM((O32, R256, R256), BF16),
            pltpu.VMEM((R256, R256), BF16),
            pltpu.VMEM((L128, R256), F32),
            pltpu.VMEM((TWO, 2304, L128), F32),
            pltpu.VMEM((W2K, R256), BF16),
            pltpu.VMEM((C64, L128, R256), F32),
        ] + [pltpu.VMEM((H8, R256, R256), BF16)] * FOUR + [
            pltpu.VMEM((1280, L128), F32),
            pltpu.VMEM((FOUR, L128, R256), BF16),
            pltpu.VMEM((R256, R256), F32),
            pltpu.SemaphoreType.DMA(()),
            pltpu.SemaphoreType.DMA((9,)),
            pltpu.SemaphoreType.DMA((9,)),
            pltpu.SemaphoreType.DMA((21,)),
            pltpu.SemaphoreType.DMA((21,)),
        ],
        compiler_params=pltpu.CompilerParams(collective_id=1, has_side_effects=True, vmem_limit_bytes=TAIL_LIMIT),
    )(qs, kv, mask, e1, g1, pair, bcg, wco, wti, wto, wom, weight, bias)


def solution(mesh):
    row_spec = P(('batch', 'seq'))
    rep_spec = P()

    def local_block(msa, mask, pair, w_pair_bias, w_row_in, b_row_gate, w_row_out, w_col_in, b_col_gate, w_col_out, w_trans_in, w_trans_out, w_opm_in, w_opm_out, b_opm_out):
        e1, g1, kv, qs = row_stage(jnp.swapaxes(msa, 1, TWO), pair, mask, w_pair_bias.T, w_row_in, b_row_gate.reshape(1, C64), w_row_out, w_col_in)
        e3, pair_out = tail_stage(qs, kv, mask, e1, g1, pair, b_col_gate.reshape(1, C64), w_col_out, w_trans_in, w_trans_out.T, w_opm_in, w_opm_out.reshape(1024, L128), b_opm_out.reshape(1, L128))
        return jnp.swapaxes(e3, 1, TWO), pair_out

    return jax.shard_map(local_block, mesh=mesh, in_specs=(row_spec, row_spec, row_spec) + (rep_spec,) * 12, out_specs=(row_spec, row_spec), check_vma=False)
```

```python
import functools

import jax
import jax.numpy as jnp
from jax import lax
from jax.experimental import pallas as pl
from jax.experimental.pallas import tpu as pltpu
from jax.sharding import PartitionSpec as P

F32, BF16 = jnp.float32, jnp.bfloat16
MESH = pl.DeviceIdType.MESH
LOG2E = 1.4426950408889634
MASK_FILL = -1e9
R256 = 256
C64 = 64
L128 = 128
H8 = 8
W2K = 2048
T16 = 16
O32 = 32
TWO = 2
FOUR = 4
K144 = 144
ALL16K = 16384
THREE = 3
VMEM_LIMIT = 46000 * 1024
TAIL_LIMIT = 40000 * 1024


def dot(left, right):
    return jnp.dot(left, right, preferred_element_type=F32)


def dot_t(left, right):
    return lax.dot_general(left, right, (((1,), (1,)), ((), ())), preferred_element_type=F32)


def iota(shape, axis):
    return lax.broadcasted_iota(jnp.int32, shape, axis)


def norm_cols(values):
    centered = values - jnp.mean(values, axis=0, keepdims=True)
    variance = jnp.mean(centered * centered, axis=0, keepdims=True)
    return (centered * lax.rsqrt(variance + 1e-5)).astype(BF16)


def eye(size):
    return (iota((size, size), 0) == iota((size, size), 1)).astype(BF16)


def pick(rows, columns, index):
    return (index(iota((rows, columns), 0)) == iota((rows, columns), 1)).astype(BF16)


def swap8(row):
    return (row % H8) * H8 + row // H8


def column(row_vector, index, size):
    hit = index(iota((size, size), 0)) == iota((size, size), 1)
    wide = jnp.broadcast_to(row_vector.astype(F32), (size, size))
    return jnp.sum(jnp.where(hit, wide, 0.0), axis=1, keepdims=True)


def place():
    me = lax.axis_index('seq')
    batch = lax.axis_index('batch')
    mate = me + 1 - TWO * lax.rem(me, TWO)
    cross = lax.rem(me + TWO, FOUR)
    return me, batch, mate, cross


def meet(batch, peers):
    barrier = pltpu.get_barrier_semaphore()
    for peer in peers:
        pl.semaphore_signal(barrier, inc=1, device_id=(batch, peer), device_id_type=MESH)
    pl.semaphore_wait(barrier, len(peers))


def rows64(index):
    return pl.ds(pl.multiple_of(index * C64, C64), C64)


def row_kernel(e_hbm, z_hbm, mask_hbm, wpb_hbm, wri_hbm, brg_hbm, wro_hbm, wci_hbm,
               e1_ref, g1_ref, kv_ref, qs_ref,
               mask_ref, wpb_ref, wri_ref, brg_ref, wro_ref, wci_ref, small_sem, z_buf, e_buf, tmp, own, full, bias, q_s, k_s, v_s, g_s, x_s, rhs, att, w_big, w_ci,
               logit_0, logit_1, top_0, top_1, out_0, out_1, z_sem, e_sem, send_sem, recv_sem):
    logit_s, top_s, out_s = (logit_0, logit_1), (top_0, top_1), (out_0, out_1)
    me, batch, mate, cross = place()
    small = [pltpu.make_async_copy(src, dst, small_sem.at[n]) for n, (src, dst) in enumerate((
        (wpb_hbm, wpb_ref), (wri_hbm, wri_ref), (wci_hbm, wci_ref), (mask_hbm, mask_ref), (wro_hbm, wro_ref), (brg_hbm, brg_ref)))]
    small[0].start()
    for part in range(H8):
        pltpu.make_async_copy(z_hbm.at[pl.ds(part * H8, H8)], z_buf.at[pl.ds(part * H8, H8)], z_sem.at[part]).start()
    for copy in small[1:]:
        copy.start()
    for part in range(H8):
        pltpu.make_async_copy(e_hbm.at[pl.ds(part * H8, H8)], e_buf.at[pl.ds(part * H8, H8)], e_sem.at[part]).start()
    meet(batch, (mate, cross))

    def big_index(row):
        in_k, in_v = row - C64, row - 192
        head_k = C64 + (in_k // T16) * H8 + in_k % H8
        head_v = jnp.where(in_v % T16 < H8, L128 + (in_v // T16) * H8 + in_v % H8, -1)
        return jnp.where(row < C64, row, jnp.where(row < 192, head_k, jnp.where(row < 320, head_v, row - L128)))

    small[0].wait()
    w_pb = wpb_ref[...]
    rhs[...] = jnp.broadcast_to((iota((K144, R256), 0) == L128).astype(BF16)[None], (T16, K144, R256))

    def bias_part(part, carry):
        pltpu.make_async_copy(z_hbm.at[pl.ds(part * H8, H8)], z_buf.at[pl.ds(part * H8, H8)], z_sem.at[part]).wait()
        z_t = jnp.transpose(z_buf[pl.ds(part * H8, H8)].reshape(W2K, L128).astype(F32))
        heads = dot(w_pb, norm_cols(z_t))
        for t in range(H8):
            for lane in range(TWO):
                at = t * R256 + lane * L128
                tmp[lane, t * H8:(t + 1) * H8, :] = heads[:, at:at + L128]
        for h in range(H8):
            for lane in range(TWO):
                own[h, pl.ds(pl.multiple_of(part * H8, H8), H8), lane * L128:(lane + 1) * L128] = tmp[lane, pl.ds(h, H8, stride=H8), :]
        return carry

    def ship(view, slot, peer):
        return pltpu.make_async_remote_copy(
            src_ref=view, dst_ref=view, send_sem=send_sem.at[slot], recv_sem=recv_sem.at[slot],
            device_id=(batch, peer), device_id_type=MESH)

    def piece(n, slot, peer):
        rows = pl.ds(pl.multiple_of(me * C64 + n * T16, T16), T16)
        return ship(full.at[:, rows, :], slot + n, peer)

    def bias_piece(n, carry):
        lax.fori_loop(TWO * n, TWO * n + TWO, bias_part, 0)
        full[:, pl.ds(pl.multiple_of(me * C64 + n * T16, T16), T16), :] = own[:, pl.ds(pl.multiple_of(n * T16, T16), T16), :].astype(BF16)
        piece(n, 0, cross).start()
        piece(n, FOUR, mate).start()
        return carry

    lax.fori_loop(0, FOUR, bias_piece, 0)
    relay = ship(full.at[:, rows64(cross), :], H8, mate)

    for copy in small[1:]:
        copy.wait()
    w_big[...] = dot_t(pick(384, R256, big_index), wri_ref[...]).astype(BF16)
    w_ci[...] = dot_t(
        pick(K144, K144, lambda row: jnp.where(row < C64, swap8(row), jnp.where(row < L128, C64 + swap8(row - C64), row))),
        wci_ref[...]).astype(BF16)
    ones = ((iota((L128, W2K), 0) % T16) == H8).astype(F32)

    def project_part(part, carry):
        pltpu.make_async_copy(e_hbm.at[pl.ds(part * H8, H8)], e_buf.at[pl.ds(part * H8, H8)], e_sem.at[part]).wait()
        lanes = pl.ds(pl.multiple_of(part * W2K, W2K), W2K)
        x_raw = jnp.concatenate([e_buf[part * H8 + t] for t in range(H8)], axis=1)
        x_s[:, lanes] = x_raw
        x_t = x_raw.astype(F32)
        proj = dot(w_big[...], norm_cols(x_t))
        q_val = proj[0:C64].astype(BF16).astype(F32) * (H8 ** -0.5 * LOG2E)
        q_hi = q_val.astype(BF16).astype(F32)
        q_lo = q_val - q_hi
        for h in range(H8):
            pair = jnp.concatenate([q_hi[h * H8:h * H8 + H8], q_lo[h * H8:h * H8 + H8]], axis=0)
            q_s[h * T16:(h + 1) * T16, lanes] = pair.astype(BF16)
        keep = mask_ref[pl.ds(pl.multiple_of(part * H8, H8), H8), :].astype(F32)
        keep_row = jnp.concatenate([keep[t:t + 1] for t in range(H8)], axis=1)
        k_s[lanes, 0:L128] = jnp.transpose(proj[C64:192] * keep_row).astype(BF16)
        fill = jnp.where(iota((T16, W2K), 0) == 0, (1.0 - keep_row) * (MASK_FILL * LOG2E), 0.0)
        k_s[lanes, L128:K144] = jnp.transpose(fill).astype(BF16)
        v_s[:, lanes] = (proj[192:320] + ones).astype(BF16)
        g_s[:, lanes] = proj[320:384].astype(BF16)
        return carry

    lax.fori_loop(0, 6, project_part, 0)
    for n in range(FOUR):
        piece(n, 0, cross).wait_recv()
    relay.start()
    lax.fori_loop(6, H8, project_part, 0)
    for n in range(FOUR):
        piece(n, FOUR, mate).wait_recv()
    relay.wait_recv()
    for n in range(H8):
        piece(n % FOUR, n // FOUR * FOUR, mate).wait_send()
    relay.wait_send()
    for h in range(H8):
        bias[h] = jnp.transpose(full[h].astype(F32)) * LOG2E

    def at_seq(s):
        s = jnp.clip(s, 0, 63)
        return s, pl.ds(pl.multiple_of(s * R256, R256), R256)

    def load_q(slot, s):
        lanes = at_seq(s)[1]
        for h in range(H8):
            sub = slice(h * T16, (h + 1) * T16)
            rhs[slot * H8 + h, sub, :] = q_s[sub, lanes]

    def score(slot, s, h):
        lanes = at_seq(s)[1]
        logits = dot(k_s[lanes, :], rhs[slot * H8 + h]) + bias[h]
        logit_s[slot][h] = logits
        tops = jnp.max(logits.reshape(FOUR, H8, H8, R256), axis=1)
        tops = jnp.maximum(jnp.maximum(tops[0], tops[1]), jnp.maximum(tops[TWO], tops[THREE]))
        top_s[slot][h] = jnp.broadcast_to(jnp.max(tops, axis=0, keepdims=True), (H8, R256))

    def soften(slot, s, h):
        lanes = at_seq(s)[1]
        v_blk = v_s[h * T16:(h + 1) * T16, lanes]
        shifted = logit_s[slot][h].reshape(O32, H8, R256) - top_s[slot][h][None]
        out_s[slot][h] = dot(v_blk, jnp.exp2(shifted).reshape(R256, R256).astype(BF16))

    def combine(slot, s, h):
        s, lanes = at_seq(s)
        some = jnp.max(mask_ref[pl.ds(s, 1), :].astype(F32), axis=1, keepdims=True) > 0.0
        values = v_s[h * T16:(h + 1) * T16, lanes].astype(F32)[0:H8]
        mean = jnp.sum(values, axis=1, keepdims=True) * (1.0 / 256.0)
        out = out_s[slot][h]
        att[h * H8:(h + 1) * H8, lanes] = jnp.where(some, out[0:H8] * (1.0 / out[H8:9]), mean)

    load_q(0, 0)
    load_q(1, 1)

    def attend(t, carry):
        for step in range(6):
            s, slot = 6 * t + step, step % TWO
            for h in range(H8):
                score(slot, s, h)
                combine(slot, s - TWO, h)
                soften(1 - slot, s - 1, h)
            load_q(slot, s + TWO)
        return carry

    lax.fori_loop(0, 11, attend, 0)

    w_ro = dot_t(eye(C64), wro_ref[...]).astype(BF16)
    gate_bias = column(brg_ref[...], lambda row: row, C64)
    qs_ref[0:C64, :] = jnp.zeros((C64, R256), F32)
    qs_ref[C64:72, :] = jnp.broadcast_to(jnp.sum(mask_ref[...].astype(F32), axis=0, keepdims=True), (H8, R256))

    def finish_part(part, carry):
        lanes = pl.ds(pl.multiple_of(part * W2K, W2K), W2K)
        gate = jax.nn.sigmoid(g_s[:, lanes].astype(F32) + gate_bias)
        gated = (gate * att[:, lanes]).astype(BF16)
        e_one = (x_s[:, lanes].astype(F32) + dot(w_ro, gated)).astype(BF16)
        e1_ref[:, lanes] = e_one
        proj = dot(w_ci[...], norm_cols(e_one.astype(F32))).astype(BF16)
        g1_ref[:, lanes] = proj[C64:L128]
        keep = mask_ref[pl.ds(pl.multiple_of(part * H8, H8), H8), :].astype(F32)
        q_sum = jnp.zeros((C64, R256), F32)
        for t in range(H8):
            cut = slice(t * R256, (t + 1) * R256)
            kv_ref[part * H8 + t] = proj[L128:K144, cut].astype(F32)
            q_sum += proj[0:C64, cut].astype(F32) * keep[t:t + 1]
        qs_ref[0:C64, :] += q_sum
        return carry

    lax.fori_loop(0, H8, finish_part, 0)


def row_stage(msa, pair, mask, wpb, wri, brg, wro, wci):
    hbm = pl.BlockSpec(memory_space=pltpu.HBM)
    vmem = pl.BlockSpec(memory_space=pltpu.VMEM)
    return pl.pallas_call(
        row_kernel,
        name='row_stage',
        out_shape=(
            jax.ShapeDtypeStruct((C64, ALL16K), BF16),
            jax.ShapeDtypeStruct((C64, ALL16K), BF16),
            jax.ShapeDtypeStruct((C64, T16, R256), F32),
            jax.ShapeDtypeStruct((72, R256), F32),
        ),
        in_specs=[hbm] * H8,
        out_specs=(vmem,) * FOUR,
        scratch_shapes=[
            pltpu.VMEM((C64, R256), jnp.int32),
            pltpu.VMEM((H8, L128), BF16),
            pltpu.VMEM((C64, R256), BF16),
            pltpu.VMEM((1, C64), BF16),
            pltpu.VMEM((C64, C64), BF16),
            pltpu.VMEM((C64, K144), BF16),
            pltpu.SemaphoreType.DMA((6,)),
            pltpu.VMEM((C64, R256, L128), BF16),
            pltpu.VMEM((C64, C64, R256), BF16),
            pltpu.VMEM((TWO, C64, L128), F32),
            pltpu.VMEM((H8, C64, R256), F32),
            pltpu.VMEM((H8, R256, R256), BF16),
            pltpu.VMEM((H8, R256, R256), F32),
            pltpu.VMEM((L128, ALL16K), BF16),
            pltpu.VMEM((ALL16K, K144), BF16),
            pltpu.VMEM((L128, ALL16K), BF16),
            pltpu.VMEM((C64, ALL16K), BF16),
            pltpu.VMEM((C64, ALL16K), BF16),
            pltpu.VMEM((T16, K144, R256), BF16),
            pltpu.VMEM((C64, ALL16K), F32),
            pltpu.VMEM((384, C64), BF16),
            pltpu.VMEM((K144, C64), BF16),
            pltpu.VMEM((H8, R256, R256), F32),
            pltpu.VMEM((H8, R256, R256), F32),
            pltpu.VMEM((H8, H8, R256), F32),
            pltpu.VMEM((H8, H8, R256), F32),
            pltpu.VMEM((H8, T16, R256), F32),
            pltpu.VMEM((H8, T16, R256), F32),
            pltpu.SemaphoreType.DMA((H8,)),
            pltpu.SemaphoreType.DMA((H8,)),
            pltpu.SemaphoreType.DMA((9,)),
            pltpu.SemaphoreType.DMA((9,)),
        ],
        compiler_params=pltpu.CompilerParams(collective_id=0, has_side_effects=True, vmem_limit_bytes=VMEM_LIMIT),
    )(msa, pair, mask, wpb, wri, brg, wro, wci)


def tail_kernel(qs_ref, kv_ref, mask_ref, e_buf, g_buf, z_hbm, bcg_ref, wco_ref, wti_ref, wto_ref, wom_ref, w_ref, b_ref,
                e3_ref, out_ref,
                first, second, stat, logit_s, z_buf,
                w_co, w_ti, w_to, w_om, ab_s, ab,
                a_half, b_full, m_full, turn_s, a_tmp, a_s, acc, p_hi0, p_lo0, p_hi1, p_lo1, w_tmp, w_t, inv_s,
                load_sem, stat_send, stat_recv, send_sem, recv_sem):
    me, batch, mate, cross = place()
    z_load = pltpu.make_async_copy(z_hbm, z_buf, load_sem)
    z_load.start()
    peers = [lax.rem(me + step, FOUR) for step in (1, TWO, THREE)]
    meet(batch, peers)

    def share(src, slots, base):
        copies = []
        for n, peer in enumerate(peers):
            copies.append(pltpu.make_async_remote_copy(
                src_ref=src, dst_ref=slots, send_sem=stat_send.at[base + n], recv_sem=stat_recv.at[base + n],
                device_id=(batch, peer), device_id_type=MESH))
        for copy in copies:
            copy.start()
        return copies

    query_copies = share(qs_ref, first.at[me], 0)
    first[me] = qs_ref[...]
    m_full[rows64(me), :] = mask_ref[...].astype(F32).astype(BF16)
    mask_copies = share(m_full.at[rows64(me), :], m_full.at[rows64(me), :], 6)

    w_co[...] = dot(dot_t(eye(C64), wco_ref[...]).astype(BF16),
                    (swap8(iota((C64, C64), 1)) == iota((C64, C64), 0)).astype(BF16)).astype(BF16)
    w_ti[...] = dot_t(eye(R256), wti_ref[...]).astype(BF16)
    w_to[...] = wto_ref[...]
    w_om[...] = dot_t(eye(C64), wom_ref[...]).astype(BF16)
    for c in range(O32):
        w_tmp[c * 40:c * 40 + O32, :] = w_ref[c * O32:(c + 1) * O32, :].astype(F32)
    for k in range(FOUR):
        for d in range(H8):
            w_t[k, :, d * O32:(d + 1) * O32] = jnp.transpose(w_tmp[pl.ds(k * H8 + d, O32, stride=40), :]).astype(BF16)

    for copy in query_copies:
        copy.wait()
    total = first[0] + first[1] + first[TWO] + first[THREE]
    population = total[C64:72] + 1e-10
    q_bar = [(total[d * H8:(d + 1) * H8] / population).astype(BF16).astype(F32) for d in range(H8)]

    def scores(s, top):
        kv = kv_ref[s]
        value = q_bar[0] * kv[0:1]
        for d in range(1, H8):
            value += q_bar[d] * kv[d:d + 1]
        value = jnp.where(mask_ref[pl.ds(s, 1), :] > 0, value * (H8 ** -0.5), MASK_FILL)
        logit_s[s] = value
        return jnp.maximum(top, value)

    top = lax.fori_loop(0, C64, scores, jnp.full((H8, R256), -3e38, F32), unroll=FOUR)

    def gather(s, sums):
        kv = kv_ref[s]
        weight = jnp.exp(logit_s[s] - top)
        return (sums[0] + weight,) + tuple(sums[d + 1] + weight * kv[H8 + d:9 + d] for d in range(H8))

    sums = lax.fori_loop(0, C64, gather, (jnp.zeros((H8, R256), F32),) * 9, unroll=FOUR)
    stat[0:H8, :] = top
    for n in range(9):
        stat[H8 + n * H8:T16 + n * H8, :] = sums[n]
    stat_copies = share(stat, second.at[me], THREE)
    second[me] = stat[...]
    for copy in stat_copies:
        copy.wait()
    tops = [second[n, 0:H8, :] for n in range(FOUR)]
    best = jnp.maximum(jnp.maximum(tops[0], tops[1]), jnp.maximum(tops[TWO], tops[THREE]))
    scale = [jnp.exp(value - best) for value in tops]

    def merge(at):
        return sum(second[n, at:at + H8, :] * scale[n] for n in range(FOUR))

    den = merge(H8)
    column_out = jnp.concatenate([merge(T16 + d * H8) / den for d in range(H8)], axis=0)
    col = jnp.concatenate([column_out] * H8, axis=1)
    gate_bias = column(bcg_ref[...], swap8, C64)

    def send(src, dst, slot, peer):
        return pltpu.make_async_remote_copy(
            src_ref=src, dst_ref=dst, send_sem=send_sem.at[slot], recv_sem=recv_sem.at[slot],
            device_id=(batch, peer), device_id_type=MESH)

    def lanes_of(device):
        return pl.ds(pl.multiple_of((device // TWO) * L128, L128), L128)

    def rows16(device, block):
        return pl.ds(pl.multiple_of(device * C64 + block * T16, T16), T16)

    def b_piece(k, src_rows, dst_rows, slot, peer):
        return send(ab.at[pl.ds(O32 + k * H8, H8), src_rows, :], b_full.at[pl.ds(k * H8, H8), dst_rows, :], slot, peer)

    whole = pl.ds(0, C64)

    def a_cross(n):
        return send(ab.at[pl.ds(0, O32), rows16(0, n), lanes_of(cross)], a_half.at[:, rows16(me, n), :], n, cross)

    def first_cross(n):
        return b_piece(0, rows16(0, n), rows16(me, n), FOUR + n, cross)

    def late_cross(k):
        return b_piece(k, whole, rows64(me), 7 + k, cross)

    def b_mate(k):
        return b_piece(k, whole, rows64(me), 12 + k, mate)

    def b_relay(k):
        far_b = b_full.at[pl.ds(k * H8, H8), rows64(cross), :]
        return send(far_b, far_b, 17 + k, mate)

    a_mate = send(ab.at[pl.ds(0, O32), :, lanes_of(me)], a_half.at[:, rows64(me), :], 11, mate)
    far_a = a_half.at[:, rows64(cross), :]
    a_relay = send(far_a, far_a, T16, mate)


    def sixteen(block, done):
        def half(part, carry):
            where = block * TWO + part
            lanes = pl.ds(pl.multiple_of(where * W2K, W2K), W2K)
            gate = jax.nn.sigmoid(g_buf[:, lanes].astype(F32) + gate_bias)
            gated = (gate * col).astype(BF16)
            e_two = (e_buf[:, lanes].astype(F32) + dot(w_co[...], gated)).astype(BF16).astype(F32)
            hidden = jnp.maximum(dot(w_ti[...], norm_cols(e_two)), 0.0).astype(BF16)
            e_three = (e_two + dot(w_to[...], hidden)).astype(BF16).astype(F32)
            for t in range(H8):
                e3_ref[where * H8 + t] = e_three[:, t * R256:(t + 1) * R256].astype(BF16)
            proj = dot(w_om[...], norm_cols(e_three)).astype(BF16).astype(F32)
            keep = mask_ref[pl.ds(pl.multiple_of(where * H8, H8), H8), :].astype(F32)
            for t in range(H8):
                at = pl.ds(pl.multiple_of((part * H8 + t) * 72, H8), C64)
                for lane in range(TWO):
                    cut = slice(lane * L128, (lane + 1) * L128)
                    ab_s[lane, at, :] = proj[:, t * R256 + lane * L128:t * R256 + (lane + 1) * L128] * keep[t:t + 1, cut]
            return carry

        lax.fori_loop(0, TWO, half, 0)
        for f in range(C64):
            for lane in range(TWO):
                ab[f, rows16(0, block), lane * L128:(lane + 1) * L128] = (
                    ab_s[lane, pl.ds(f, T16, stride=72), :].astype(BF16))
        a_cross(block).start()
        first_cross(block).start()
        return done

    lax.fori_loop(0, FOUR, sixteen, 0)
    for k in range(1, FOUR):
        late_cross(k).start()
    a_mate.start()
    for k in range(FOUR):
        b_mate(k).start()

    a_half[:, rows64(me), :] = ab[0:O32, :, lanes_of(me)]
    b_full[:, rows64(me), :] = ab[O32:C64, :, :]
    for copy in mask_copies:
        copy.wait()
    keep_all = m_full[...]
    inv_s[...] = 1.0 / (dot(jnp.transpose(keep_all.astype(F32)).astype(BF16), keep_all) + 1e-3)
    z_load.wait()
    e_bias = b_ref[...].astype(F32)

    for n in range(FOUR):
        a_cross(n).wait_recv()
    a_relay.start()
    for n in range(FOUR):
        first_cross(n).wait_recv()
    b_relay(0).start()
    a_mate.wait_recv()
    a_relay.wait_recv()
    offset = pl.multiple_of(lax.rem(me, TWO) * C64, C64)

    def turn(c, carry):
        turn_s[...] = jnp.transpose(a_half[c].astype(F32))
        mine = turn_s[pl.ds(offset, C64), :]
        for lane in range(TWO):
            a_tmp[lane, pl.ds(pl.multiple_of(c * 72, H8), C64), :] = mine[:, lane * L128:(lane + 1) * L128]
        return carry

    lax.fori_loop(0, O32, turn, 0)
    for i in range(C64):
        for lane in range(TWO):
            a_s[i * O32:(i + 1) * O32, lane * L128:(lane + 1) * L128] = a_tmp[lane, pl.ds(i, O32, stride=72), :].astype(BF16)

    slots = ((p_hi0, p_lo0), (p_hi1, p_lo1))

    def outer(slot, index, d):
        p_hi, p_lo = slots[slot]
        k, n = index // H8, lax.rem(index, H8)
        value = dot(a_s[pl.ds(pl.multiple_of(n * R256, R256), R256), :], b_full[k * H8 + d])
        high = value.astype(BF16)
        low = (value - high.astype(F32)).astype(BF16)
        for i in range(H8):
            p_hi[i, d * O32:(d + 1) * O32, :] = high[i * O32:(i + 1) * O32]
            p_lo[i, d * O32:(d + 1) * O32, :] = low[i * O32:(i + 1) * O32]

    def project(slot, index, i):
        p_hi, p_lo = slots[slot]
        index = jnp.maximum(index, 0)
        k, at = index // H8, lax.rem(index, H8) * H8 + i
        part = dot(w_t[k], p_hi[i]) + dot(w_t[k], p_lo[i])
        acc[at] = jnp.where(k == 0, part, acc[at] + part)

    def settle(index, i):
        at = jnp.maximum(index - 24, 0) * H8 + i
        update = acc[at] * inv_s[pl.ds(me * C64 + at, 1), :]
        out_ref[at] = (z_buf[at].astype(F32) + jnp.transpose(update) + e_bias).astype(BF16)

    def pair(last, t, carry):
        k = t // FOUR

        @pl.when(lax.rem(t, FOUR) == 0)
        def _():
            b_mate(k).wait_recv()
            b_relay(k).wait_recv()

        if not last:
            @pl.when(lax.rem(t, FOUR) == TWO)
            def _():
                late_cross(k + 1).wait_recv()
                b_relay(k + 1).start()

        for slot in range(TWO):
            index = TWO * t + slot
            for n in range(H8):
                outer(slot, index, n)
                project(1 - slot, index - 1, n)
                if last:
                    settle(index - TWO, n)
        return carry

    lax.fori_loop(0, 12, functools.partial(pair, False), 0)
    lax.fori_loop(12, T16, functools.partial(pair, True), 0)
    for n in range(H8):
        project(1, 31, n)
        settle(30, n)
    for n in range(H8):
        settle(31, n)
    a_mate.wait_send()
    a_relay.wait_send()
    for n in range(FOUR):
        a_cross(n).wait_send()
        first_cross(n).wait_send()
        b_mate(n).wait_send()
        b_relay(n).wait_send()
    for k in range(1, FOUR):
        late_cross(k).wait_send()


def tail_stage(qs, kv, mask, e1, g1, pair, bcg, wco, wti, wto, wom, weight, bias):
    any_spec = pl.BlockSpec(memory_space=pl.ANY)
    vmem = pl.BlockSpec(memory_space=pltpu.VMEM)
    return pl.pallas_call(
        tail_kernel,
        name='tail_stage',
        out_shape=(jax.ShapeDtypeStruct((C64, C64, R256), BF16), jax.ShapeDtypeStruct((C64, R256, L128), BF16)),
        in_specs=[vmem] * 5 + [any_spec] + [vmem] * 7,
        out_specs=(vmem, vmem),
        scratch_shapes=[
            pltpu.VMEM((FOUR, 72, R256), F32),
            pltpu.VMEM((FOUR, 80, R256), F32),
            pltpu.VMEM((80, R256), F32),
            pltpu.VMEM((C64, H8, R256), F32),
            pltpu.VMEM((C64, R256, L128), BF16),
            pltpu.VMEM((C64, C64), BF16),
            pltpu.VMEM((R256, C64), BF16),
            pltpu.VMEM((C64, R256), BF16),
            pltpu.VMEM((C64, C64), BF16),
            pltpu.VMEM((TWO, 1152, L128), F32),
            pltpu.VMEM((C64, C64, R256), BF16),
            pltpu.VMEM((O32, R256, L128), BF16),
            pltpu.VMEM((O32, R256, R256), BF16),
            pltpu.VMEM((R256, R256), BF16),
            pltpu.VMEM((L128, R256), F32),
            pltpu.VMEM((TWO, 2304, L128), F32),
            pltpu.VMEM((W2K, R256), BF16),
            pltpu.VMEM((C64, L128, R256), F32),
        ] + [pltpu.VMEM((H8, R256, R256), BF16)] * FOUR + [
            pltpu.VMEM((1280, L128), F32),
            pltpu.VMEM((FOUR, L128, R256), BF16),
            pltpu.VMEM((R256, R256), F32),
            pltpu.SemaphoreType.DMA(()),
            pltpu.SemaphoreType.DMA((9,)),
            pltpu.SemaphoreType.DMA((9,)),
            pltpu.SemaphoreType.DMA((21,)),
            pltpu.SemaphoreType.DMA((21,)),
        ],
        compiler_params=pltpu.CompilerParams(collective_id=1, has_side_effects=True, vmem_limit_bytes=TAIL_LIMIT),
    )(qs, kv, mask, e1, g1, pair, bcg, wco, wti, wto, wom, weight, bias)


def solution(mesh):
    row_spec = P(('batch', 'seq'))
    rep_spec = P()

    def local_block(msa, mask, pair, w_pair_bias, w_row_in, b_row_gate, w_row_out, w_col_in, b_col_gate, w_col_out, w_trans_in, w_trans_out, w_opm_in, w_opm_out, b_opm_out):
        pinned = [pltpu.with_memory_space_constraint(value, pltpu.HBM) for value in (
            jnp.swapaxes(msa, 1, TWO), pair, mask, w_pair_bias.T, w_row_in, b_row_gate.reshape(1, C64), w_row_out, w_col_in)]
        e1, g1, kv, qs = row_stage(*pinned)
        e3, pair_out = tail_stage(qs, kv, mask, e1, g1, pair, b_col_gate.reshape(1, C64), w_col_out, w_trans_in, w_trans_out.T, w_opm_in, w_opm_out.reshape(1024, L128), b_opm_out.reshape(1, L128))
        return jnp.swapaxes(e3, 1, TWO), pair_out

    return jax.shard_map(local_block, mesh=mesh, in_specs=(row_spec, row_spec, row_spec) + (rep_spec,) * 12, out_specs=(row_spec, row_spec), check_vma=False)
```

```python
import functools

import jax
import jax.numpy as jnp
from jax import lax
from jax.experimental import pallas as pl
from jax.experimental.pallas import tpu as pltpu
from jax.sharding import PartitionSpec as P

F32, BF16 = jnp.float32, jnp.bfloat16
MESH = pl.DeviceIdType.MESH
LOG2E = 1.4426950408889634
MASK_FILL = -1e9
R256 = 256
C64 = 64
L128 = 128
H8 = 8
W2K = 2048
T16 = 16
O32 = 32
TWO = 2
FOUR = 4
K144 = 144
ALL16K = 16384
THREE = 3
VMEM_LIMIT = 46000 * 1024
TAIL_LIMIT = 40000 * 1024


def dot(left, right):
    return jnp.dot(left, right, preferred_element_type=F32)


def dot_t(left, right):
    return lax.dot_general(left, right, (((1,), (1,)), ((), ())), preferred_element_type=F32)


def iota(shape, axis):
    return lax.broadcasted_iota(jnp.int32, shape, axis)


def norm_cols(values):
    centered = values - jnp.mean(values, axis=0, keepdims=True)
    variance = jnp.mean(centered * centered, axis=0, keepdims=True)
    return (centered * lax.rsqrt(variance + 1e-5)).astype(BF16)


def eye(size):
    return (iota((size, size), 0) == iota((size, size), 1)).astype(BF16)


def pick(rows, columns, index):
    return (index(iota((rows, columns), 0)) == iota((rows, columns), 1)).astype(BF16)


def swap8(row):
    return (row % H8) * H8 + row // H8


def column(row_vector, index, size):
    hit = index(iota((size, size), 0)) == iota((size, size), 1)
    wide = jnp.broadcast_to(row_vector.astype(F32), (size, size))
    return jnp.sum(jnp.where(hit, wide, 0.0), axis=1, keepdims=True)


def place():
    me = lax.axis_index('seq')
    batch = lax.axis_index('batch')
    mate = me + 1 - TWO * lax.rem(me, TWO)
    cross = lax.rem(me + TWO, FOUR)
    return me, batch, mate, cross


def meet(batch, peers):
    barrier = pltpu.get_barrier_semaphore()
    for peer in peers:
        pl.semaphore_signal(barrier, inc=1, device_id=(batch, peer), device_id_type=MESH)
    pl.semaphore_wait(barrier, len(peers))


def rows64(index):
    return pl.ds(pl.multiple_of(index * C64, C64), C64)


def row_kernel(e_hbm, z_hbm, mask_hbm, wpb_hbm, wri_hbm, brg_hbm, wro_hbm, wci_hbm,
               e1_ref, g1_ref, kv_ref, qs_ref,
               mask_ref, wpb_ref, wri_ref, brg_ref, wro_ref, wci_ref, small_sem, z_buf, e_buf, tmp, own, full, bias, q_s, k_s, v_s, g_s, x_s, rhs, att, w_big, w_ci,
               logit_0, top_0, logit_1, top_1, logit_2, top_2, logit_3, top_3, logit_4, top_4, logit_5, top_5, logit_6, top_6, logit_7, top_7, out_0, out_1, z_sem, e_sem, send_sem, recv_sem):
    logit_s = (logit_0, logit_1, logit_2, logit_3, logit_4, logit_5, logit_6, logit_7)
    top_s = (top_0, top_1, top_2, top_3, top_4, top_5, top_6, top_7)
    out_s = (out_0, out_1)
    me, batch, mate, cross = place()
    small = [pltpu.make_async_copy(src, dst, small_sem.at[n]) for n, (src, dst) in enumerate((
        (wpb_hbm, wpb_ref), (wri_hbm, wri_ref), (wci_hbm, wci_ref), (mask_hbm, mask_ref), (wro_hbm, wro_ref), (brg_hbm, brg_ref)))]
    small[0].start()
    for part in range(H8):
        pltpu.make_async_copy(z_hbm.at[pl.ds(part * H8, H8)], z_buf.at[pl.ds(part * H8, H8)], z_sem.at[part]).start()
    for copy in small[1:]:
        copy.start()
    for part in range(H8):
        pltpu.make_async_copy(e_hbm.at[pl.ds(part * H8, H8)], e_buf.at[pl.ds(part * H8, H8)], e_sem.at[part]).start()
    meet(batch, (mate, cross))

    def big_index(row):
        in_k, in_v = row - C64, row - 192
        head_k = C64 + (in_k // T16) * H8 + in_k % H8
        head_v = jnp.where(in_v % T16 < H8, L128 + (in_v // T16) * H8 + in_v % H8, -1)
        return jnp.where(row < C64, row, jnp.where(row < 192, head_k, jnp.where(row < 320, head_v, row - L128)))

    small[0].wait()
    w_pb = wpb_ref[...]
    rhs[...] = jnp.broadcast_to((iota((K144, R256), 0) == L128).astype(BF16)[None], (T16, K144, R256))

    def bias_part(part, carry):
        pltpu.make_async_copy(z_hbm.at[pl.ds(part * H8, H8)], z_buf.at[pl.ds(part * H8, H8)], z_sem.at[part]).wait()
        z_t = jnp.transpose(z_buf[pl.ds(part * H8, H8)].reshape(W2K, L128).astype(F32))
        heads = dot(w_pb, norm_cols(z_t))
        for t in range(H8):
            for lane in range(TWO):
                at = t * R256 + lane * L128
                tmp[lane, t * H8:(t + 1) * H8, :] = heads[:, at:at + L128]
        for h in range(H8):
            for lane in range(TWO):
                own[h, pl.ds(pl.multiple_of(part * H8, H8), H8), lane * L128:(lane + 1) * L128] = tmp[lane, pl.ds(h, H8, stride=H8), :]
        return carry

    def ship(view, slot, peer):
        return pltpu.make_async_remote_copy(
            src_ref=view, dst_ref=view, send_sem=send_sem.at[slot], recv_sem=recv_sem.at[slot],
            device_id=(batch, peer), device_id_type=MESH)

    def piece(n, slot, peer):
        rows = pl.ds(pl.multiple_of(me * C64 + n * T16, T16), T16)
        return ship(full.at[:, rows, :], slot + n, peer)

    def bias_piece(n, carry):
        lax.fori_loop(TWO * n, TWO * n + TWO, bias_part, 0)
        full[:, pl.ds(pl.multiple_of(me * C64 + n * T16, T16), T16), :] = own[:, pl.ds(pl.multiple_of(n * T16, T16), T16), :].astype(BF16)
        piece(n, 0, cross).start()
        piece(n, FOUR, mate).start()
        return carry

    lax.fori_loop(0, FOUR, bias_piece, 0)
    relay = ship(full.at[:, rows64(cross), :], H8, mate)

    for copy in small[1:]:
        copy.wait()
    w_big[...] = dot_t(pick(384, R256, big_index), wri_ref[...]).astype(BF16)
    w_ci[...] = dot_t(
        pick(K144, K144, lambda row: jnp.where(row < C64, swap8(row), jnp.where(row < L128, C64 + swap8(row - C64), row))),
        wci_ref[...]).astype(BF16)
    ones = ((iota((L128, W2K), 0) % T16) == H8).astype(F32)

    def project_part(part, carry):
        pltpu.make_async_copy(e_hbm.at[pl.ds(part * H8, H8)], e_buf.at[pl.ds(part * H8, H8)], e_sem.at[part]).wait()
        lanes = pl.ds(pl.multiple_of(part * W2K, W2K), W2K)
        x_raw = jnp.concatenate([e_buf[part * H8 + t] for t in range(H8)], axis=1)
        x_s[:, lanes] = x_raw
        x_t = x_raw.astype(F32)
        proj = dot(w_big[...], norm_cols(x_t))
        q_val = proj[0:C64].astype(BF16).astype(F32) * (H8 ** -0.5 * LOG2E)
        q_hi = q_val.astype(BF16).astype(F32)
        q_lo = q_val - q_hi
        for h in range(H8):
            pair = jnp.concatenate([q_hi[h * H8:h * H8 + H8], q_lo[h * H8:h * H8 + H8]], axis=0)
            q_s[h * T16:(h + 1) * T16, lanes] = pair.astype(BF16)
        keep = mask_ref[pl.ds(pl.multiple_of(part * H8, H8), H8), :].astype(F32)
        keep_row = jnp.concatenate([keep[t:t + 1] for t in range(H8)], axis=1)
        k_s[lanes, 0:L128] = jnp.transpose(proj[C64:192] * keep_row).astype(BF16)
        fill = jnp.where(iota((T16, W2K), 0) == 0, (1.0 - keep_row) * (MASK_FILL * LOG2E), 0.0)
        k_s[lanes, L128:K144] = jnp.transpose(fill).astype(BF16)
        v_s[:, lanes] = (proj[192:320] + ones).astype(BF16)
        g_s[:, lanes] = proj[320:384].astype(BF16)
        return carry

    lax.fori_loop(0, 6, project_part, 0)
    for n in range(FOUR):
        piece(n, 0, cross).wait_recv()
    relay.start()
    lax.fori_loop(6, H8, project_part, 0)
    for n in range(FOUR):
        piece(n, FOUR, mate).wait_recv()
    relay.wait_recv()
    for n in range(H8):
        piece(n % FOUR, n // FOUR * FOUR, mate).wait_send()
    relay.wait_send()
    for h in range(H8):
        bias[h] = jnp.transpose(full[h].astype(F32)) * LOG2E

    def at_seq(s):
        s = jnp.clip(s, 0, 63)
        return s, pl.ds(pl.multiple_of(s * R256, R256), R256)

    def load_q(p):
        for n in range(TWO):
            lanes = at_seq(TWO * p + n)[1]
            for h in range(H8):
                sub = slice(h * T16, (h + 1) * T16)
                rhs[n * H8 + h, sub, :] = q_s[sub, lanes]

    def score(p, h):
        slot = h % FOUR
        raw = [dot(k_s[at_seq(TWO * p + n)[1], :], rhs[n * H8 + h]) for n in range(TWO)]
        tops = [[], []]
        for at in range(0, R256, C64):
            shared = bias[h, at:at + C64, :]
            for n in range(TWO):
                logits = raw[n][at:at + C64] + shared
                logit_s[TWO * slot + n][at:at + C64, :] = logits
                tops[n].append(jnp.max(logits.reshape(C64 // H8, H8, R256), axis=0))
        for n in range(TWO):
            best = functools.reduce(jnp.maximum, tops[n])
            top_s[TWO * slot + n][...] = jnp.broadcast_to(jnp.max(best, axis=0, keepdims=True), (H8, R256))

    def soften(p, h):
        if h < 0:
            p, h = p - 1, h + H8
        slot = h % FOUR
        for n in range(TWO):
            v_blk = v_s[h * T16:(h + 1) * T16, at_seq(TWO * p + n)[1]]
            shifted = logit_s[TWO * slot + n][...].reshape(O32, H8, R256) - top_s[TWO * slot + n][...][None]
            out_s[n][h] = dot(v_blk, jnp.exp2(shifted).reshape(R256, R256).astype(BF16))

    def combine(p, h):
        for n in range(TWO):
            s, lanes = at_seq(TWO * p + n)
            some = jnp.max(mask_ref[pl.ds(s, 1), :].astype(F32), axis=1, keepdims=True) > 0.0
            values = v_s[h * T16:(h + 1) * T16, lanes].astype(F32)[0:H8]
            mean = jnp.sum(values, axis=1, keepdims=True) * (1.0 / 256.0)
            out = out_s[n][h]
            att[h * H8:(h + 1) * H8, lanes] = jnp.where(some, out[0:H8] * (1.0 / out[H8:9]), mean)

    load_q(0)

    def attend(t, carry):
        for step in range(THREE):
            p = THREE * t + step
            for h in range(H8):
                score(p, h)
                if h >= TWO:
                    combine(p - 1, h - TWO)
                soften(p, h - TWO)
                if h == TWO - 1:
                    for late in range(H8 - TWO, H8):
                        combine(p - 1, late)
            load_q(p + 1)
        return carry

    lax.fori_loop(0, 33 // THREE, attend, 0)

    w_ro = dot_t(eye(C64), wro_ref[...]).astype(BF16)
    gate_bias = column(brg_ref[...], lambda row: row, C64)
    qs_ref[0:C64, :] = jnp.zeros((C64, R256), F32)
    qs_ref[C64:72, :] = jnp.broadcast_to(jnp.sum(mask_ref[...].astype(F32), axis=0, keepdims=True), (H8, R256))

    def finish_part(part, carry):
        lanes = pl.ds(pl.multiple_of(part * W2K, W2K), W2K)
        gate = jax.nn.sigmoid(g_s[:, lanes].astype(F32) + gate_bias)
        gated = (gate * att[:, lanes]).astype(BF16)
        e_one = (x_s[:, lanes].astype(F32) + dot(w_ro, gated)).astype(BF16)
        e1_ref[:, lanes] = e_one
        proj = dot(w_ci[...], norm_cols(e_one.astype(F32))).astype(BF16)
        g1_ref[:, lanes] = proj[C64:L128]
        keep = mask_ref[pl.ds(pl.multiple_of(part * H8, H8), H8), :].astype(F32)
        q_sum = jnp.zeros((C64, R256), F32)
        for t in range(H8):
            cut = slice(t * R256, (t + 1) * R256)
            kv_ref[part * H8 + t] = proj[L128:K144, cut].astype(F32)
            q_sum += proj[0:C64, cut].astype(F32) * keep[t:t + 1]
        qs_ref[0:C64, :] += q_sum
        return carry

    lax.fori_loop(0, H8, finish_part, 0)


def row_stage(msa, pair, mask, wpb, wri, brg, wro, wci):
    hbm = pl.BlockSpec(memory_space=pltpu.HBM)
    vmem = pl.BlockSpec(memory_space=pltpu.VMEM)
    return pl.pallas_call(
        row_kernel,
        name='row_stage',
        out_shape=(
            jax.ShapeDtypeStruct((C64, ALL16K), BF16),
            jax.ShapeDtypeStruct((C64, ALL16K), BF16),
            jax.ShapeDtypeStruct((C64, T16, R256), F32),
            jax.ShapeDtypeStruct((72, R256), F32),
        ),
        in_specs=[hbm] * H8,
        out_specs=(vmem,) * FOUR,
        scratch_shapes=[
            pltpu.VMEM((C64, R256), jnp.int32),
            pltpu.VMEM((H8, L128), BF16),
            pltpu.VMEM((C64, R256), BF16),
            pltpu.VMEM((1, C64), BF16),
            pltpu.VMEM((C64, C64), BF16),
            pltpu.VMEM((C64, K144), BF16),
            pltpu.SemaphoreType.DMA((6,)),
            pltpu.VMEM((C64, R256, L128), BF16),
            pltpu.VMEM((C64, C64, R256), BF16),
            pltpu.VMEM((TWO, C64, L128), F32),
            pltpu.VMEM((H8, C64, R256), F32),
            pltpu.VMEM((H8, R256, R256), BF16),
            pltpu.VMEM((H8, R256, R256), F32),
            pltpu.VMEM((L128, ALL16K), BF16),
            pltpu.VMEM((ALL16K, K144), BF16),
            pltpu.VMEM((L128, ALL16K), BF16),
            pltpu.VMEM((C64, ALL16K), BF16),
            pltpu.VMEM((C64, ALL16K), BF16),
            pltpu.VMEM((T16, K144, R256), BF16),
            pltpu.VMEM((C64, ALL16K), F32),
            pltpu.VMEM((384, C64), BF16),
            pltpu.VMEM((K144, C64), BF16),
        ] + [pltpu.VMEM((R256, R256), F32), pltpu.VMEM((H8, R256), F32)] * H8 + [
            pltpu.VMEM((H8, T16, R256), F32),
            pltpu.VMEM((H8, T16, R256), F32),
            pltpu.SemaphoreType.DMA((H8,)),
            pltpu.SemaphoreType.DMA((H8,)),
            pltpu.SemaphoreType.DMA((9,)),
            pltpu.SemaphoreType.DMA((9,)),
        ],
        compiler_params=pltpu.CompilerParams(collective_id=0, has_side_effects=True, vmem_limit_bytes=VMEM_LIMIT),
    )(msa, pair, mask, wpb, wri, brg, wro, wci)


def tail_kernel(qs_ref, kv_ref, mask_ref, e_buf, g_buf, z_hbm, bcg_ref, wco_ref, wti_ref, wto_ref, wom_ref, w_ref, b_ref,
                e3_ref, out_ref,
                first, second, stat, logit_s, z_buf,
                w_co, w_ti, w_to, w_om, ab_s, ab,
                a_half, b_full, m_full, turn_s, a_tmp, a_s, acc, p_hi0, p_lo0, p_hi1, p_lo1, w_tmp, w_t, inv_s,
                load_sem, stat_send, stat_recv, send_sem, recv_sem):
    me, batch, mate, cross = place()
    z_load = pltpu.make_async_copy(z_hbm, z_buf, load_sem)
    z_load.start()
    meet(batch, (mate, cross))

    def pass_on(src, dst, slot, peer):
        copy = pltpu.make_async_remote_copy(
            src_ref=src, dst_ref=dst, send_sem=stat_send.at[slot], recv_sem=stat_recv.at[slot],
            device_id=(batch, peer), device_id_type=MESH)
        copy.start()
        return copy

    query_mate = pass_on(qs_ref, first.at[0], 0, mate)
    query_mate.wait_recv()
    first[1] = qs_ref[...] + first[0]
    query_cross = pass_on(first.at[1], first.at[TWO], 1, cross)
    m_full[rows64(me), :] = mask_ref[...].astype(F32).astype(BF16)
    m_view = m_full.at[rows64(me), :]
    mask_cross = pass_on(m_view, m_view, FOUR, cross)
    mask_mate = pass_on(m_view, m_view, 5, mate)

    w_co[...] = dot(dot_t(eye(C64), wco_ref[...]).astype(BF16),
                    (swap8(iota((C64, C64), 1)) == iota((C64, C64), 0)).astype(BF16)).astype(BF16)
    w_ti[...] = dot_t(eye(R256), wti_ref[...]).astype(BF16)
    w_to[...] = wto_ref[...]
    w_om[...] = dot_t(eye(C64), wom_ref[...]).astype(BF16)
    for c in range(O32):
        w_tmp[c * 40:c * 40 + O32, :] = w_ref[c * O32:(c + 1) * O32, :].astype(F32)
    for k in range(FOUR):
        for d in range(H8):
            w_t[k, :, d * O32:(d + 1) * O32] = jnp.transpose(w_tmp[pl.ds(k * H8 + d, O32, stride=40), :]).astype(BF16)

    query_cross.wait_recv()
    total = first[1] + first[TWO]
    population = total[C64:72] + 1e-10
    q_bar = [(total[d * H8:(d + 1) * H8] / population).astype(BF16).astype(F32) for d in range(H8)]

    def scores(s, top):
        kv = kv_ref[s]
        value = q_bar[0] * kv[0:1]
        for d in range(1, H8):
            value += q_bar[d] * kv[d:d + 1]
        value = jnp.where(mask_ref[pl.ds(s, 1), :] > 0, value * (H8 ** -0.5), MASK_FILL)
        logit_s[s] = value
        return jnp.maximum(top, value)

    top = lax.fori_loop(0, C64, scores, jnp.full((H8, R256), -3e38, F32), unroll=FOUR)

    def gather(s, sums):
        kv = kv_ref[s]
        weight = jnp.exp(logit_s[s] - top)
        return (sums[0] + weight,) + tuple(sums[d + 1] + weight * kv[H8 + d:9 + d] for d in range(H8))

    sums = lax.fori_loop(0, C64, gather, (jnp.zeros((H8, R256), F32),) * 9, unroll=FOUR)
    stat[0:H8, :] = top
    for n in range(9):
        stat[H8 + n * H8:T16 + n * H8, :] = sums[n]
    stat_mate = pass_on(stat, second.at[0], TWO, mate)

    def merge(left, right, dst):
        best = jnp.maximum(left[0:H8, :], right[0:H8, :])
        scale = [jnp.exp(side[0:H8, :] - best) for side in (left, right)]
        dst[0:H8, :] = best
        for at in range(H8, 80, H8):
            dst[at:at + H8, :] = left[at:at + H8, :] * scale[0] + right[at:at + H8, :] * scale[1]

    stat_mate.wait_recv()
    merge(stat, second.at[0], second.at[1])
    stat_cross = pass_on(second.at[1], second.at[TWO], THREE, cross)
    far_mask = m_full.at[rows64(cross), :]
    mask_cross.wait_recv()
    mask_relay = pass_on(far_mask, far_mask, 6, mate)
    stat_cross.wait_recv()
    merge(second.at[1], second.at[TWO], second.at[THREE])
    den = second[THREE, H8:T16, :]
    column_out = jnp.concatenate([second[THREE, T16 + d * H8:24 + d * H8, :] / den for d in range(H8)], axis=0)
    col = jnp.concatenate([column_out] * H8, axis=1)
    gate_bias = column(bcg_ref[...], swap8, C64)

    def send(src, dst, slot, peer):
        return pltpu.make_async_remote_copy(
            src_ref=src, dst_ref=dst, send_sem=send_sem.at[slot], recv_sem=recv_sem.at[slot],
            device_id=(batch, peer), device_id_type=MESH)

    def lanes_of(device):
        return pl.ds(pl.multiple_of((device // TWO) * L128, L128), L128)

    def rows16(device, block):
        return pl.ds(pl.multiple_of(device * C64 + block * T16, T16), T16)

    def b_piece(k, src_rows, dst_rows, slot, peer):
        return send(ab.at[pl.ds(O32 + k * H8, H8), src_rows, :], b_full.at[pl.ds(k * H8, H8), dst_rows, :], slot, peer)

    whole = pl.ds(0, C64)

    def a_cross(n):
        return send(ab.at[pl.ds(0, O32), rows16(0, n), lanes_of(cross)], a_half.at[:, rows16(me, n), :], n, cross)

    def first_cross(n):
        return b_piece(0, rows16(0, n), rows16(me, n), FOUR + n, cross)

    def late_cross(k):
        return b_piece(k, whole, rows64(me), 7 + k, cross)

    def b_mate(k):
        return b_piece(k, whole, rows64(me), 12 + k, mate)

    def b_relay(k):
        far_b = b_full.at[pl.ds(k * H8, H8), rows64(cross), :]
        return send(far_b, far_b, 17 + k, mate)

    a_mate = send(ab.at[pl.ds(0, O32), :, lanes_of(me)], a_half.at[:, rows64(me), :], 11, mate)
    far_a = a_half.at[:, rows64(cross), :]
    a_relay = send(far_a, far_a, T16, mate)


    def sixteen(block, done):
        def half(part, carry):
            where = block * TWO + part
            lanes = pl.ds(pl.multiple_of(where * W2K, W2K), W2K)
            gate = jax.nn.sigmoid(g_buf[:, lanes].astype(F32) + gate_bias)
            gated = (gate * col).astype(BF16)
            e_two = (e_buf[:, lanes].astype(F32) + dot(w_co[...], gated)).astype(BF16).astype(F32)
            hidden = jnp.maximum(dot(w_ti[...], norm_cols(e_two)), 0.0).astype(BF16)
            e_three = (e_two + dot(w_to[...], hidden)).astype(BF16).astype(F32)
            for t in range(H8):
                e3_ref[where * H8 + t] = e_three[:, t * R256:(t + 1) * R256].astype(BF16)
            proj = dot(w_om[...], norm_cols(e_three)).astype(BF16).astype(F32)
            keep = mask_ref[pl.ds(pl.multiple_of(where * H8, H8), H8), :].astype(F32)
            for t in range(H8):
                at = pl.ds(pl.multiple_of((part * H8 + t) * 72, H8), C64)
                for lane in range(TWO):
                    cut = slice(lane * L128, (lane + 1) * L128)
                    ab_s[lane, at, :] = proj[:, t * R256 + lane * L128:t * R256 + (lane + 1) * L128] * keep[t:t + 1, cut]
            return carry

        lax.fori_loop(0, TWO, half, 0)
        for f in range(C64):
            for lane in range(TWO):
                ab[f, rows16(0, block), lane * L128:(lane + 1) * L128] = (
                    ab_s[lane, pl.ds(f, T16, stride=72), :].astype(BF16))
        a_cross(block).start()
        first_cross(block).start()
        return done

    lax.fori_loop(0, FOUR, sixteen, 0)
    for k in range(1, FOUR):
        late_cross(k).start()
    a_mate.start()
    for k in range(FOUR):
        b_mate(k).start()

    a_half[:, rows64(me), :] = ab[0:O32, :, lanes_of(me)]
    b_full[:, rows64(me), :] = ab[O32:C64, :, :]
    mask_mate.wait_recv()
    mask_relay.wait_recv()
    keep_all = m_full[...]
    inv_s[...] = 1.0 / (dot(jnp.transpose(keep_all.astype(F32)).astype(BF16), keep_all) + 1e-3)
    z_load.wait()
    e_bias = b_ref[...].astype(F32)

    for n in range(FOUR):
        a_cross(n).wait_recv()
    a_relay.start()
    for n in range(FOUR):
        first_cross(n).wait_recv()
    b_relay(0).start()
    a_mate.wait_recv()
    a_relay.wait_recv()
    offset = pl.multiple_of(lax.rem(me, TWO) * C64, C64)

    def turn(c, carry):
        turn_s[...] = jnp.transpose(a_half[c].astype(F32))
        mine = turn_s[pl.ds(offset, C64), :]
        for lane in range(TWO):
            a_tmp[lane, pl.ds(pl.multiple_of(c * 72, H8), C64), :] = mine[:, lane * L128:(lane + 1) * L128]
        return carry

    lax.fori_loop(0, O32, turn, 0)
    for i in range(C64):
        for lane in range(TWO):
            a_s[i * O32:(i + 1) * O32, lane * L128:(lane + 1) * L128] = a_tmp[lane, pl.ds(i, O32, stride=72), :].astype(BF16)

    slots = ((p_hi0, p_lo0), (p_hi1, p_lo1))

    def outer(slot, index, d):
        p_hi, p_lo = slots[slot]
        k, n = index // H8, lax.rem(index, H8)
        value = dot(a_s[pl.ds(pl.multiple_of(n * R256, R256), R256), :], b_full[k * H8 + d])
        high = value.astype(BF16)
        low = (value - high.astype(F32)).astype(BF16)
        for i in range(H8):
            p_hi[i, d * O32:(d + 1) * O32, :] = high[i * O32:(i + 1) * O32]
            p_lo[i, d * O32:(d + 1) * O32, :] = low[i * O32:(i + 1) * O32]

    def project(slot, index, i):
        p_hi, p_lo = slots[slot]
        index = jnp.maximum(index, 0)
        k, at = index // H8, lax.rem(index, H8) * H8 + i
        part = dot(w_t[k], p_hi[i]) + dot(w_t[k], p_lo[i])
        acc[at] = jnp.where(k == 0, part, acc[at] + part)

    def settle(index, i):
        at = jnp.maximum(index - 24, 0) * H8 + i
        update = acc[at] * inv_s[pl.ds(me * C64 + at, 1), :]
        out_ref[at] = (z_buf[at].astype(F32) + jnp.transpose(update) + e_bias).astype(BF16)

    def pair(last, t, carry):
        k = t // FOUR

        @pl.when(lax.rem(t, FOUR) == 0)
        def _():
            b_mate(k).wait_recv()
            b_relay(k).wait_recv()

        if not last:
            @pl.when(lax.rem(t, FOUR) == THREE)
            def _():
                late_cross(k + 1).wait_recv()
                b_relay(k + 1).start()

        for slot in range(TWO):
            index = TWO * t + slot
            for n in range(H8):
                outer(slot, index, n)
                project(1 - slot, index - 1, n)
                if last:
                    settle(index - TWO, n)
        return carry

    lax.fori_loop(0, 12, functools.partial(pair, False), 0)
    lax.fori_loop(12, T16, functools.partial(pair, True), 0)
    for n in range(H8):
        project(1, 31, n)
        settle(30, n)
    for n in range(H8):
        settle(31, n)
    for copy in (query_mate, query_cross, stat_mate, stat_cross, mask_cross, mask_mate, mask_relay, a_mate, a_relay):
        copy.wait_send()
    for n in range(FOUR):
        a_cross(n).wait_send()
        first_cross(n).wait_send()
        b_mate(n).wait_send()
        b_relay(n).wait_send()
    for k in range(1, FOUR):
        late_cross(k).wait_send()


def tail_stage(qs, kv, mask, e1, g1, pair, bcg, wco, wti, wto, wom, weight, bias):
    any_spec = pl.BlockSpec(memory_space=pl.ANY)
    vmem = pl.BlockSpec(memory_space=pltpu.VMEM)
    return pl.pallas_call(
        tail_kernel,
        name='tail_stage',
        out_shape=(jax.ShapeDtypeStruct((C64, C64, R256), BF16), jax.ShapeDtypeStruct((C64, R256, L128), BF16)),
        in_specs=[vmem] * 5 + [any_spec] + [vmem] * 7,
        out_specs=(vmem, vmem),
        scratch_shapes=[
            pltpu.VMEM((THREE, 72, R256), F32),
            pltpu.VMEM((FOUR, 80, R256), F32),
            pltpu.VMEM((80, R256), F32),
            pltpu.VMEM((C64, H8, R256), F32),
            pltpu.VMEM((C64, R256, L128), BF16),
            pltpu.VMEM((C64, C64), BF16),
            pltpu.VMEM((R256, C64), BF16),
            pltpu.VMEM((C64, R256), BF16),
            pltpu.VMEM((C64, C64), BF16),
            pltpu.VMEM((TWO, 1152, L128), F32),
            pltpu.VMEM((C64, C64, R256), BF16),
            pltpu.VMEM((O32, R256, L128), BF16),
            pltpu.VMEM((O32, R256, R256), BF16),
            pltpu.VMEM((R256, R256), BF16),
            pltpu.VMEM((L128, R256), F32),
            pltpu.VMEM((TWO, 2304, L128), F32),
            pltpu.VMEM((W2K, R256), BF16),
            pltpu.VMEM((C64, L128, R256), F32),
        ] + [pltpu.VMEM((H8, R256, R256), BF16)] * FOUR + [
            pltpu.VMEM((1280, L128), F32),
            pltpu.VMEM((FOUR, L128, R256), BF16),
            pltpu.VMEM((R256, R256), F32),
            pltpu.SemaphoreType.DMA(()),
            pltpu.SemaphoreType.DMA((7,)),
            pltpu.SemaphoreType.DMA((7,)),
            pltpu.SemaphoreType.DMA((21,)),
            pltpu.SemaphoreType.DMA((21,)),
        ],
        compiler_params=pltpu.CompilerParams(collective_id=1, has_side_effects=True, vmem_limit_bytes=TAIL_LIMIT),
    )(qs, kv, mask, e1, g1, pair, bcg, wco, wti, wto, wom, weight, bias)


def solution(mesh):
    row_spec = P(('batch', 'seq'))
    rep_spec = P()

    def local_block(msa, mask, pair, w_pair_bias, w_row_in, b_row_gate, w_row_out, w_col_in, b_col_gate, w_col_out, w_trans_in, w_trans_out, w_opm_in, w_opm_out, b_opm_out):
        pinned = [pltpu.with_memory_space_constraint(value, pltpu.HBM) for value in (
            jnp.swapaxes(msa, 1, TWO), pair, mask, w_pair_bias.T, w_row_in, b_row_gate.reshape(1, C64), w_row_out, w_col_in)]
        e1, g1, kv, qs = row_stage(*pinned)
        e3, pair_out = tail_stage(qs, kv, mask, e1, g1, pair, b_col_gate.reshape(1, C64), w_col_out, w_trans_in, w_trans_out.T, w_opm_in, w_opm_out.reshape(1024, L128), b_opm_out.reshape(1, L128))
        return jnp.swapaxes(e3, 1, TWO), pair_out

    return jax.shard_map(local_block, mesh=mesh, in_specs=(row_spec, row_spec, row_spec) + (rep_spec,) * 12, out_specs=(row_spec, row_spec), check_vma=False)
```

```python
import functools

import jax
import jax.numpy as jnp
from jax import lax
from jax.experimental import pallas as pl
from jax.experimental.pallas import tpu as pltpu
from jax.sharding import PartitionSpec as P

F32, BF16 = jnp.float32, jnp.bfloat16
MESH = pl.DeviceIdType.MESH
LOG2E = 1.4426950408889634
MASK_FILL = -1e9
R256 = 256
C64 = 64
L128 = 128
H8 = 8
W2K = 2048
T16 = 16
O32 = 32
TWO = 2
FOUR = 4
K144 = 144
ALL16K = 16384
THREE = 3
VMEM_LIMIT = 46000 * 1024
TAIL_LIMIT = 40000 * 1024


def dot(left, right):
    return jnp.dot(left, right, preferred_element_type=F32)


def dot_t(left, right):
    return lax.dot_general(left, right, (((1,), (1,)), ((), ())), preferred_element_type=F32)


def iota(shape, axis):
    return lax.broadcasted_iota(jnp.int32, shape, axis)


def norm_cols(values):
    centered = values - jnp.mean(values, axis=0, keepdims=True)
    variance = jnp.mean(centered * centered, axis=0, keepdims=True)
    return (centered * lax.rsqrt(variance + 1e-5)).astype(BF16)


def eye(size):
    return (iota((size, size), 0) == iota((size, size), 1)).astype(BF16)


def pick(rows, columns, index):
    return (index(iota((rows, columns), 0)) == iota((rows, columns), 1)).astype(BF16)


def swap8(row):
    return (row % H8) * H8 + row // H8


def column(row_vector, index, size):
    hit = index(iota((size, size), 0)) == iota((size, size), 1)
    wide = jnp.broadcast_to(row_vector.astype(F32), (size, size))
    return jnp.sum(jnp.where(hit, wide, 0.0), axis=1, keepdims=True)


def place():
    me = lax.axis_index('seq')
    batch = lax.axis_index('batch')
    mate = me + 1 - TWO * lax.rem(me, TWO)
    cross = lax.rem(me + TWO, FOUR)
    return me, batch, mate, cross


def meet(batch, peers):
    barrier = pltpu.get_barrier_semaphore()
    for peer in peers:
        pl.semaphore_signal(barrier, inc=1, device_id=(batch, peer), device_id_type=MESH)
    pl.semaphore_wait(barrier, len(peers))


def rows64(index):
    return pl.ds(pl.multiple_of(index * C64, C64), C64)


def row_kernel(e_hbm, z_hbm, mask_hbm, wpb_hbm, wri_hbm, brg_hbm, wro_hbm, wci_hbm,
               e1_ref, g1_ref, kv_ref, qs_ref,
               mask_ref, wpb_ref, wri_ref, brg_ref, wro_ref, wci_ref, small_sem, z_buf, e_buf, tmp, own, full, bias, q_s, k_s, v_s, g_s, x_s, rhs, att, w_big, w_ci,
               logit_0, top_0, logit_1, top_1, logit_2, top_2, logit_3, top_3, logit_4, top_4, logit_5, top_5, logit_6, top_6, logit_7, top_7, out_0, out_1, z_sem, e_sem, send_sem, recv_sem):
    logit_s = (logit_0, logit_1, logit_2, logit_3, logit_4, logit_5, logit_6, logit_7)
    top_s = (top_0, top_1, top_2, top_3, top_4, top_5, top_6, top_7)
    out_s = (out_0, out_1)
    me, batch, mate, cross = place()
    small = [pltpu.make_async_copy(src, dst, small_sem.at[n]) for n, (src, dst) in enumerate((
        (wpb_hbm, wpb_ref), (wri_hbm, wri_ref), (wci_hbm, wci_ref), (mask_hbm, mask_ref), (wro_hbm, wro_ref), (brg_hbm, brg_ref)))]
    small[0].start()
    for part in range(H8):
        pltpu.make_async_copy(z_hbm.at[pl.ds(part * H8, H8)], z_buf.at[pl.ds(part * H8, H8)], z_sem.at[part]).start()
    for copy in small[1:]:
        copy.start()
    for part in range(H8):
        pltpu.make_async_copy(e_hbm.at[pl.ds(part * H8, H8)], e_buf.at[pl.ds(part * H8, H8)], e_sem.at[part]).start()
    meet(batch, (mate, cross))

    def big_index(row):
        in_k, in_v = row - C64, row - 192
        head_k = C64 + (in_k // T16) * H8 + in_k % H8
        head_v = jnp.where(in_v % T16 < H8, L128 + (in_v // T16) * H8 + in_v % H8, -1)
        return jnp.where(row < C64, row, jnp.where(row < 192, head_k, jnp.where(row < 320, head_v, row - L128)))

    small[0].wait()
    w_pb = wpb_ref[...]
    rhs[...] = jnp.broadcast_to((iota((K144, R256), 0) == L128).astype(BF16)[None], (T16, K144, R256))

    def bias_part(part, carry):
        pltpu.make_async_copy(z_hbm.at[pl.ds(part * H8, H8)], z_buf.at[pl.ds(part * H8, H8)], z_sem.at[part]).wait()
        z_t = jnp.transpose(z_buf[pl.ds(part * H8, H8)].reshape(W2K, L128).astype(F32))
        heads = dot(w_pb, norm_cols(z_t))
        for t in range(H8):
            for lane in range(TWO):
                at = t * R256 + lane * L128
                tmp[lane, t * H8:(t + 1) * H8, :] = heads[:, at:at + L128]
        for h in range(H8):
            for lane in range(TWO):
                own[h, pl.ds(pl.multiple_of(part * H8, H8), H8), lane * L128:(lane + 1) * L128] = tmp[lane, pl.ds(h, H8, stride=H8), :]
        return carry

    def ship(view, slot, peer):
        return pltpu.make_async_remote_copy(
            src_ref=view, dst_ref=view, send_sem=send_sem.at[slot], recv_sem=recv_sem.at[slot],
            device_id=(batch, peer), device_id_type=MESH)

    def piece(n, slot, peer):
        rows = pl.ds(pl.multiple_of(me * C64 + n * T16, T16), T16)
        return ship(full.at[:, rows, :], slot + n, peer)

    def bias_piece(n, carry):
        lax.fori_loop(TWO * n, TWO * n + TWO, bias_part, 0)
        full[:, pl.ds(pl.multiple_of(me * C64 + n * T16, T16), T16), :] = own[:, pl.ds(pl.multiple_of(n * T16, T16), T16), :].astype(BF16)
        piece(n, 0, cross).start()
        piece(n, FOUR, mate).start()
        return carry

    lax.fori_loop(0, FOUR, bias_piece, 0)
    relay = ship(full.at[:, rows64(cross), :], H8, mate)

    for copy in small[1:]:
        copy.wait()
    w_big[...] = dot_t(pick(384, R256, big_index), wri_ref[...]).astype(BF16)
    w_ci[...] = dot_t(
        pick(K144, K144, lambda row: jnp.where(row < C64, swap8(row), jnp.where(row < L128, C64 + swap8(row - C64), row))),
        wci_ref[...]).astype(BF16)
    ones = ((iota((L128, W2K), 0) % T16) == H8).astype(F32)

    def project_part(part, carry):
        pltpu.make_async_copy(e_hbm.at[pl.ds(part * H8, H8)], e_buf.at[pl.ds(part * H8, H8)], e_sem.at[part]).wait()
        lanes = pl.ds(pl.multiple_of(part * W2K, W2K), W2K)
        x_raw = jnp.concatenate([e_buf[part * H8 + t] for t in range(H8)], axis=1)
        x_s[:, lanes] = x_raw
        x_t = x_raw.astype(F32)
        proj = dot(w_big[...], norm_cols(x_t))
        q_val = proj[0:C64].astype(BF16).astype(F32) * (H8 ** -0.5 * LOG2E)
        q_hi = q_val.astype(BF16).astype(F32)
        q_lo = q_val - q_hi
        for h in range(H8):
            pair = jnp.concatenate([q_hi[h * H8:h * H8 + H8], q_lo[h * H8:h * H8 + H8]], axis=0)
            q_s[h * T16:(h + 1) * T16, lanes] = pair.astype(BF16)
        keep = mask_ref[pl.ds(pl.multiple_of(part * H8, H8), H8), :].astype(F32)
        keep_row = jnp.concatenate([keep[t:t + 1] for t in range(H8)], axis=1)
        k_s[lanes, 0:L128] = jnp.transpose(proj[C64:192] * keep_row).astype(BF16)
        fill = jnp.where(iota((T16, W2K), 0) == 0, (1.0 - keep_row) * (MASK_FILL * LOG2E), 0.0)
        k_s[lanes, L128:K144] = jnp.transpose(fill).astype(BF16)
        v_s[:, lanes] = (proj[192:320] + ones).astype(BF16)
        g_s[:, lanes] = proj[320:384].astype(BF16)
        return carry

    lax.fori_loop(0, 6, project_part, 0)
    for n in range(FOUR):
        piece(n, 0, cross).wait_recv()
    relay.start()
    lax.fori_loop(6, H8, project_part, 0)
    for n in range(FOUR):
        piece(n, FOUR, mate).wait_recv()
    relay.wait_recv()
    for n in range(H8):
        piece(n % FOUR, n // FOUR * FOUR, mate).wait_send()
    relay.wait_send()
    for h in range(H8):
        bias[h] = jnp.transpose(full[h].astype(F32)) * LOG2E

    def at_seq(s):
        s = jnp.clip(s, 0, 63)
        return s, pl.ds(pl.multiple_of(s * R256, R256), R256)

    def load_q(p):
        for n in range(TWO):
            lanes = at_seq(TWO * p + n)[1]
            for h in range(H8):
                sub = slice(h * T16, (h + 1) * T16)
                rhs[n * H8 + h, sub, :] = q_s[sub, lanes]

    def score(p, h):
        slot = h % FOUR
        raw = [dot(k_s[at_seq(TWO * p + n)[1], :], rhs[n * H8 + h]) for n in range(TWO)]
        tops = [[], []]
        for at in range(0, R256, C64):
            shared = bias[h, at:at + C64, :]
            for n in range(TWO):
                logits = raw[n][at:at + C64] + shared
                logit_s[TWO * slot + n][at:at + C64, :] = logits
                tops[n].append(jnp.max(logits.reshape(C64 // H8, H8, R256), axis=0))
        for n in range(TWO):
            best = functools.reduce(jnp.maximum, tops[n])
            top_s[TWO * slot + n][...] = jnp.broadcast_to(jnp.max(best, axis=0, keepdims=True), (H8, R256))

    def soften(p, h):
        if h < 0:
            p, h = p - 1, h + H8
        slot = h % FOUR
        for n in range(TWO):
            v_blk = v_s[h * T16:(h + 1) * T16, at_seq(TWO * p + n)[1]]
            shifted = logit_s[TWO * slot + n][...].reshape(O32, H8, R256) - top_s[TWO * slot + n][...][None]
            out_s[n][h] = dot(v_blk, jnp.exp2(shifted).reshape(R256, R256).astype(BF16))

    def combine(p, h):
        for n in range(TWO):
            s, lanes = at_seq(TWO * p + n)
            some = jnp.max(mask_ref[pl.ds(s, 1), :].astype(F32), axis=1, keepdims=True) > 0.0
            values = v_s[h * T16:(h + 1) * T16, lanes].astype(F32)[0:H8]
            mean = jnp.sum(values, axis=1, keepdims=True) * (1.0 / 256.0)
            out = out_s[n][h]
            att[h * H8:(h + 1) * H8, lanes] = jnp.where(some, out[0:H8] * (1.0 / out[H8:9]), mean)

    load_q(0)

    def attend(t, carry):
        for step in range(THREE):
            p = THREE * t + step
            for h in range(H8):
                score(p, h)
                if h >= TWO:
                    combine(p - 1, h - TWO)
                soften(p, h - TWO)
                if h == TWO - 1:
                    for late in range(H8 - TWO, H8):
                        combine(p - 1, late)
            load_q(p + 1)
        return carry

    lax.fori_loop(0, 33 // THREE, attend, 0)

    w_ro = dot_t(eye(C64), wro_ref[...]).astype(BF16)
    gate_bias = column(brg_ref[...], lambda row: row, C64)
    qs_ref[0:C64, :] = jnp.zeros((C64, R256), F32)
    qs_ref[C64:72, :] = jnp.broadcast_to(jnp.sum(mask_ref[...].astype(F32), axis=0, keepdims=True), (H8, R256))

    def finish_part(part, carry):
        lanes = pl.ds(pl.multiple_of(part * W2K, W2K), W2K)
        gate = jax.nn.sigmoid(g_s[:, lanes].astype(F32) + gate_bias)
        gated = (gate * att[:, lanes]).astype(BF16)
        e_one = (x_s[:, lanes].astype(F32) + dot(w_ro, gated)).astype(BF16)
        e1_ref[:, lanes] = e_one
        proj = dot(w_ci[...], norm_cols(e_one.astype(F32))).astype(BF16)
        g1_ref[:, lanes] = proj[C64:L128]
        keep = mask_ref[pl.ds(pl.multiple_of(part * H8, H8), H8), :].astype(F32)
        q_sum = jnp.zeros((C64, R256), F32)
        for t in range(H8):
            cut = slice(t * R256, (t + 1) * R256)
            kv_ref[part * H8 + t] = proj[L128:K144, cut].astype(F32)
            q_sum += proj[0:C64, cut].astype(F32) * keep[t:t + 1]
        qs_ref[0:C64, :] += q_sum
        return carry

    lax.fori_loop(0, H8, finish_part, 0)


def row_stage(msa, pair, mask, wpb, wri, brg, wro, wci):
    hbm = pl.BlockSpec(memory_space=pltpu.HBM)
    vmem = pl.BlockSpec(memory_space=pltpu.VMEM)
    return pl.pallas_call(
        row_kernel,
        name='row_stage',
        out_shape=(
            jax.ShapeDtypeStruct((C64, ALL16K), BF16),
            jax.ShapeDtypeStruct((C64, ALL16K), BF16),
            jax.ShapeDtypeStruct((C64, T16, R256), F32),
            jax.ShapeDtypeStruct((72, R256), F32),
        ),
        in_specs=[hbm] * H8,
        out_specs=(vmem,) * FOUR,
        scratch_shapes=[
            pltpu.VMEM((C64, R256), jnp.int32),
            pltpu.VMEM((H8, L128), BF16),
            pltpu.VMEM((C64, R256), BF16),
            pltpu.VMEM((1, C64), BF16),
            pltpu.VMEM((C64, C64), BF16),
            pltpu.VMEM((C64, K144), BF16),
            pltpu.SemaphoreType.DMA((6,)),
            pltpu.VMEM((C64, R256, L128), BF16),
            pltpu.VMEM((C64, C64, R256), BF16),
            pltpu.VMEM((TWO, C64, L128), F32),
            pltpu.VMEM((H8, C64, R256), F32),
            pltpu.VMEM((H8, R256, R256), BF16),
            pltpu.VMEM((H8, R256, R256), F32),
            pltpu.VMEM((L128, ALL16K), BF16),
            pltpu.VMEM((ALL16K, K144), BF16),
            pltpu.VMEM((L128, ALL16K), BF16),
            pltpu.VMEM((C64, ALL16K), BF16),
            pltpu.VMEM((C64, ALL16K), BF16),
            pltpu.VMEM((T16, K144, R256), BF16),
            pltpu.VMEM((C64, ALL16K), F32),
            pltpu.VMEM((384, C64), BF16),
            pltpu.VMEM((K144, C64), BF16),
        ] + [pltpu.VMEM((R256, R256), F32), pltpu.VMEM((H8, R256), F32)] * H8 + [
            pltpu.VMEM((H8, T16, R256), F32),
            pltpu.VMEM((H8, T16, R256), F32),
            pltpu.SemaphoreType.DMA((H8,)),
            pltpu.SemaphoreType.DMA((H8,)),
            pltpu.SemaphoreType.DMA((9,)),
            pltpu.SemaphoreType.DMA((9,)),
        ],
        compiler_params=pltpu.CompilerParams(collective_id=0, has_side_effects=True, vmem_limit_bytes=VMEM_LIMIT),
    )(msa, pair, mask, wpb, wri, brg, wro, wci)


def tail_kernel(qs_ref, kv_ref, mask_ref, e_buf, g_buf, z_hbm, bcg_ref, wco_ref, wti_ref, wto_ref, wom_ref, w_ref, b_ref,
                e3_ref, out_ref,
                first, second, stat, logit_s, z_buf,
                w_co, w_ti, w_to, w_om, ab_s, ab,
                a_half, b_full, m_full, turn_s, a_tmp, a_s, acc, p_hi0, p_lo0, p_hi1, p_lo1, w_tmp, w_t, inv_s,
                load_sem, stat_send, stat_recv, send_sem, recv_sem):
    me, batch, mate, cross = place()
    z_load = pltpu.make_async_copy(z_hbm, z_buf, load_sem)
    z_load.start()
    meet(batch, (mate, cross))

    def pass_on(src, dst, slot, peer):
        copy = pltpu.make_async_remote_copy(
            src_ref=src, dst_ref=dst, send_sem=stat_send.at[slot], recv_sem=stat_recv.at[slot],
            device_id=(batch, peer), device_id_type=MESH)
        copy.start()
        return copy

    query_mate = pass_on(qs_ref, first.at[0], 0, mate)
    query_mate.wait_recv()
    first[1] = qs_ref[...] + first[0]
    query_cross = pass_on(first.at[1], first.at[TWO], 1, cross)
    m_full[rows64(me), :] = mask_ref[...].astype(F32).astype(BF16)
    m_view = m_full.at[rows64(me), :]
    mask_cross = pass_on(m_view, m_view, FOUR, cross)
    mask_mate = pass_on(m_view, m_view, 5, mate)

    w_co[...] = dot(dot_t(eye(C64), wco_ref[...]).astype(BF16),
                    (swap8(iota((C64, C64), 1)) == iota((C64, C64), 0)).astype(BF16)).astype(BF16)
    w_ti[...] = dot_t(eye(R256), wti_ref[...]).astype(BF16)
    w_to[...] = wto_ref[...]
    w_om[...] = dot_t(eye(C64), wom_ref[...]).astype(BF16)
    for c in range(O32):
        w_tmp[c * 40:c * 40 + O32, :] = w_ref[c * O32:(c + 1) * O32, :].astype(F32)
    for k in range(FOUR):
        for d in range(H8):
            w_t[k, :, d * O32:(d + 1) * O32] = jnp.transpose(w_tmp[pl.ds(k * H8 + d, O32, stride=40), :]).astype(BF16)

    query_cross.wait_recv()
    total = first[1] + first[TWO]
    population = total[C64:72] + 1e-10
    q_bar = [(total[d * H8:(d + 1) * H8] / population).astype(BF16).astype(F32) for d in range(H8)]

    def scores(s, top):
        kv = kv_ref[s]
        value = q_bar[0] * kv[0:1]
        for d in range(1, H8):
            value += q_bar[d] * kv[d:d + 1]
        value = jnp.where(mask_ref[pl.ds(s, 1), :] > 0, value * (H8 ** -0.5), MASK_FILL)
        logit_s[s] = value
        return jnp.maximum(top, value)

    top = lax.fori_loop(0, C64, scores, jnp.full((H8, R256), -3e38, F32), unroll=FOUR)

    def gather(s, sums):
        kv = kv_ref[s]
        weight = jnp.exp(logit_s[s] - top)
        return (sums[0] + weight,) + tuple(sums[d + 1] + weight * kv[H8 + d:9 + d] for d in range(H8))

    sums = lax.fori_loop(0, C64, gather, (jnp.zeros((H8, R256), F32),) * 9, unroll=FOUR)
    stat[0:H8, :] = top
    for n in range(9):
        stat[H8 + n * H8:T16 + n * H8, :] = sums[n]
    stat_mate = pass_on(stat, second.at[0], TWO, mate)

    def merge(left, right, dst):
        best = jnp.maximum(left[0:H8, :], right[0:H8, :])
        scale = [jnp.exp(side[0:H8, :] - best) for side in (left, right)]
        dst[0:H8, :] = best
        for at in range(H8, 80, H8):
            dst[at:at + H8, :] = left[at:at + H8, :] * scale[0] + right[at:at + H8, :] * scale[1]

    stat_mate.wait_recv()
    merge(stat, second.at[0], second.at[1])
    stat_cross = pass_on(second.at[1], second.at[TWO], THREE, cross)
    far_mask = m_full.at[rows64(cross), :]
    mask_cross.wait_recv()
    mask_relay = pass_on(far_mask, far_mask, 6, mate)
    stat_cross.wait_recv()
    merge(second.at[1], second.at[TWO], second.at[THREE])
    den = second[THREE, H8:T16, :]
    column_out = jnp.concatenate([second[THREE, T16 + d * H8:24 + d * H8, :] / den for d in range(H8)], axis=0)
    col = jnp.concatenate([column_out] * H8, axis=1)
    gate_bias = column(bcg_ref[...], swap8, C64)

    def send(src, dst, slot, peer):
        return pltpu.make_async_remote_copy(
            src_ref=src, dst_ref=dst, send_sem=send_sem.at[slot], recv_sem=recv_sem.at[slot],
            device_id=(batch, peer), device_id_type=MESH)

    def lanes_of(device):
        return pl.ds(pl.multiple_of((device // TWO) * L128, L128), L128)

    def rows16(device, block):
        return pl.ds(pl.multiple_of(device * C64 + block * T16, T16), T16)

    def b_piece(k, src_rows, dst_rows, slot, peer):
        return send(ab.at[pl.ds(O32 + k * H8, H8), src_rows, :], b_full.at[pl.ds(k * H8, H8), dst_rows, :], slot, peer)

    whole = pl.ds(0, C64)

    def a_cross(n):
        return send(ab.at[pl.ds(0, O32), rows16(0, n), lanes_of(cross)], a_half.at[:, rows16(me, n), :], n, cross)

    def late_cross(k):
        return b_piece(k, whole, rows64(me), FOUR + k, cross)

    def b_mate(k):
        return b_piece(k, whole, rows64(me), H8 + k, mate)

    def b_relay(k):
        far_b = b_full.at[pl.ds(k * H8, H8), rows64(cross), :]
        return send(far_b, far_b, 12 + k, mate)

    a_mate = send(ab.at[pl.ds(0, O32), :, lanes_of(me)], a_half.at[:, rows64(me), :], T16, mate)
    far_a = a_half.at[:, rows64(cross), :]
    a_relay = send(far_a, far_a, 17, mate)


    def sixteen(block, done):
        def half(part, carry):
            where = block * TWO + part
            lanes = pl.ds(pl.multiple_of(where * W2K, W2K), W2K)
            gate = jax.nn.sigmoid(g_buf[:, lanes].astype(F32) + gate_bias)
            gated = (gate * col).astype(BF16)
            e_two = (e_buf[:, lanes].astype(F32) + dot(w_co[...], gated)).astype(BF16).astype(F32)
            hidden = jnp.maximum(dot(w_ti[...], norm_cols(e_two)), 0.0).astype(BF16)
            e_three = (e_two + dot(w_to[...], hidden)).astype(BF16).astype(F32)
            for t in range(H8):
                e3_ref[where * H8 + t] = e_three[:, t * R256:(t + 1) * R256].astype(BF16)
            proj = dot(w_om[...], norm_cols(e_three)).astype(BF16).astype(F32)
            keep = mask_ref[pl.ds(pl.multiple_of(where * H8, H8), H8), :].astype(F32)
            for t in range(H8):
                at = pl.ds(pl.multiple_of((part * H8 + t) * 72, H8), C64)
                for lane in range(TWO):
                    cut = slice(lane * L128, (lane + 1) * L128)
                    ab_s[lane, at, :] = proj[:, t * R256 + lane * L128:t * R256 + (lane + 1) * L128] * keep[t:t + 1, cut]
            return carry

        lax.fori_loop(0, TWO, half, 0)
        for f in range(C64):
            for lane in range(TWO):
                ab[f, rows16(0, block), lane * L128:(lane + 1) * L128] = (
                    ab_s[lane, pl.ds(f, T16, stride=72), :].astype(BF16))
        a_cross(block).start()
        return done

    lax.fori_loop(0, FOUR, sixteen, 0)
    a_mate.start()
    for k in range(FOUR):
        late_cross(k).start()
        b_mate(k).start()

    a_half[:, rows64(me), :] = ab[0:O32, :, lanes_of(me)]
    b_full[:, rows64(me), :] = ab[O32:C64, :, :]
    mask_mate.wait_recv()
    mask_relay.wait_recv()
    keep_all = m_full[...]
    inv_s[...] = 1.0 / (dot(jnp.transpose(keep_all.astype(F32)).astype(BF16), keep_all) + 1e-3)
    z_load.wait()
    e_bias = b_ref[...].astype(F32)

    for n in range(FOUR):
        a_cross(n).wait_recv()
    a_relay.start()
    a_mate.wait_recv()
    a_relay.wait_recv()
    offset = pl.multiple_of(lax.rem(me, TWO) * C64, C64)

    def turn(c, carry):
        turn_s[...] = jnp.transpose(a_half[c].astype(F32))
        mine = turn_s[pl.ds(offset, C64), :]
        for lane in range(TWO):
            a_tmp[lane, pl.ds(pl.multiple_of(c * 72, H8), C64), :] = mine[:, lane * L128:(lane + 1) * L128]
        return carry

    lax.fori_loop(0, O32, turn, 0)
    for i in range(C64):
        for lane in range(TWO):
            a_s[i * O32:(i + 1) * O32, lane * L128:(lane + 1) * L128] = a_tmp[lane, pl.ds(i, O32, stride=72), :].astype(BF16)

    late_cross(0).wait_recv()
    b_relay(0).start()
    slots = ((p_hi0, p_lo0), (p_hi1, p_lo1))

    def outer(slot, index, d):
        p_hi, p_lo = slots[slot]
        k, n = index // H8, lax.rem(index, H8)
        value = dot(a_s[pl.ds(pl.multiple_of(n * R256, R256), R256), :], b_full[k * H8 + d])
        high = value.astype(BF16)
        low = (value - high.astype(F32)).astype(BF16)
        for i in range(H8):
            p_hi[i, d * O32:(d + 1) * O32, :] = high[i * O32:(i + 1) * O32]
            p_lo[i, d * O32:(d + 1) * O32, :] = low[i * O32:(i + 1) * O32]

    def project(slot, index, i):
        p_hi, p_lo = slots[slot]
        index = jnp.maximum(index, 0)
        k, at = index // H8, lax.rem(index, H8) * H8 + i
        part = dot(w_t[k], p_hi[i]) + dot(w_t[k], p_lo[i])
        acc[at] = jnp.where(k == 0, part, acc[at] + part)

    def settle(index, i):
        at = jnp.maximum(index - 24, 0) * H8 + i
        update = acc[at] * inv_s[pl.ds(me * C64 + at, 1), :]
        out_ref[at] = (z_buf[at].astype(F32) + jnp.transpose(update) + e_bias).astype(BF16)

    def pair(last, t, carry):
        k = t // FOUR

        @pl.when(lax.rem(t, FOUR) == 0)
        def _():
            b_mate(k).wait_recv()
            b_relay(k).wait_recv()

        if not last:
            @pl.when(lax.rem(t, FOUR) == TWO)
            def _():
                late_cross(k + 1).wait_recv()
                b_relay(k + 1).start()

        for slot in range(TWO):
            index = TWO * t + slot
            for n in range(H8):
                outer(slot, index, n)
                project(1 - slot, index - 1, n)
                if last:
                    settle(index - TWO, n)
        return carry

    lax.fori_loop(0, 12, functools.partial(pair, False), 0)
    lax.fori_loop(12, T16, functools.partial(pair, True), 0)
    for n in range(H8):
        project(1, 31, n)
        settle(30, n)
    for n in range(H8):
        settle(31, n)
    for copy in (query_mate, query_cross, stat_mate, stat_cross, mask_cross, mask_mate, mask_relay, a_mate, a_relay):
        copy.wait_send()
    for n in range(FOUR):
        a_cross(n).wait_send()
        late_cross(n).wait_send()
        b_mate(n).wait_send()
        b_relay(n).wait_send()


def tail_stage(qs, kv, mask, e1, g1, pair, bcg, wco, wti, wto, wom, weight, bias):
    any_spec = pl.BlockSpec(memory_space=pl.ANY)
    vmem = pl.BlockSpec(memory_space=pltpu.VMEM)
    return pl.pallas_call(
        tail_kernel,
        name='tail_stage',
        out_shape=(jax.ShapeDtypeStruct((C64, C64, R256), BF16), jax.ShapeDtypeStruct((C64, R256, L128), BF16)),
        in_specs=[vmem] * 5 + [any_spec] + [vmem] * 7,
        out_specs=(vmem, vmem),
        scratch_shapes=[
            pltpu.VMEM((THREE, 72, R256), F32),
            pltpu.VMEM((FOUR, 80, R256), F32),
            pltpu.VMEM((80, R256), F32),
            pltpu.VMEM((C64, H8, R256), F32),
            pltpu.VMEM((C64, R256, L128), BF16),
            pltpu.VMEM((C64, C64), BF16),
            pltpu.VMEM((R256, C64), BF16),
            pltpu.VMEM((C64, R256), BF16),
            pltpu.VMEM((C64, C64), BF16),
            pltpu.VMEM((TWO, 1152, L128), F32),
            pltpu.VMEM((C64, C64, R256), BF16),
            pltpu.VMEM((O32, R256, L128), BF16),
            pltpu.VMEM((O32, R256, R256), BF16),
            pltpu.VMEM((R256, R256), BF16),
            pltpu.VMEM((L128, R256), F32),
            pltpu.VMEM((TWO, 2304, L128), F32),
            pltpu.VMEM((W2K, R256), BF16),
            pltpu.VMEM((C64, L128, R256), F32),
        ] + [pltpu.VMEM((H8, R256, R256), BF16)] * FOUR + [
            pltpu.VMEM((1280, L128), F32),
            pltpu.VMEM((FOUR, L128, R256), BF16),
            pltpu.VMEM((R256, R256), F32),
            pltpu.SemaphoreType.DMA(()),
            pltpu.SemaphoreType.DMA((7,)),
            pltpu.SemaphoreType.DMA((7,)),
            pltpu.SemaphoreType.DMA((18,)),
            pltpu.SemaphoreType.DMA((18,)),
        ],
        compiler_params=pltpu.CompilerParams(collective_id=1, has_side_effects=True, vmem_limit_bytes=TAIL_LIMIT),
    )(qs, kv, mask, e1, g1, pair, bcg, wco, wti, wto, wom, weight, bias)


def solution(mesh):
    row_spec = P(('batch', 'seq'))
    rep_spec = P()

    def local_block(msa, mask, pair, w_pair_bias, w_row_in, b_row_gate, w_row_out, w_col_in, b_col_gate, w_col_out, w_trans_in, w_trans_out, w_opm_in, w_opm_out, b_opm_out):
        pinned = [pltpu.with_memory_space_constraint(value, pltpu.HBM) for value in (
            jnp.swapaxes(msa, 1, TWO), pair, mask, w_pair_bias.T, w_row_in, b_row_gate.reshape(1, C64), w_row_out, w_col_in)]
        e1, g1, kv, qs = row_stage(*pinned)
        e3, pair_out = tail_stage(qs, kv, mask, e1, g1, pair, b_col_gate.reshape(1, C64), w_col_out, w_trans_in, w_trans_out.T, w_opm_in, w_opm_out.reshape(1024, L128), b_opm_out.reshape(1, L128))
        return jnp.swapaxes(e3, 1, TWO), pair_out

    return jax.shard_map(local_block, mesh=mesh, in_specs=(row_spec, row_spec, row_spec) + (rep_spec,) * 12, out_specs=(row_spec, row_spec), check_vma=False)
```

```python
import functools

import jax
import jax.numpy as jnp
from jax import lax
from jax.experimental import pallas as pl
from jax.experimental.pallas import tpu as pltpu
from jax.sharding import PartitionSpec as P

F32, BF16 = jnp.float32, jnp.bfloat16
MESH = pl.DeviceIdType.MESH
LOG2E = 1.4426950408889634
MASK_FILL = -1e9
R256 = 256
C64 = 64
L128 = 128
H8 = 8
W2K = 2048
T16 = 16
O32 = 32
TWO = 2
FOUR = 4
K144 = 144
ALL16K = 16384
THREE = 3
VMEM_LIMIT = 46000 * 1024
TAIL_LIMIT = 40000 * 1024


def dot(left, right):
    return jnp.dot(left, right, preferred_element_type=F32)


def dot_t(left, right):
    return lax.dot_general(left, right, (((1,), (1,)), ((), ())), preferred_element_type=F32)


def iota(shape, axis):
    return lax.broadcasted_iota(jnp.int32, shape, axis)


def norm_cols(values):
    centered = values - jnp.mean(values, axis=0, keepdims=True)
    variance = jnp.mean(centered * centered, axis=0, keepdims=True)
    return (centered * lax.rsqrt(variance + 1e-5)).astype(BF16)


def eye(size):
    return (iota((size, size), 0) == iota((size, size), 1)).astype(BF16)


def pick(rows, columns, index):
    return (index(iota((rows, columns), 0)) == iota((rows, columns), 1)).astype(BF16)


def swap8(row):
    return (row % H8) * H8 + row // H8


def column(row_vector, index, size):
    hit = index(iota((size, size), 0)) == iota((size, size), 1)
    wide = jnp.broadcast_to(row_vector.astype(F32), (size, size))
    return jnp.sum(jnp.where(hit, wide, 0.0), axis=1, keepdims=True)


def place():
    me = lax.axis_index('seq')
    batch = lax.axis_index('batch')
    mate = me + 1 - TWO * lax.rem(me, TWO)
    cross = lax.rem(me + TWO, FOUR)
    return me, batch, mate, cross


def meet(batch, peers):
    barrier = pltpu.get_barrier_semaphore()
    for peer in peers:
        pl.semaphore_signal(barrier, inc=1, device_id=(batch, peer), device_id_type=MESH)
    pl.semaphore_wait(barrier, len(peers))


def rows64(index):
    return pl.ds(pl.multiple_of(index * C64, C64), C64)


def row_kernel(e_hbm, z_hbm, mask_hbm, wpb_hbm, wri_hbm, brg_hbm, wro_hbm, wci_hbm,
               e1_ref, g1_ref, kv_ref, qs_ref,
               mask_ref, wpb_ref, wri_ref, brg_ref, wro_ref, wci_ref, small_sem, z_buf, e_buf, tmp, own, full, bias, q_s, k_s, v_s, g_s, x_s, rhs, att, w_big, w_ci,
               logit_0, top_0, logit_1, top_1, logit_2, top_2, logit_3, top_3, logit_4, top_4, logit_5, top_5, logit_6, top_6, logit_7, top_7, out_0, out_1, z_sem, e_sem, send_sem, recv_sem):
    logit_s = (logit_0, logit_1, logit_2, logit_3, logit_4, logit_5, logit_6, logit_7)
    top_s = (top_0, top_1, top_2, top_3, top_4, top_5, top_6, top_7)
    out_s = (out_0, out_1)
    me, batch, mate, cross = place()
    small = [pltpu.make_async_copy(src, dst, small_sem.at[n]) for n, (src, dst) in enumerate((
        (wpb_hbm, wpb_ref), (wri_hbm, wri_ref), (wci_hbm, wci_ref), (mask_hbm, mask_ref), (wro_hbm, wro_ref), (brg_hbm, brg_ref)))]
    small[0].start()
    for part in range(H8):
        pltpu.make_async_copy(z_hbm.at[pl.ds(part * H8, H8)], z_buf.at[pl.ds(part * H8, H8)], z_sem.at[part]).start()
    for copy in small[1:]:
        copy.start()
    for part in range(H8):
        pltpu.make_async_copy(e_hbm.at[pl.ds(part * H8, H8)], e_buf.at[pl.ds(part * H8, H8)], e_sem.at[part]).start()
    meet(batch, (mate, cross))

    def big_index(row):
        in_k, in_v = row - C64, row - 192
        head_k = C64 + (in_k // T16) * H8 + in_k % H8
        head_v = jnp.where(in_v % T16 < H8, L128 + (in_v // T16) * H8 + in_v % H8, -1)
        return jnp.where(row < C64, row, jnp.where(row < 192, head_k, jnp.where(row < 320, head_v, row - L128)))

    small[0].wait()
    w_pb = wpb_ref[...]
    rhs[...] = jnp.broadcast_to((iota((K144, R256), 0) == L128).astype(BF16)[None], (T16, K144, R256))

    def bias_part(part, carry):
        pltpu.make_async_copy(z_hbm.at[pl.ds(part * H8, H8)], z_buf.at[pl.ds(part * H8, H8)], z_sem.at[part]).wait()
        z_t = jnp.transpose(z_buf[pl.ds(part * H8, H8)].reshape(W2K, L128).astype(F32))
        heads = dot(w_pb, norm_cols(z_t))
        for t in range(H8):
            for lane in range(TWO):
                at = t * R256 + lane * L128
                tmp[lane, t * H8:(t + 1) * H8, :] = heads[:, at:at + L128]
        for h in range(H8):
            for lane in range(TWO):
                own[h, pl.ds(pl.multiple_of(part * H8, H8), H8), lane * L128:(lane + 1) * L128] = tmp[lane, pl.ds(h, H8, stride=H8), :]
        return carry

    def ship(view, slot, peer):
        return pltpu.make_async_remote_copy(
            src_ref=view, dst_ref=view, send_sem=send_sem.at[slot], recv_sem=recv_sem.at[slot],
            device_id=(batch, peer), device_id_type=MESH)

    def piece(n, slot, peer):
        rows = pl.ds(pl.multiple_of(me * C64 + n * T16, T16), T16)
        return ship(full.at[:, rows, :], slot + n, peer)

    def bias_piece(n, carry):
        lax.fori_loop(TWO * n, TWO * n + TWO, bias_part, 0)
        full[:, pl.ds(pl.multiple_of(me * C64 + n * T16, T16), T16), :] = own[:, pl.ds(pl.multiple_of(n * T16, T16), T16), :].astype(BF16)
        piece(n, 0, cross).start()
        piece(n, FOUR, mate).start()
        return carry

    lax.fori_loop(0, FOUR, bias_piece, 0)
    relay = ship(full.at[:, rows64(cross), :], H8, mate)

    for copy in small[1:]:
        copy.wait()
    w_big[...] = dot_t(pick(384, R256, big_index), wri_ref[...]).astype(BF16)
    w_ci[...] = dot_t(
        pick(K144, K144, lambda row: jnp.where(row < C64, swap8(row), jnp.where(row < L128, C64 + swap8(row - C64), row))),
        wci_ref[...]).astype(BF16)
    ones = ((iota((L128, W2K), 0) % T16) == H8).astype(F32)

    def project_part(part, carry):
        pltpu.make_async_copy(e_hbm.at[pl.ds(part * H8, H8)], e_buf.at[pl.ds(part * H8, H8)], e_sem.at[part]).wait()
        lanes = pl.ds(pl.multiple_of(part * W2K, W2K), W2K)
        x_raw = jnp.concatenate([e_buf[part * H8 + t] for t in range(H8)], axis=1)
        x_s[:, lanes] = x_raw
        x_t = x_raw.astype(F32)
        proj = dot(w_big[...], norm_cols(x_t))
        q_val = proj[0:C64].astype(BF16).astype(F32) * (H8 ** -0.5 * LOG2E)
        q_hi = q_val.astype(BF16).astype(F32)
        q_lo = q_val - q_hi
        for h in range(H8):
            pair = jnp.concatenate([q_hi[h * H8:h * H8 + H8], q_lo[h * H8:h * H8 + H8]], axis=0)
            q_s[h * T16:(h + 1) * T16, lanes] = pair.astype(BF16)
        keep = mask_ref[pl.ds(pl.multiple_of(part * H8, H8), H8), :].astype(F32)
        keep_row = jnp.concatenate([keep[t:t + 1] for t in range(H8)], axis=1)
        k_s[lanes, 0:L128] = jnp.transpose(proj[C64:192] * keep_row).astype(BF16)
        fill = jnp.where(iota((T16, W2K), 0) == 0, (1.0 - keep_row) * (MASK_FILL * LOG2E), 0.0)
        k_s[lanes, L128:K144] = jnp.transpose(fill).astype(BF16)
        v_s[:, lanes] = (proj[192:320] + ones).astype(BF16)
        g_s[:, lanes] = proj[320:384].astype(BF16)
        return carry

    lax.fori_loop(0, 6, project_part, 0)
    for n in range(FOUR):
        piece(n, 0, cross).wait_recv()
    relay.start()
    lax.fori_loop(6, H8, project_part, 0)
    for n in range(FOUR):
        piece(n, FOUR, mate).wait_recv()
    relay.wait_recv()
    for n in range(H8):
        piece(n % FOUR, n // FOUR * FOUR, mate).wait_send()
    relay.wait_send()
    for h in range(H8):
        bias[h] = jnp.transpose(full[h].astype(F32)) * LOG2E

    def at_seq(s):
        s = jnp.clip(s, 0, 63)
        return s, pl.ds(pl.multiple_of(s * R256, R256), R256)

    def load_q(p):
        for n in range(TWO):
            lanes = at_seq(TWO * p + n)[1]
            for h in range(H8):
                sub = slice(h * T16, (h + 1) * T16)
                rhs[n * H8 + h, sub, :] = q_s[sub, lanes]

    def score(p, h):
        slot = h % FOUR
        raw = [dot(k_s[at_seq(TWO * p + n)[1], :], rhs[n * H8 + h]) for n in range(TWO)]
        tops = [[], []]
        for at in range(0, R256, C64):
            shared = bias[h, at:at + C64, :]
            for n in range(TWO):
                logits = raw[n][at:at + C64] + shared
                logit_s[TWO * slot + n][at:at + C64, :] = logits
                tops[n].append(jnp.max(logits.reshape(C64 // H8, H8, R256), axis=0))
        for n in range(TWO):
            best = functools.reduce(jnp.maximum, tops[n])
            top_s[TWO * slot + n][...] = jnp.broadcast_to(jnp.max(best, axis=0, keepdims=True), (H8, R256))

    def soften(p, h):
        if h < 0:
            p, h = p - 1, h + H8
        slot = h % FOUR
        for n in range(TWO):
            v_blk = v_s[h * T16:(h + 1) * T16, at_seq(TWO * p + n)[1]]
            shifted = logit_s[TWO * slot + n][...].reshape(O32, H8, R256) - top_s[TWO * slot + n][...][None]
            out_s[n][h] = dot(v_blk, jnp.exp2(shifted).reshape(R256, R256).astype(BF16))

    def combine(p, h):
        for n in range(TWO):
            s, lanes = at_seq(TWO * p + n)
            some = jnp.max(mask_ref[pl.ds(s, 1), :].astype(F32), axis=1, keepdims=True) > 0.0
            values = v_s[h * T16:(h + 1) * T16, lanes].astype(F32)[0:H8]
            mean = jnp.sum(values, axis=1, keepdims=True) * (1.0 / 256.0)
            out = out_s[n][h]
            att[h * H8:(h + 1) * H8, lanes] = jnp.where(some, out[0:H8] * (1.0 / out[H8:9]), mean)

    load_q(0)

    def attend(t, carry):
        for step in range(THREE):
            p = THREE * t + step
            for h in range(H8):
                score(p, h)
                if h >= TWO:
                    combine(p - 1, h - TWO)
                soften(p, h - TWO)
                if h == TWO - 1:
                    for late in range(H8 - TWO, H8):
                        combine(p - 1, late)
            load_q(p + 1)
        return carry

    lax.fori_loop(0, 33 // THREE, attend, 0)

    w_ro = dot_t(eye(C64), wro_ref[...]).astype(BF16)
    gate_bias = column(brg_ref[...], lambda row: row, C64)
    qs_ref[0:C64, :] = jnp.zeros((C64, R256), F32)
    qs_ref[C64:72, :] = jnp.broadcast_to(jnp.sum(mask_ref[...].astype(F32), axis=0, keepdims=True), (H8, R256))

    def finish_part(part, carry):
        lanes = pl.ds(pl.multiple_of(part * W2K, W2K), W2K)
        gate = jax.nn.sigmoid(g_s[:, lanes].astype(F32) + gate_bias)
        gated = (gate * att[:, lanes]).astype(BF16)
        e_one = (x_s[:, lanes].astype(F32) + dot(w_ro, gated)).astype(BF16)
        e1_ref[:, lanes] = e_one
        proj = dot(w_ci[...], norm_cols(e_one.astype(F32))).astype(BF16)
        g1_ref[:, lanes] = proj[C64:L128]
        keep = mask_ref[pl.ds(pl.multiple_of(part * H8, H8), H8), :].astype(F32)
        q_sum = jnp.zeros((C64, R256), F32)
        for t in range(H8):
            cut = slice(t * R256, (t + 1) * R256)
            kv_ref[part * H8 + t] = proj[L128:K144, cut].astype(F32)
            q_sum += proj[0:C64, cut].astype(F32) * keep[t:t + 1]
        qs_ref[0:C64, :] += q_sum
        return carry

    lax.fori_loop(0, H8, finish_part, 0)


def row_stage(msa, pair, mask, wpb, wri, brg, wro, wci):
    hbm = pl.BlockSpec(memory_space=pltpu.HBM)
    vmem = pl.BlockSpec(memory_space=pltpu.VMEM)
    return pl.pallas_call(
        row_kernel,
        name='row_stage',
        out_shape=(
            jax.ShapeDtypeStruct((C64, ALL16K), BF16),
            jax.ShapeDtypeStruct((C64, ALL16K), BF16),
            jax.ShapeDtypeStruct((C64, T16, R256), F32),
            jax.ShapeDtypeStruct((72, R256), F32),
        ),
        in_specs=[hbm] * H8,
        out_specs=(vmem,) * FOUR,
        scratch_shapes=[
            pltpu.VMEM((C64, R256), jnp.int32),
            pltpu.VMEM((H8, L128), BF16),
            pltpu.VMEM((C64, R256), BF16),
            pltpu.VMEM((1, C64), BF16),
            pltpu.VMEM((C64, C64), BF16),
            pltpu.VMEM((C64, K144), BF16),
            pltpu.SemaphoreType.DMA((6,)),
            pltpu.VMEM((C64, R256, L128), BF16),
            pltpu.VMEM((C64, C64, R256), BF16),
            pltpu.VMEM((TWO, C64, L128), F32),
            pltpu.VMEM((H8, C64, R256), F32),
            pltpu.VMEM((H8, R256, R256), BF16),
            pltpu.VMEM((H8, R256, R256), F32),
            pltpu.VMEM((L128, ALL16K), BF16),
            pltpu.VMEM((ALL16K, K144), BF16),
            pltpu.VMEM((L128, ALL16K), BF16),
            pltpu.VMEM((C64, ALL16K), BF16),
            pltpu.VMEM((C64, ALL16K), BF16),
            pltpu.VMEM((T16, K144, R256), BF16),
            pltpu.VMEM((C64, ALL16K), F32),
            pltpu.VMEM((384, C64), BF16),
            pltpu.VMEM((K144, C64), BF16),
        ] + [pltpu.VMEM((R256, R256), F32), pltpu.VMEM((H8, R256), F32)] * H8 + [
            pltpu.VMEM((H8, T16, R256), F32),
            pltpu.VMEM((H8, T16, R256), F32),
            pltpu.SemaphoreType.DMA((H8,)),
            pltpu.SemaphoreType.DMA((H8,)),
            pltpu.SemaphoreType.DMA((9,)),
            pltpu.SemaphoreType.DMA((9,)),
        ],
        compiler_params=pltpu.CompilerParams(collective_id=0, has_side_effects=True, vmem_limit_bytes=VMEM_LIMIT),
    )(msa, pair, mask, wpb, wri, brg, wro, wci)


def tail_kernel(qs_ref, kv_ref, mask_ref, e_buf, g_buf, z_hbm, bcg_ref, wco_ref, wti_ref, wto_ref, wom_ref, w_ref, b_ref,
                e3_ref, out_ref,
                first, second, stat, logit_s, z_buf,
                w_co, w_ti, w_to, w_om, ab_s, ab,
                a_half, b_full, m_full, turn_s, a_tmp, a_s, acc, p_hi0, p_lo0, p_hi1, p_lo1, w_tmp, w_t, inv_s,
                load_sem, stat_send, stat_recv, send_sem, recv_sem):
    me, batch, mate, cross = place()
    z_load = pltpu.make_async_copy(z_hbm, z_buf, load_sem)
    z_load.start()
    meet(batch, (mate, cross))

    def pass_on(src, dst, slot, peer):
        copy = pltpu.make_async_remote_copy(
            src_ref=src, dst_ref=dst, send_sem=stat_send.at[slot], recv_sem=stat_recv.at[slot],
            device_id=(batch, peer), device_id_type=MESH)
        copy.start()
        return copy

    query_mate = pass_on(qs_ref, first.at[0], 0, mate)
    query_mate.wait_recv()
    first[1] = qs_ref[...] + first[0]
    query_cross = pass_on(first.at[1], first.at[TWO], 1, cross)
    m_full[rows64(me), :] = mask_ref[...].astype(F32).astype(BF16)
    m_view = m_full.at[rows64(me), :]
    mask_cross = pass_on(m_view, m_view, FOUR, cross)
    mask_mate = pass_on(m_view, m_view, 5, mate)

    w_co[...] = dot(dot_t(eye(C64), wco_ref[...]).astype(BF16),
                    (swap8(iota((C64, C64), 1)) == iota((C64, C64), 0)).astype(BF16)).astype(BF16)
    w_ti[...] = dot_t(eye(R256), wti_ref[...]).astype(BF16)
    w_to[...] = wto_ref[...]
    w_om[...] = dot_t(eye(C64), wom_ref[...]).astype(BF16)
    for c in range(O32):
        w_tmp[c * 40:c * 40 + O32, :] = w_ref[c * O32:(c + 1) * O32, :].astype(F32)
    for k in range(FOUR):
        for d in range(H8):
            w_t[k, :, d * O32:(d + 1) * O32] = jnp.transpose(w_tmp[pl.ds(k * H8 + d, O32, stride=40), :]).astype(BF16)

    query_cross.wait_recv()
    total = first[1] + first[TWO]
    population = total[C64:72] + 1e-10
    q_bar = [(total[d * H8:(d + 1) * H8] / population).astype(BF16).astype(F32) for d in range(H8)]

    def scores(s, top):
        kv = kv_ref[s]
        value = q_bar[0] * kv[0:1]
        for d in range(1, H8):
            value += q_bar[d] * kv[d:d + 1]
        value = jnp.where(mask_ref[pl.ds(s, 1), :] > 0, value * (H8 ** -0.5), MASK_FILL)
        logit_s[s] = value
        return jnp.maximum(top, value)

    top = lax.fori_loop(0, C64, scores, jnp.full((H8, R256), -3e38, F32), unroll=FOUR)

    def gather(s, sums):
        kv = kv_ref[s]
        weight = jnp.exp(logit_s[s] - top)
        return (sums[0] + weight,) + tuple(sums[d + 1] + weight * kv[H8 + d:9 + d] for d in range(H8))

    sums = lax.fori_loop(0, C64, gather, (jnp.zeros((H8, R256), F32),) * 9, unroll=FOUR)
    stat[0:H8, :] = top
    for n in range(9):
        stat[H8 + n * H8:T16 + n * H8, :] = sums[n]
    stat_mate = pass_on(stat, second.at[0], TWO, mate)

    def merge(left, right, dst):
        best = jnp.maximum(left[0:H8, :], right[0:H8, :])
        scale = [jnp.exp(side[0:H8, :] - best) for side in (left, right)]
        dst[0:H8, :] = best
        for at in range(H8, 80, H8):
            dst[at:at + H8, :] = left[at:at + H8, :] * scale[0] + right[at:at + H8, :] * scale[1]

    stat_mate.wait_recv()
    merge(stat, second.at[0], second.at[1])
    stat_cross = pass_on(second.at[1], second.at[TWO], THREE, cross)
    far_mask = m_full.at[rows64(cross), :]
    mask_cross.wait_recv()
    mask_relay = pass_on(far_mask, far_mask, 6, mate)
    stat_cross.wait_recv()
    merge(second.at[1], second.at[TWO], second.at[THREE])
    den = second[THREE, H8:T16, :]
    column_out = jnp.concatenate([second[THREE, T16 + d * H8:24 + d * H8, :] / den for d in range(H8)], axis=0)
    col = jnp.concatenate([column_out] * H8, axis=1)
    gate_bias = column(bcg_ref[...], swap8, C64)

    def send(src, dst, slot, peer):
        return pltpu.make_async_remote_copy(
            src_ref=src, dst_ref=dst, send_sem=send_sem.at[slot], recv_sem=recv_sem.at[slot],
            device_id=(batch, peer), device_id_type=MESH)

    def lanes_of(device):
        return pl.ds(pl.multiple_of((device // TWO) * L128, L128), L128)

    def rows16(device, block):
        return pl.ds(pl.multiple_of(device * C64 + block * T16, T16), T16)

    def b_piece(k, src_rows, dst_rows, slot, peer):
        return send(ab.at[pl.ds(O32 + k * H8, H8), src_rows, :], b_full.at[pl.ds(k * H8, H8), dst_rows, :], slot, peer)

    whole = pl.ds(0, C64)

    def a_cross(n):
        return send(ab.at[pl.ds(0, O32), rows16(0, n), lanes_of(cross)], a_half.at[:, rows16(me, n), :], n, cross)

    def late_cross(k):
        return b_piece(k, whole, rows64(me), FOUR + k, cross)

    def b_mate(k):
        return b_piece(k, whole, rows64(me), H8 + k, mate)

    def b_relay(k):
        far_b = b_full.at[pl.ds(k * H8, H8), rows64(cross), :]
        return send(far_b, far_b, 12 + k, mate)

    a_mate = send(ab.at[pl.ds(0, O32), :, lanes_of(me)], a_half.at[:, rows64(me), :], T16, mate)
    far_a = a_half.at[:, rows64(cross), :]
    a_relay = send(far_a, far_a, 17, mate)


    def sixteen(block, done):
        def half(part, carry):
            where = block * TWO + part
            lanes = pl.ds(pl.multiple_of(where * W2K, W2K), W2K)
            gate = jax.nn.sigmoid(g_buf[:, lanes].astype(F32) + gate_bias)
            gated = (gate * col).astype(BF16)
            e_two = (e_buf[:, lanes].astype(F32) + dot(w_co[...], gated)).astype(BF16).astype(F32)
            hidden = jnp.maximum(dot(w_ti[...], norm_cols(e_two)), 0.0).astype(BF16)
            e_three = (e_two + dot(w_to[...], hidden)).astype(BF16).astype(F32)
            for t in range(H8):
                e3_ref[where * H8 + t] = e_three[:, t * R256:(t + 1) * R256].astype(BF16)
            proj = dot(w_om[...], norm_cols(e_three)).astype(BF16).astype(F32)
            keep = mask_ref[pl.ds(pl.multiple_of(where * H8, H8), H8), :].astype(F32)
            for t in range(H8):
                at = pl.ds(pl.multiple_of((part * H8 + t) * 72, H8), C64)
                for lane in range(TWO):
                    cut = slice(lane * L128, (lane + 1) * L128)
                    ab_s[lane, at, :] = proj[:, t * R256 + lane * L128:t * R256 + (lane + 1) * L128] * keep[t:t + 1, cut]
            return carry

        lax.fori_loop(0, TWO, half, 0)
        for f in range(C64):
            for lane in range(TWO):
                ab[f, rows16(0, block), lane * L128:(lane + 1) * L128] = (
                    ab_s[lane, pl.ds(f, T16, stride=72), :].astype(BF16))
        a_cross(block).start()
        return done

    lax.fori_loop(0, FOUR, sixteen, 0)
    a_mate.start()
    for k in range(FOUR):
        late_cross(k).start()
        b_mate(k).start()

    a_half[:, rows64(me), :] = ab[0:O32, :, lanes_of(me)]
    b_full[:, rows64(me), :] = ab[O32:C64, :, :]
    mask_mate.wait_recv()
    mask_relay.wait_recv()
    keep_all = m_full[...]
    inv_s[...] = 1.0 / (dot(jnp.transpose(keep_all.astype(F32)).astype(BF16), keep_all) + 1e-3)
    z_load.wait()
    e_bias = b_ref[...].astype(F32)

    for n in range(FOUR):
        a_cross(n).wait_recv()
    a_relay.start()
    a_mate.wait_recv()
    a_relay.wait_recv()
    offset = pl.multiple_of(lax.rem(me, TWO) * C64, C64)

    def turn(c, carry):
        turn_s[...] = jnp.transpose(a_half[c].astype(F32))
        mine = turn_s[pl.ds(offset, C64), :]
        for lane in range(TWO):
            a_tmp[lane, pl.ds(pl.multiple_of(c * 72, H8), C64), :] = mine[:, lane * L128:(lane + 1) * L128]
        return carry

    lax.fori_loop(0, O32, turn, 0)
    for i in range(C64):
        for lane in range(TWO):
            a_s[i * O32:(i + 1) * O32, lane * L128:(lane + 1) * L128] = a_tmp[lane, pl.ds(i, O32, stride=72), :].astype(BF16)

    late_cross(0).wait_recv()
    b_relay(0).start()
    slots = ((p_hi0, p_lo0), (p_hi1, p_lo1))

    def outer(slot, index, d):
        p_hi, p_lo = slots[slot]
        k, n = index // H8, lax.rem(index, H8)
        value = dot(a_s[pl.ds(pl.multiple_of(n * R256, R256), R256), :], b_full[k * H8 + d])
        high = value.astype(BF16)
        low = (value - high.astype(F32)).astype(BF16)
        for i in range(H8):
            p_hi[i, d * O32:(d + 1) * O32, :] = high[i * O32:(i + 1) * O32]
            p_lo[i, d * O32:(d + 1) * O32, :] = low[i * O32:(i + 1) * O32]

    def project(slot, index, i):
        p_hi, p_lo = slots[slot]
        index = jnp.maximum(index, 0)
        k, at = index // H8, lax.rem(index, H8) * H8 + i
        part = dot(w_t[k], p_hi[i]) + dot(w_t[k], p_lo[i])
        acc[at] = jnp.where(k == 0, part, acc[at] + part)

    def settle(index, i):
        at = jnp.maximum(index - 24, 0) * H8 + i
        update = acc[at] * inv_s[pl.ds(me * C64 + at, 1), :]
        out_ref[at] = (z_buf[at].astype(F32) + jnp.transpose(update) + e_bias).astype(BF16)

    def pair(last, t, carry):
        k = t // TWO

        @pl.when(lax.rem(t, TWO) == 0)
        def _():
            b_mate(k).wait_recv()
            b_relay(k).wait_recv()

        if not last:
            @pl.when(lax.rem(t, TWO) == 1)
            def _():
                late_cross(k + 1).wait_recv()
                b_relay(k + 1).start()

        for step in range(FOUR):
            index, slot = FOUR * t + step, step % TWO
            for n in range(H8):
                outer(slot, index, n)
                project(1 - slot, index - 1, n)
                if last:
                    settle(index - TWO, n)
        return carry

    lax.fori_loop(0, 6, functools.partial(pair, False), 0)
    lax.fori_loop(6, H8, functools.partial(pair, True), 0)
    for n in range(H8):
        project(1, 31, n)
        settle(30, n)
    for n in range(H8):
        settle(31, n)
    for copy in (query_mate, query_cross, stat_mate, stat_cross, mask_cross, mask_mate, mask_relay, a_mate, a_relay):
        copy.wait_send()
    for n in range(FOUR):
        a_cross(n).wait_send()
        late_cross(n).wait_send()
        b_mate(n).wait_send()
        b_relay(n).wait_send()


def tail_stage(qs, kv, mask, e1, g1, pair, bcg, wco, wti, wto, wom, weight, bias):
    any_spec = pl.BlockSpec(memory_space=pl.ANY)
    vmem = pl.BlockSpec(memory_space=pltpu.VMEM)
    return pl.pallas_call(
        tail_kernel,
        name='tail_stage',
        out_shape=(jax.ShapeDtypeStruct((C64, C64, R256), BF16), jax.ShapeDtypeStruct((C64, R256, L128), BF16)),
        in_specs=[vmem] * 5 + [any_spec] + [vmem] * 7,
        out_specs=(vmem, vmem),
        scratch_shapes=[
            pltpu.VMEM((THREE, 72, R256), F32),
            pltpu.VMEM((FOUR, 80, R256), F32),
            pltpu.VMEM((80, R256), F32),
            pltpu.VMEM((C64, H8, R256), F32),
            pltpu.VMEM((C64, R256, L128), BF16),
            pltpu.VMEM((C64, C64), BF16),
            pltpu.VMEM((R256, C64), BF16),
            pltpu.VMEM((C64, R256), BF16),
            pltpu.VMEM((C64, C64), BF16),
            pltpu.VMEM((TWO, 1152, L128), F32),
            pltpu.VMEM((C64, C64, R256), BF16),
            pltpu.VMEM((O32, R256, L128), BF16),
            pltpu.VMEM((O32, R256, R256), BF16),
            pltpu.VMEM((R256, R256), BF16),
            pltpu.VMEM((L128, R256), F32),
            pltpu.VMEM((TWO, 2304, L128), F32),
            pltpu.VMEM((W2K, R256), BF16),
            pltpu.VMEM((C64, L128, R256), F32),
        ] + [pltpu.VMEM((H8, R256, R256), BF16)] * FOUR + [
            pltpu.VMEM((1280, L128), F32),
            pltpu.VMEM((FOUR, L128, R256), BF16),
            pltpu.VMEM((R256, R256), F32),
            pltpu.SemaphoreType.DMA(()),
            pltpu.SemaphoreType.DMA((7,)),
            pltpu.SemaphoreType.DMA((7,)),
            pltpu.SemaphoreType.DMA((18,)),
            pltpu.SemaphoreType.DMA((18,)),
        ],
        compiler_params=pltpu.CompilerParams(collective_id=1, has_side_effects=True, vmem_limit_bytes=TAIL_LIMIT),
    )(qs, kv, mask, e1, g1, pair, bcg, wco, wti, wto, wom, weight, bias)


def solution(mesh):
    row_spec = P(('batch', 'seq'))
    rep_spec = P()

    def local_block(msa, mask, pair, w_pair_bias, w_row_in, b_row_gate, w_row_out, w_col_in, b_col_gate, w_col_out, w_trans_in, w_trans_out, w_opm_in, w_opm_out, b_opm_out):
        pinned = [pltpu.with_memory_space_constraint(value, pltpu.HBM) for value in (
            jnp.swapaxes(msa, 1, TWO), pair, mask, w_pair_bias.T, w_row_in, b_row_gate.reshape(1, C64), w_row_out, w_col_in)]
        e1, g1, kv, qs = row_stage(*pinned)
        e3, pair_out = tail_stage(qs, kv, mask, e1, g1, pair, b_col_gate.reshape(1, C64), w_col_out, w_trans_in, w_trans_out.T, w_opm_in, w_opm_out.reshape(1024, L128), b_opm_out.reshape(1, L128))
        return jnp.swapaxes(e3, 1, TWO), pair_out

    return jax.shard_map(local_block, mesh=mesh, in_specs=(row_spec, row_spec, row_spec) + (rep_spec,) * 12, out_specs=(row_spec, row_spec), check_vma=False)
```

```python
import functools

import jax
import jax.numpy as jnp
from jax import lax
from jax.experimental import pallas as pl
from jax.experimental.pallas import tpu as pltpu
from jax.sharding import PartitionSpec as P

F32, BF16 = jnp.float32, jnp.bfloat16
MESH = pl.DeviceIdType.MESH
LOG2E = 1.4426950408889634
MASK_FILL = -1e9
R256 = 256
C64 = 64
L128 = 128
H8 = 8
W2K = 2048
T16 = 16
O32 = 32
TWO = 2
FOUR = 4
K144 = 144
ALL16K = 16384
THREE = 3
VMEM_LIMIT = 46000 * 1024
TAIL_LIMIT = 40000 * 1024


def dot(left, right):
    return jnp.dot(left, right, preferred_element_type=F32)


def dot_t(left, right):
    return lax.dot_general(left, right, (((1,), (1,)), ((), ())), preferred_element_type=F32)


def iota(shape, axis):
    return lax.broadcasted_iota(jnp.int32, shape, axis)


def norm_cols(values):
    centered = values - jnp.mean(values, axis=0, keepdims=True)
    variance = jnp.mean(centered * centered, axis=0, keepdims=True)
    return (centered * lax.rsqrt(variance + 1e-5)).astype(BF16)


def eye(size):
    return (iota((size, size), 0) == iota((size, size), 1)).astype(BF16)


def pick(rows, columns, index):
    return (index(iota((rows, columns), 0)) == iota((rows, columns), 1)).astype(BF16)


def swap8(row):
    return (row % H8) * H8 + row // H8


def column(row_vector, index, size):
    hit = index(iota((size, size), 0)) == iota((size, size), 1)
    wide = jnp.broadcast_to(row_vector.astype(F32), (size, size))
    return jnp.sum(jnp.where(hit, wide, 0.0), axis=1, keepdims=True)


def place():
    me = lax.axis_index('seq')
    batch = lax.axis_index('batch')
    mate = me + 1 - TWO * lax.rem(me, TWO)
    cross = lax.rem(me + TWO, FOUR)
    return me, batch, mate, cross


def meet(batch, peers):
    barrier = pltpu.get_barrier_semaphore()
    for peer in peers:
        pl.semaphore_signal(barrier, inc=1, device_id=(batch, peer), device_id_type=MESH)
    pl.semaphore_wait(barrier, len(peers))


def rows64(index):
    return pl.ds(pl.multiple_of(index * C64, C64), C64)


def row_kernel(e_hbm, z_hbm, mask_hbm, wpb_hbm, wri_hbm, brg_hbm, wro_hbm, wci_hbm,
               e1_ref, g1_ref, kv_ref, qs_ref,
               mask_ref, wpb_ref, wri_ref, brg_ref, wro_ref, wci_ref, small_sem, q_tot, z_buf, e_buf, tmp, own, full, bias, q_s, k_s, v_s, g_s, x_s, rhs, att, w_big, w_ci,
               logit_0, top_0, logit_1, top_1, logit_2, top_2, logit_3, top_3, logit_4, top_4, logit_5, top_5, logit_6, top_6, logit_7, top_7, out_0, out_1, z_sem, e_sem, send_sem, recv_sem):
    logit_s = (logit_0, logit_1, logit_2, logit_3, logit_4, logit_5, logit_6, logit_7)
    top_s = (top_0, top_1, top_2, top_3, top_4, top_5, top_6, top_7)
    out_s = (out_0, out_1)
    me, batch, mate, cross = place()
    small = [pltpu.make_async_copy(src, dst, small_sem.at[n]) for n, (src, dst) in enumerate((
        (wpb_hbm, wpb_ref), (wri_hbm, wri_ref), (wci_hbm, wci_ref), (mask_hbm, mask_ref), (wro_hbm, wro_ref), (brg_hbm, brg_ref)))]
    small[0].start()
    for part in range(H8):
        pltpu.make_async_copy(z_hbm.at[pl.ds(part * H8, H8)], z_buf.at[pl.ds(part * H8, H8)], z_sem.at[part]).start()
    for copy in small[1:]:
        copy.start()
    for part in range(H8):
        pltpu.make_async_copy(e_hbm.at[pl.ds(part * H8, H8)], e_buf.at[pl.ds(part * H8, H8)], e_sem.at[part]).start()
    meet(batch, (mate, cross))

    def big_index(row):
        in_k, in_v = row - C64, row - 192
        head_k = C64 + (in_k // T16) * H8 + in_k % H8
        head_v = jnp.where(in_v % T16 < H8, L128 + (in_v // T16) * H8 + in_v % H8, -1)
        return jnp.where(row < C64, row, jnp.where(row < 192, head_k, jnp.where(row < 320, head_v, row - L128)))

    small[0].wait()
    w_pb = wpb_ref[...]
    rhs[...] = jnp.broadcast_to((iota((K144, R256), 0) == L128).astype(BF16)[None], (T16, K144, R256))

    def bias_part(part, carry):
        pltpu.make_async_copy(z_hbm.at[pl.ds(part * H8, H8)], z_buf.at[pl.ds(part * H8, H8)], z_sem.at[part]).wait()
        z_t = jnp.transpose(z_buf[pl.ds(part * H8, H8)].reshape(W2K, L128).astype(F32))
        heads = dot(w_pb, norm_cols(z_t))
        for t in range(H8):
            for lane in range(TWO):
                at = t * R256 + lane * L128
                tmp[lane, t * H8:(t + 1) * H8, :] = heads[:, at:at + L128]
        for h in range(H8):
            for lane in range(TWO):
                own[h, pl.ds(pl.multiple_of(part * H8, H8), H8), lane * L128:(lane + 1) * L128] = tmp[lane, pl.ds(h, H8, stride=H8), :]
        return carry

    def ship(view, slot, peer):
        return pltpu.make_async_remote_copy(
            src_ref=view, dst_ref=view, send_sem=send_sem.at[slot], recv_sem=recv_sem.at[slot],
            device_id=(batch, peer), device_id_type=MESH)

    def piece(n, slot, peer):
        rows = pl.ds(pl.multiple_of(me * C64 + n * T16, T16), T16)
        return ship(full.at[:, rows, :], slot + n, peer)

    def bias_piece(n, carry):
        lax.fori_loop(TWO * n, TWO * n + TWO, bias_part, 0)
        full[:, pl.ds(pl.multiple_of(me * C64 + n * T16, T16), T16), :] = own[:, pl.ds(pl.multiple_of(n * T16, T16), T16), :].astype(BF16)
        piece(n, 0, cross).start()
        piece(n, FOUR, mate).start()
        return carry

    lax.fori_loop(0, FOUR, bias_piece, 0)
    relay = ship(full.at[:, rows64(cross), :], H8, mate)

    for copy in small[1:]:
        copy.wait()
    w_big[...] = dot_t(pick(384, R256, big_index), wri_ref[...]).astype(BF16)
    w_ci[...] = dot_t(
        pick(K144, K144, lambda row: jnp.where(row < C64, swap8(row), jnp.where(row < L128, C64 + swap8(row - C64), row))),
        wci_ref[...]).astype(BF16)
    ones = ((iota((L128, W2K), 0) % T16) == H8).astype(F32)

    def project_part(part, carry):
        pltpu.make_async_copy(e_hbm.at[pl.ds(part * H8, H8)], e_buf.at[pl.ds(part * H8, H8)], e_sem.at[part]).wait()
        lanes = pl.ds(pl.multiple_of(part * W2K, W2K), W2K)
        x_raw = jnp.concatenate([e_buf[part * H8 + t] for t in range(H8)], axis=1)
        x_s[:, lanes] = x_raw
        x_t = x_raw.astype(F32)
        proj = dot(w_big[...], norm_cols(x_t))
        q_val = proj[0:C64].astype(BF16).astype(F32) * (H8 ** -0.5 * LOG2E)
        q_hi = q_val.astype(BF16).astype(F32)
        q_lo = q_val - q_hi
        for h in range(H8):
            pair = jnp.concatenate([q_hi[h * H8:h * H8 + H8], q_lo[h * H8:h * H8 + H8]], axis=0)
            q_s[h * T16:(h + 1) * T16, lanes] = pair.astype(BF16)
        keep = mask_ref[pl.ds(pl.multiple_of(part * H8, H8), H8), :].astype(F32)
        keep_row = jnp.concatenate([keep[t:t + 1] for t in range(H8)], axis=1)
        k_s[lanes, 0:L128] = jnp.transpose(proj[C64:192] * keep_row).astype(BF16)
        fill = jnp.where(iota((T16, W2K), 0) == 0, (1.0 - keep_row) * (MASK_FILL * LOG2E), 0.0)
        k_s[lanes, L128:K144] = jnp.transpose(fill).astype(BF16)
        v_s[:, lanes] = (proj[192:320] + ones).astype(BF16)
        g_s[:, lanes] = proj[320:384].astype(BF16)
        return carry

    lax.fori_loop(0, 6, project_part, 0)
    for n in range(FOUR):
        piece(n, 0, cross).wait_recv()
    relay.start()
    lax.fori_loop(6, H8, project_part, 0)
    for n in range(FOUR):
        piece(n, FOUR, mate).wait_recv()
    relay.wait_recv()
    for n in range(H8):
        piece(n % FOUR, n // FOUR * FOUR, mate).wait_send()
    relay.wait_send()
    for h in range(H8):
        bias[h] = jnp.transpose(full[h].astype(F32)) * LOG2E

    def at_seq(s):
        s = jnp.clip(s, 0, 63)
        return s, pl.ds(pl.multiple_of(s * R256, R256), R256)

    def load_q(p):
        for n in range(TWO):
            lanes = at_seq(TWO * p + n)[1]
            for h in range(H8):
                sub = slice(h * T16, (h + 1) * T16)
                rhs[n * H8 + h, sub, :] = q_s[sub, lanes]

    def score(p, h):
        slot = h % FOUR
        raw = [dot(k_s[at_seq(TWO * p + n)[1], :], rhs[n * H8 + h]) for n in range(TWO)]
        tops = [[], []]
        for at in range(0, R256, C64):
            shared = bias[h, at:at + C64, :]
            for n in range(TWO):
                logits = raw[n][at:at + C64] + shared
                logit_s[TWO * slot + n][at:at + C64, :] = logits
                tops[n].append(jnp.max(logits.reshape(C64 // H8, H8, R256), axis=0))
        for n in range(TWO):
            best = functools.reduce(jnp.maximum, tops[n])
            top_s[TWO * slot + n][...] = jnp.broadcast_to(jnp.max(best, axis=0, keepdims=True), (H8, R256))

    def soften(p, h):
        if h < 0:
            p, h = p - 1, h + H8
        slot = h % FOUR
        for n in range(TWO):
            v_blk = v_s[h * T16:(h + 1) * T16, at_seq(TWO * p + n)[1]]
            shifted = logit_s[TWO * slot + n][...].reshape(O32, H8, R256) - top_s[TWO * slot + n][...][None]
            out_s[n][h] = dot(v_blk, jnp.exp2(shifted).reshape(R256, R256).astype(BF16))

    def combine(p, h):
        for n in range(TWO):
            s, lanes = at_seq(TWO * p + n)
            some = jnp.max(mask_ref[pl.ds(s, 1), :].astype(F32), axis=1, keepdims=True) > 0.0
            values = v_s[h * T16:(h + 1) * T16, lanes].astype(F32)[0:H8]
            mean = jnp.sum(values, axis=1, keepdims=True) * (1.0 / 256.0)
            out = out_s[n][h]
            att[h * H8:(h + 1) * H8, lanes] = jnp.where(some, out[0:H8] * (1.0 / out[H8:9]), mean)

    load_q(0)

    def attend(t, carry):
        for step in range(THREE):
            p = THREE * t + step
            for h in range(H8):
                score(p, h)
                if h >= TWO:
                    combine(p - 1, h - TWO)
                soften(p, h - TWO)
                if h == TWO - 1:
                    for late in range(H8 - TWO, H8):
                        combine(p - 1, late)
            load_q(p + 1)
        return carry

    lax.fori_loop(0, 33 // THREE, attend, 0)

    w_ro = dot_t(eye(C64), wro_ref[...]).astype(BF16)
    gate_bias = column(brg_ref[...], lambda row: row, C64)
    q_tot[0, 0:C64, :] = jnp.zeros((C64, R256), F32)
    q_tot[0, C64:72, :] = jnp.broadcast_to(jnp.sum(mask_ref[...].astype(F32), axis=0, keepdims=True), (H8, R256))

    def finish_part(part, carry):
        lanes = pl.ds(pl.multiple_of(part * W2K, W2K), W2K)
        gate = jax.nn.sigmoid(g_s[:, lanes].astype(F32) + gate_bias)
        gated = (gate * att[:, lanes]).astype(BF16)
        e_one = (x_s[:, lanes].astype(F32) + dot(w_ro, gated)).astype(BF16)
        e1_ref[:, lanes] = e_one
        normed = norm_cols(e_one.astype(F32))
        x_s[:, lanes] = normed
        query = dot(w_ci[0:C64, :], normed).astype(BF16).astype(F32)
        keep = mask_ref[pl.ds(pl.multiple_of(part * H8, H8), H8), :].astype(F32)
        q_sum = jnp.zeros((C64, R256), F32)
        for t in range(H8):
            q_sum += query[:, t * R256:(t + 1) * R256] * keep[t:t + 1]
        q_tot[0, 0:C64, :] += q_sum
        return carry

    lax.fori_loop(0, H8, finish_part, 0)

    def pass_on(src, dst, slot, peer):
        copy = pltpu.make_async_remote_copy(
            src_ref=q_tot.at[src], dst_ref=q_tot.at[dst], send_sem=send_sem.at[slot], recv_sem=recv_sem.at[slot],
            device_id=(batch, peer), device_id_type=MESH)
        copy.start()
        return copy

    def column_part(part, carry):
        lanes = pl.ds(pl.multiple_of(part * W2K, W2K), W2K)
        proj = dot(w_ci[C64:K144, :], x_s[:, lanes]).astype(BF16)
        g1_ref[:, lanes] = proj[0:C64]
        for t in range(H8):
            kv_ref[part * H8 + t] = proj[C64:80, t * R256:(t + 1) * R256].astype(F32)
        return carry

    query_mate = pass_on(0, 1, 9, mate)
    lax.fori_loop(0, THREE, column_part, 0)
    query_mate.wait_recv()
    q_tot[TWO] = q_tot[0] + q_tot[1]
    query_cross = pass_on(TWO, THREE, 10, cross)
    lax.fori_loop(THREE, H8, column_part, 0)
    query_cross.wait_recv()
    qs_ref[...] = q_tot[TWO] + q_tot[THREE]
    query_mate.wait_send()
    query_cross.wait_send()


def row_stage(msa, pair, mask, wpb, wri, brg, wro, wci):
    hbm = pl.BlockSpec(memory_space=pltpu.HBM)
    vmem = pl.BlockSpec(memory_space=pltpu.VMEM)
    return pl.pallas_call(
        row_kernel,
        name='row_stage',
        out_shape=(
            jax.ShapeDtypeStruct((C64, ALL16K), BF16),
            jax.ShapeDtypeStruct((C64, ALL16K), BF16),
            jax.ShapeDtypeStruct((C64, T16, R256), F32),
            jax.ShapeDtypeStruct((72, R256), F32),
        ),
        in_specs=[hbm] * H8,
        out_specs=(vmem,) * FOUR,
        scratch_shapes=[
            pltpu.VMEM((C64, R256), jnp.int32),
            pltpu.VMEM((H8, L128), BF16),
            pltpu.VMEM((C64, R256), BF16),
            pltpu.VMEM((1, C64), BF16),
            pltpu.VMEM((C64, C64), BF16),
            pltpu.VMEM((C64, K144), BF16),
            pltpu.SemaphoreType.DMA((6,)),
            pltpu.VMEM((FOUR, 72, R256), F32),
            pltpu.VMEM((C64, R256, L128), BF16),
            pltpu.VMEM((C64, C64, R256), BF16),
            pltpu.VMEM((TWO, C64, L128), F32),
            pltpu.VMEM((H8, C64, R256), F32),
            pltpu.VMEM((H8, R256, R256), BF16),
            pltpu.VMEM((H8, R256, R256), F32),
            pltpu.VMEM((L128, ALL16K), BF16),
            pltpu.VMEM((ALL16K, K144), BF16),
            pltpu.VMEM((L128, ALL16K), BF16),
            pltpu.VMEM((C64, ALL16K), BF16),
            pltpu.VMEM((C64, ALL16K), BF16),
            pltpu.VMEM((T16, K144, R256), BF16),
            pltpu.VMEM((C64, ALL16K), F32),
            pltpu.VMEM((384, C64), BF16),
            pltpu.VMEM((K144, C64), BF16),
        ] + [pltpu.VMEM((R256, R256), F32), pltpu.VMEM((H8, R256), F32)] * H8 + [
            pltpu.VMEM((H8, T16, R256), F32),
            pltpu.VMEM((H8, T16, R256), F32),
            pltpu.SemaphoreType.DMA((H8,)),
            pltpu.SemaphoreType.DMA((H8,)),
            pltpu.SemaphoreType.DMA((11,)),
            pltpu.SemaphoreType.DMA((11,)),
        ],
        compiler_params=pltpu.CompilerParams(collective_id=0, has_side_effects=True, vmem_limit_bytes=VMEM_LIMIT),
    )(msa, pair, mask, wpb, wri, brg, wro, wci)


def tail_kernel(qs_ref, kv_ref, mask_ref, e_buf, g_buf, z_hbm, bcg_ref, wco_ref, wti_ref, wto_ref, wom_ref, w_ref, b_ref,
                e3_ref, out_ref,
                second, stat, logit_s, z_buf,
                w_co, w_ti, w_to, w_om, ab_s, ab,
                a_half, b_full, m_full, turn_s, a_tmp, a_s, acc, p_hi0, p_lo0, p_hi1, p_lo1, w_tmp, w_t, inv_s,
                load_sem, stat_send, stat_recv, send_sem, recv_sem):
    me, batch, mate, cross = place()
    z_load = pltpu.make_async_copy(z_hbm, z_buf, load_sem)
    z_load.start()
    barrier = pltpu.get_barrier_semaphore()
    for peer in (mate, cross):
        pl.semaphore_signal(barrier, inc=1, device_id=(batch, peer), device_id_type=MESH)

    def pass_on(src, dst, slot, peer):
        copy = pltpu.make_async_remote_copy(
            src_ref=src, dst_ref=dst, send_sem=stat_send.at[slot], recv_sem=stat_recv.at[slot],
            device_id=(batch, peer), device_id_type=MESH)
        copy.start()
        return copy

    w_co[...] = dot(dot_t(eye(C64), wco_ref[...]).astype(BF16),
                    (swap8(iota((C64, C64), 1)) == iota((C64, C64), 0)).astype(BF16)).astype(BF16)
    w_ti[...] = dot_t(eye(R256), wti_ref[...]).astype(BF16)
    w_to[...] = wto_ref[...]
    w_om[...] = dot_t(eye(C64), wom_ref[...]).astype(BF16)
    for c in range(O32):
        w_tmp[c * 40:c * 40 + O32, :] = w_ref[c * O32:(c + 1) * O32, :].astype(F32)
    for k in range(FOUR):
        for d in range(H8):
            w_t[k, :, d * O32:(d + 1) * O32] = jnp.transpose(w_tmp[pl.ds(k * H8 + d, O32, stride=40), :]).astype(BF16)

    total = qs_ref[...]
    population = total[C64:72] + 1e-10
    q_bar = [(total[d * H8:(d + 1) * H8] / population).astype(BF16).astype(F32) for d in range(H8)]

    def scores(s, top):
        kv = kv_ref[s]
        value = q_bar[0] * kv[0:1]
        for d in range(1, H8):
            value += q_bar[d] * kv[d:d + 1]
        value = jnp.where(mask_ref[pl.ds(s, 1), :] > 0, value * (H8 ** -0.5), MASK_FILL)
        logit_s[s] = value
        return jnp.maximum(top, value)

    top = lax.fori_loop(0, C64, scores, jnp.full((H8, R256), -3e38, F32), unroll=H8)

    def gather(s, sums):
        kv = kv_ref[s]
        weight = jnp.exp(logit_s[s] - top)
        return (sums[0] + weight,) + tuple(sums[d + 1] + weight * kv[H8 + d:9 + d] for d in range(H8))

    sums = lax.fori_loop(0, C64, gather, (jnp.zeros((H8, R256), F32),) * 9, unroll=H8)
    stat[0:H8, :] = top
    for n in range(9):
        stat[H8 + n * H8:T16 + n * H8, :] = sums[n]
    m_full[rows64(me), :] = mask_ref[...].astype(F32).astype(BF16)
    m_view = m_full.at[rows64(me), :]
    pl.semaphore_wait(barrier, TWO)
    stat_mate = pass_on(stat, second.at[0], TWO, mate)
    mask_cross = pass_on(m_view, m_view, FOUR, cross)
    mask_mate = pass_on(m_view, m_view, 5, mate)

    def merge(left, right, dst):
        best = jnp.maximum(left[0:H8, :], right[0:H8, :])
        scale = [jnp.exp(side[0:H8, :] - best) for side in (left, right)]
        dst[0:H8, :] = best
        for at in range(H8, 80, H8):
            dst[at:at + H8, :] = left[at:at + H8, :] * scale[0] + right[at:at + H8, :] * scale[1]

    stat_mate.wait_recv()
    merge(stat, second.at[0], second.at[1])
    stat_cross = pass_on(second.at[1], second.at[TWO], THREE, cross)
    far_mask = m_full.at[rows64(cross), :]
    mask_cross.wait_recv()
    mask_relay = pass_on(far_mask, far_mask, 6, mate)
    stat_cross.wait_recv()
    merge(second.at[1], second.at[TWO], second.at[THREE])
    den = second[THREE, H8:T16, :]
    column_out = jnp.concatenate([second[THREE, T16 + d * H8:24 + d * H8, :] / den for d in range(H8)], axis=0)
    col = jnp.concatenate([column_out] * H8, axis=1)
    gate_bias = column(bcg_ref[...], swap8, C64)

    def send(src, dst, slot, peer):
        return pltpu.make_async_remote_copy(
            src_ref=src, dst_ref=dst, send_sem=send_sem.at[slot], recv_sem=recv_sem.at[slot],
            device_id=(batch, peer), device_id_type=MESH)

    def lanes_of(device):
        return pl.ds(pl.multiple_of((device // TWO) * L128, L128), L128)

    def rows16(device, block):
        return pl.ds(pl.multiple_of(device * C64 + block * T16, T16), T16)

    def b_piece(k, src_rows, dst_rows, slot, peer):
        return send(ab.at[pl.ds(O32 + k * H8, H8), src_rows, :], b_full.at[pl.ds(k * H8, H8), dst_rows, :], slot, peer)

    whole = pl.ds(0, C64)

    def a_cross(n):
        return send(ab.at[pl.ds(0, O32), rows16(0, n), lanes_of(cross)], a_half.at[:, rows16(me, n), :], n, cross)

    def late_cross(k):
        return b_piece(k, whole, rows64(me), FOUR + k, cross)

    def b_mate(k):
        return b_piece(k, whole, rows64(me), H8 + k, mate)

    def b_relay(k):
        far_b = b_full.at[pl.ds(k * H8, H8), rows64(cross), :]
        return send(far_b, far_b, 12 + k, mate)

    a_mate = send(ab.at[pl.ds(0, O32), :, lanes_of(me)], a_half.at[:, rows64(me), :], T16, mate)
    far_a = a_half.at[:, rows64(cross), :]
    a_relay = send(far_a, far_a, 17, mate)


    def sixteen(block, done):
        def half(part, carry):
            where = block * TWO + part
            lanes = pl.ds(pl.multiple_of(where * W2K, W2K), W2K)
            gate = jax.nn.sigmoid(g_buf[:, lanes].astype(F32) + gate_bias)
            gated = (gate * col).astype(BF16)
            e_two = (e_buf[:, lanes].astype(F32) + dot(w_co[...], gated)).astype(BF16).astype(F32)
            hidden = jnp.maximum(dot(w_ti[...], norm_cols(e_two)), 0.0).astype(BF16)
            e_three = (e_two + dot(w_to[...], hidden)).astype(BF16).astype(F32)
            for t in range(H8):
                e3_ref[where * H8 + t] = e_three[:, t * R256:(t + 1) * R256].astype(BF16)
            proj = dot(w_om[...], norm_cols(e_three)).astype(BF16).astype(F32)
            keep = mask_ref[pl.ds(pl.multiple_of(where * H8, H8), H8), :].astype(F32)
            for t in range(H8):
                at = pl.ds(pl.multiple_of((part * H8 + t) * 72, H8), C64)
                for lane in range(TWO):
                    cut = slice(lane * L128, (lane + 1) * L128)
                    ab_s[lane, at, :] = proj[:, t * R256 + lane * L128:t * R256 + (lane + 1) * L128] * keep[t:t + 1, cut]
            return carry

        lax.fori_loop(0, TWO, half, 0)
        for f in range(C64):
            for lane in range(TWO):
                ab[f, rows16(0, block), lane * L128:(lane + 1) * L128] = (
                    ab_s[lane, pl.ds(f, T16, stride=72), :].astype(BF16))
        a_cross(block).start()
        return done

    lax.fori_loop(0, FOUR, sixteen, 0)
    a_mate.start()
    for k in range(FOUR):
        late_cross(k).start()
        b_mate(k).start()

    a_half[:, rows64(me), :] = ab[0:O32, :, lanes_of(me)]
    b_full[:, rows64(me), :] = ab[O32:C64, :, :]
    mask_mate.wait_recv()
    mask_relay.wait_recv()
    keep_all = m_full[...]
    inv_s[...] = 1.0 / (dot(jnp.transpose(keep_all.astype(F32)).astype(BF16), keep_all) + 1e-3)
    z_load.wait()
    e_bias = b_ref[...].astype(F32)

    for n in range(FOUR):
        a_cross(n).wait_recv()
    a_relay.start()
    a_mate.wait_recv()
    a_relay.wait_recv()
    offset = pl.multiple_of(lax.rem(me, TWO) * C64, C64)

    def turn(c, carry):
        turn_s[...] = jnp.transpose(a_half[c].astype(F32))
        mine = turn_s[pl.ds(offset, C64), :]
        for lane in range(TWO):
            a_tmp[lane, pl.ds(pl.multiple_of(c * 72, H8), C64), :] = mine[:, lane * L128:(lane + 1) * L128]
        return carry

    lax.fori_loop(0, O32, turn, 0)
    for i in range(C64):
        for lane in range(TWO):
            a_s[i * O32:(i + 1) * O32, lane * L128:(lane + 1) * L128] = a_tmp[lane, pl.ds(i, O32, stride=72), :].astype(BF16)

    late_cross(0).wait_recv()
    b_relay(0).start()
    slots = ((p_hi0, p_lo0), (p_hi1, p_lo1))

    def outer(slot, index, d):
        p_hi, p_lo = slots[slot]
        k, n = index // H8, lax.rem(index, H8)
        value = dot(a_s[pl.ds(pl.multiple_of(n * R256, R256), R256), :], b_full[k * H8 + d])
        high = value.astype(BF16)
        low = (value - high.astype(F32)).astype(BF16)
        for i in range(H8):
            p_hi[i, d * O32:(d + 1) * O32, :] = high[i * O32:(i + 1) * O32]
            p_lo[i, d * O32:(d + 1) * O32, :] = low[i * O32:(i + 1) * O32]

    def project(slot, index, i):
        p_hi, p_lo = slots[slot]
        index = jnp.maximum(index, 0)
        k, at = index // H8, lax.rem(index, H8) * H8 + i
        part = dot(w_t[k], p_hi[i]) + dot(w_t[k], p_lo[i])
        acc[at] = jnp.where(k == 0, part, acc[at] + part)

    def settle(index, i):
        at = jnp.maximum(index - 24, 0) * H8 + i
        update = acc[at] * inv_s[pl.ds(me * C64 + at, 1), :]
        out_ref[at] = (z_buf[at].astype(F32) + jnp.transpose(update) + e_bias).astype(BF16)

    def pair(last, t, carry):
        k = t // TWO

        @pl.when(lax.rem(t, TWO) == 0)
        def _():
            b_mate(k).wait_recv()
            b_relay(k).wait_recv()

        if not last:
            @pl.when(lax.rem(t, TWO) == 1)
            def _():
                late_cross(k + 1).wait_recv()
                b_relay(k + 1).start()

        for step in range(FOUR):
            index, slot = FOUR * t + step, step % TWO
            for n in range(H8):
                outer(slot, index, n)
                project(1 - slot, index - 1, n)
                if last:
                    settle(index - TWO, n)
        return carry

    lax.fori_loop(0, 6, functools.partial(pair, False), 0)
    lax.fori_loop(6, H8, functools.partial(pair, True), 0)
    for n in range(H8):
        project(1, 31, n)
        settle(30, n)
    for n in range(H8):
        settle(31, n)
    for copy in (stat_mate, stat_cross, mask_cross, mask_mate, mask_relay, a_mate, a_relay):
        copy.wait_send()
    for n in range(FOUR):
        a_cross(n).wait_send()
        late_cross(n).wait_send()
        b_mate(n).wait_send()
        b_relay(n).wait_send()


def tail_stage(qs, kv, mask, e1, g1, pair, bcg, wco, wti, wto, wom, weight, bias):
    any_spec = pl.BlockSpec(memory_space=pl.ANY)
    vmem = pl.BlockSpec(memory_space=pltpu.VMEM)
    return pl.pallas_call(
        tail_kernel,
        name='tail_stage',
        out_shape=(jax.ShapeDtypeStruct((C64, C64, R256), BF16), jax.ShapeDtypeStruct((C64, R256, L128), BF16)),
        in_specs=[vmem] * 5 + [any_spec] + [vmem] * 7,
        out_specs=(vmem, vmem),
        scratch_shapes=[
            pltpu.VMEM((FOUR, 80, R256), F32),
            pltpu.VMEM((80, R256), F32),
            pltpu.VMEM((C64, H8, R256), F32),
            pltpu.VMEM((C64, R256, L128), BF16),
            pltpu.VMEM((C64, C64), BF16),
            pltpu.VMEM((R256, C64), BF16),
            pltpu.VMEM((C64, R256), BF16),
            pltpu.VMEM((C64, C64), BF16),
            pltpu.VMEM((TWO, 1152, L128), F32),
            pltpu.VMEM((C64, C64, R256), BF16),
            pltpu.VMEM((O32, R256, L128), BF16),
            pltpu.VMEM((O32, R256, R256), BF16),
            pltpu.VMEM((R256, R256), BF16),
            pltpu.VMEM((L128, R256), F32),
            pltpu.VMEM((TWO, 2304, L128), F32),
            pltpu.VMEM((W2K, R256), BF16),
            pltpu.VMEM((C64, L128, R256), F32),
        ] + [pltpu.VMEM((H8, R256, R256), BF16)] * FOUR + [
            pltpu.VMEM((1280, L128), F32),
            pltpu.VMEM((FOUR, L128, R256), BF16),
            pltpu.VMEM((R256, R256), F32),
            pltpu.SemaphoreType.DMA(()),
            pltpu.SemaphoreType.DMA((7,)),
            pltpu.SemaphoreType.DMA((7,)),
            pltpu.SemaphoreType.DMA((18,)),
            pltpu.SemaphoreType.DMA((18,)),
        ],
        compiler_params=pltpu.CompilerParams(collective_id=1, has_side_effects=True, vmem_limit_bytes=TAIL_LIMIT),
    )(qs, kv, mask, e1, g1, pair, bcg, wco, wti, wto, wom, weight, bias)


def solution(mesh):
    row_spec = P(('batch', 'seq'))
    rep_spec = P()

    def local_block(msa, mask, pair, w_pair_bias, w_row_in, b_row_gate, w_row_out, w_col_in, b_col_gate, w_col_out, w_trans_in, w_trans_out, w_opm_in, w_opm_out, b_opm_out):
        pinned = [pltpu.with_memory_space_constraint(value, pltpu.HBM) for value in (
            jnp.swapaxes(msa, 1, TWO), pair, mask, w_pair_bias.T, w_row_in, b_row_gate.reshape(1, C64), w_row_out, w_col_in)]
        e1, g1, kv, qs = row_stage(*pinned)
        e3, pair_out = tail_stage(qs, kv, mask, e1, g1, pair, b_col_gate.reshape(1, C64), w_col_out, w_trans_in, w_trans_out.T, w_opm_in, w_opm_out.reshape(1024, L128), b_opm_out.reshape(1, L128))
        return jnp.swapaxes(e3, 1, TWO), pair_out

    return jax.shard_map(local_block, mesh=mesh, in_specs=(row_spec, row_spec, row_spec) + (rep_spec,) * 12, out_specs=(row_spec, row_spec), check_vma=False)
```

```python
import functools

import jax
import jax.numpy as jnp
from jax import lax
from jax.experimental import pallas as pl
from jax.experimental.pallas import tpu as pltpu
from jax.sharding import PartitionSpec as P

F32, BF16 = jnp.float32, jnp.bfloat16
MESH = pl.DeviceIdType.MESH
LOG2E = 1.4426950408889634
MASK_FILL = -1e9
R256 = 256
C64 = 64
L128 = 128
H8 = 8
W2K = 2048
T16 = 16
O32 = 32
TWO = 2
FOUR = 4
K144 = 144
ALL16K = 16384
THREE = 3
VMEM_LIMIT = 46000 * 1024
TAIL_LIMIT = 40000 * 1024


def dot(left, right):
    return jnp.dot(left, right, preferred_element_type=F32)


def dot_t(left, right):
    return lax.dot_general(left, right, (((1,), (1,)), ((), ())), preferred_element_type=F32)


def iota(shape, axis):
    return lax.broadcasted_iota(jnp.int32, shape, axis)


def norm_cols(values):
    centered = values - jnp.mean(values, axis=0, keepdims=True)
    variance = jnp.mean(centered * centered, axis=0, keepdims=True)
    return (centered * lax.rsqrt(variance + 1e-5)).astype(BF16)


def eye(size):
    return (iota((size, size), 0) == iota((size, size), 1)).astype(BF16)


def pick(rows, columns, index):
    return (index(iota((rows, columns), 0)) == iota((rows, columns), 1)).astype(BF16)


def swap8(row):
    return (row % H8) * H8 + row // H8


def column(row_vector, index, size):
    hit = index(iota((size, size), 0)) == iota((size, size), 1)
    wide = jnp.broadcast_to(row_vector.astype(F32), (size, size))
    return jnp.sum(jnp.where(hit, wide, 0.0), axis=1, keepdims=True)


def place():
    me = lax.axis_index('seq')
    batch = lax.axis_index('batch')
    mate = me + 1 - TWO * lax.rem(me, TWO)
    cross = lax.rem(me + TWO, FOUR)
    return me, batch, mate, cross


def rows64(index):
    return pl.ds(pl.multiple_of(index * C64, C64), C64)


def row_kernel(e_hbm, z_hbm, mask_hbm, wpb_hbm, wri_hbm, brg_hbm, wro_hbm, wci_hbm,
               e1_ref, g1_ref, kv_ref, qs_ref,
               mask_ref, wpb_ref, wri_ref, brg_ref, wro_ref, wci_ref, small_sem, q_tot, z_buf, e_buf, tmp, own, full, bias, q_s, k_s, v_s, g_s, x_s, rhs, att, w_big, w_ci,
               logit_0, top_0, logit_1, top_1, logit_2, top_2, logit_3, top_3, logit_4, top_4, logit_5, top_5, logit_6, top_6, logit_7, top_7, out_0, out_1, z_sem, e_sem, send_sem, recv_sem):
    logit_s = (logit_0, logit_1, logit_2, logit_3, logit_4, logit_5, logit_6, logit_7)
    top_s = (top_0, top_1, top_2, top_3, top_4, top_5, top_6, top_7)
    out_s = (out_0, out_1)
    me, batch, mate, cross = place()
    small = [pltpu.make_async_copy(src, dst, small_sem.at[n]) for n, (src, dst) in enumerate((
        (wpb_hbm, wpb_ref), (wri_hbm, wri_ref), (wci_hbm, wci_ref), (mask_hbm, mask_ref), (wro_hbm, wro_ref), (brg_hbm, brg_ref)))]
    small[0].start()
    for part in range(H8):
        pltpu.make_async_copy(z_hbm.at[pl.ds(part * H8, H8)], z_buf.at[pl.ds(part * H8, H8)], z_sem.at[part]).start()
    for copy in small[1:]:
        copy.start()
    for part in range(H8):
        pltpu.make_async_copy(e_hbm.at[pl.ds(part * H8, H8)], e_buf.at[pl.ds(part * H8, H8)], e_sem.at[part]).start()
    barrier = pltpu.get_barrier_semaphore()
    for peer in (mate, cross):
        pl.semaphore_signal(barrier, inc=1, device_id=(batch, peer), device_id_type=MESH)

    def big_index(row):
        in_k, in_v = row - C64, row - 192
        head_k = C64 + (in_k // T16) * H8 + in_k % H8
        head_v = jnp.where(in_v % T16 < H8, L128 + (in_v // T16) * H8 + in_v % H8, -1)
        return jnp.where(row < C64, row, jnp.where(row < 192, head_k, jnp.where(row < 320, head_v, row - L128)))

    small[0].wait()
    w_pb = wpb_ref[...]
    rhs[...] = jnp.broadcast_to((iota((K144, R256), 0) == L128).astype(BF16)[None], (T16, K144, R256))

    def bias_part(part, carry):
        pltpu.make_async_copy(z_hbm.at[pl.ds(part * H8, H8)], z_buf.at[pl.ds(part * H8, H8)], z_sem.at[part]).wait()
        z_t = jnp.transpose(z_buf[pl.ds(part * H8, H8)].reshape(W2K, L128).astype(F32))
        heads = dot(w_pb, norm_cols(z_t))
        for t in range(H8):
            for lane in range(TWO):
                at = t * R256 + lane * L128
                tmp[lane, t * H8:(t + 1) * H8, :] = heads[:, at:at + L128]
        for h in range(H8):
            for lane in range(TWO):
                own[h, pl.ds(pl.multiple_of(part * H8, H8), H8), lane * L128:(lane + 1) * L128] = tmp[lane, pl.ds(h, H8, stride=H8), :]
        return carry

    def ship(view, slot, peer):
        return pltpu.make_async_remote_copy(
            src_ref=view, dst_ref=view, send_sem=send_sem.at[slot], recv_sem=recv_sem.at[slot],
            device_id=(batch, peer), device_id_type=MESH)

    def piece(n, slot, peer):
        rows = pl.ds(pl.multiple_of(me * C64 + n * T16, T16), T16)
        return ship(full.at[:, rows, :], slot + n, peer)

    def bias_send(n):
        full[:, pl.ds(pl.multiple_of(me * C64 + n * T16, T16), T16), :] = own[:, pl.ds(pl.multiple_of(n * T16, T16), T16), :].astype(BF16)
        piece(n, 0, cross).start()
        piece(n, FOUR, mate).start()

    def bias_piece(n, carry):
        lax.fori_loop(TWO * n, TWO * n + TWO, bias_part, 0)
        bias_send(n)
        return carry

    lax.fori_loop(0, TWO, bias_part, 0)
    pl.semaphore_wait(barrier, TWO)
    bias_send(0)
    lax.fori_loop(1, FOUR, bias_piece, 0)
    relay = ship(full.at[:, rows64(cross), :], H8, mate)

    for copy in small[1:]:
        copy.wait()
    w_big[...] = dot_t(pick(384, R256, big_index), wri_ref[...]).astype(BF16)
    w_ci[...] = dot_t(
        pick(K144, K144, lambda row: jnp.where(row < C64, swap8(row), jnp.where(row < L128, C64 + swap8(row - C64), row))),
        wci_ref[...]).astype(BF16)
    ones = ((iota((L128, W2K), 0) % T16) == H8).astype(F32)

    def project_part(part, carry):
        pltpu.make_async_copy(e_hbm.at[pl.ds(part * H8, H8)], e_buf.at[pl.ds(part * H8, H8)], e_sem.at[part]).wait()
        lanes = pl.ds(pl.multiple_of(part * W2K, W2K), W2K)
        x_raw = jnp.concatenate([e_buf[part * H8 + t] for t in range(H8)], axis=1)
        x_s[:, lanes] = x_raw
        x_t = x_raw.astype(F32)
        proj = dot(w_big[...], norm_cols(x_t))
        q_val = proj[0:C64].astype(BF16).astype(F32) * (H8 ** -0.5 * LOG2E)
        q_hi = q_val.astype(BF16).astype(F32)
        q_lo = q_val - q_hi
        for h in range(H8):
            pair = jnp.concatenate([q_hi[h * H8:h * H8 + H8], q_lo[h * H8:h * H8 + H8]], axis=0)
            q_s[h * T16:(h + 1) * T16, lanes] = pair.astype(BF16)
        keep = mask_ref[pl.ds(pl.multiple_of(part * H8, H8), H8), :].astype(F32)
        keep_row = jnp.concatenate([keep[t:t + 1] for t in range(H8)], axis=1)
        k_s[lanes, 0:L128] = jnp.transpose(proj[C64:192] * keep_row).astype(BF16)
        fill = jnp.where(iota((T16, W2K), 0) == 0, (1.0 - keep_row) * (MASK_FILL * LOG2E), 0.0)
        k_s[lanes, L128:K144] = jnp.transpose(fill).astype(BF16)
        v_s[:, lanes] = (proj[192:320] + ones).astype(BF16)
        g_s[:, lanes] = proj[320:384].astype(BF16)
        return carry

    lax.fori_loop(0, 6, project_part, 0)
    for n in range(FOUR):
        piece(n, 0, cross).wait_recv()
    relay.start()
    lax.fori_loop(6, H8, project_part, 0)
    for n in range(FOUR):
        piece(n, FOUR, mate).wait_recv()
    relay.wait_recv()
    for n in range(H8):
        piece(n % FOUR, n // FOUR * FOUR, mate).wait_send()
    relay.wait_send()
    for h in range(H8):
        bias[h] = jnp.transpose(full[h].astype(F32)) * LOG2E

    def at_seq(s):
        s = jnp.clip(s, 0, 63)
        return s, pl.ds(pl.multiple_of(s * R256, R256), R256)

    def load_q(p):
        for n in range(TWO):
            lanes = at_seq(TWO * p + n)[1]
            for h in range(H8):
                sub = slice(h * T16, (h + 1) * T16)
                rhs[n * H8 + h, sub, :] = q_s[sub, lanes]

    def score(p, h):
        slot = h % FOUR
        raw = [dot(k_s[at_seq(TWO * p + n)[1], :], rhs[n * H8 + h]) for n in range(TWO)]
        tops = [[], []]
        for at in range(0, R256, C64):
            shared = bias[h, at:at + C64, :]
            for n in range(TWO):
                logits = raw[n][at:at + C64] + shared
                logit_s[TWO * slot + n][at:at + C64, :] = logits
                tops[n].append(jnp.max(logits.reshape(C64 // H8, H8, R256), axis=0))
        for n in range(TWO):
            best = functools.reduce(jnp.maximum, tops[n])
            top_s[TWO * slot + n][...] = jnp.broadcast_to(jnp.max(best, axis=0, keepdims=True), (H8, R256))

    def soften(p, h):
        if h < 0:
            p, h = p - 1, h + H8
        slot = h % FOUR
        for n in range(TWO):
            v_blk = v_s[h * T16:(h + 1) * T16, at_seq(TWO * p + n)[1]]
            shifted = logit_s[TWO * slot + n][...].reshape(O32, H8, R256) - top_s[TWO * slot + n][...][None]
            out_s[n][h] = dot(v_blk, jnp.exp2(shifted).reshape(R256, R256).astype(BF16))

    def combine(p, h):
        for n in range(TWO):
            s, lanes = at_seq(TWO * p + n)
            some = jnp.max(mask_ref[pl.ds(s, 1), :].astype(F32), axis=1, keepdims=True) > 0.0
            values = v_s[h * T16:(h + 1) * T16, lanes].astype(F32)[0:H8]
            mean = jnp.sum(values, axis=1, keepdims=True) * (1.0 / 256.0)
            out = out_s[n][h]
            att[h * H8:(h + 1) * H8, lanes] = jnp.where(some, out[0:H8] * (1.0 / out[H8:9]), mean)

    load_q(0)

    def attend(t, carry):
        for step in range(THREE):
            p = THREE * t + step
            for h in range(H8):
                score(p, h)
                if h >= TWO:
                    combine(p - 1, h - TWO)
                soften(p, h - TWO)
                if h == TWO - 1:
                    for late in range(H8 - TWO, H8):
                        combine(p - 1, late)
            load_q(p + 1)
        return carry

    lax.fori_loop(0, 33 // THREE, attend, 0)

    w_ro = dot_t(eye(C64), wro_ref[...]).astype(BF16)
    gate_bias = column(brg_ref[...], lambda row: row, C64)
    q_tot[0, 0:C64, :] = jnp.zeros((C64, R256), F32)
    q_tot[0, C64:72, :] = jnp.broadcast_to(jnp.sum(mask_ref[...].astype(F32), axis=0, keepdims=True), (H8, R256))

    def finish_part(part, carry):
        lanes = pl.ds(pl.multiple_of(part * W2K, W2K), W2K)
        gate = jax.nn.sigmoid(g_s[:, lanes].astype(F32) + gate_bias)
        gated = (gate * att[:, lanes]).astype(BF16)
        e_one = (x_s[:, lanes].astype(F32) + dot(w_ro, gated)).astype(BF16)
        e1_ref[:, lanes] = e_one
        normed = norm_cols(e_one.astype(F32))
        x_s[:, lanes] = normed
        query = dot(w_ci[0:C64, :], normed).astype(BF16).astype(F32)
        keep = mask_ref[pl.ds(pl.multiple_of(part * H8, H8), H8), :].astype(F32)
        q_sum = jnp.zeros((C64, R256), F32)
        for t in range(H8):
            q_sum += query[:, t * R256:(t + 1) * R256] * keep[t:t + 1]
        q_tot[0, 0:C64, :] += q_sum
        return carry

    lax.fori_loop(0, H8, finish_part, 0)

    def pass_on(src, dst, slot, peer):
        copy = pltpu.make_async_remote_copy(
            src_ref=q_tot.at[src], dst_ref=q_tot.at[dst], send_sem=send_sem.at[slot], recv_sem=recv_sem.at[slot],
            device_id=(batch, peer), device_id_type=MESH)
        copy.start()
        return copy

    def column_part(part, carry):
        lanes = pl.ds(pl.multiple_of(part * W2K, W2K), W2K)
        proj = dot(w_ci[C64:K144, :], x_s[:, lanes]).astype(BF16)
        g1_ref[:, lanes] = proj[0:C64]
        for t in range(H8):
            kv_ref[part * H8 + t] = proj[C64:80, t * R256:(t + 1) * R256].astype(F32)
        return carry

    query_mate = pass_on(0, 1, 9, mate)
    lax.fori_loop(0, THREE, column_part, 0)
    query_mate.wait_recv()
    q_tot[TWO] = q_tot[0] + q_tot[1]
    query_cross = pass_on(TWO, THREE, 10, cross)
    lax.fori_loop(THREE, H8, column_part, 0)
    query_cross.wait_recv()
    qs_ref[...] = q_tot[TWO] + q_tot[THREE]
    query_mate.wait_send()
    query_cross.wait_send()


def row_stage(msa, pair, mask, wpb, wri, brg, wro, wci):
    hbm = pl.BlockSpec(memory_space=pltpu.HBM)
    vmem = pl.BlockSpec(memory_space=pltpu.VMEM)
    return pl.pallas_call(
        row_kernel,
        name='row_stage',
        out_shape=(
            jax.ShapeDtypeStruct((C64, ALL16K), BF16),
            jax.ShapeDtypeStruct((C64, ALL16K), BF16),
            jax.ShapeDtypeStruct((C64, T16, R256), F32),
            jax.ShapeDtypeStruct((72, R256), F32),
        ),
        in_specs=[hbm] * H8,
        out_specs=(vmem,) * FOUR,
        scratch_shapes=[
            pltpu.VMEM((C64, R256), jnp.int32),
            pltpu.VMEM((H8, L128), BF16),
            pltpu.VMEM((C64, R256), BF16),
            pltpu.VMEM((1, C64), BF16),
            pltpu.VMEM((C64, C64), BF16),
            pltpu.VMEM((C64, K144), BF16),
            pltpu.SemaphoreType.DMA((6,)),
            pltpu.VMEM((FOUR, 72, R256), F32),
            pltpu.VMEM((C64, R256, L128), BF16),
            pltpu.VMEM((C64, C64, R256), BF16),
            pltpu.VMEM((TWO, C64, L128), F32),
            pltpu.VMEM((H8, C64, R256), F32),
            pltpu.VMEM((H8, R256, R256), BF16),
            pltpu.VMEM((H8, R256, R256), F32),
            pltpu.VMEM((L128, ALL16K), BF16),
            pltpu.VMEM((ALL16K, K144), BF16),
            pltpu.VMEM((L128, ALL16K), BF16),
            pltpu.VMEM((C64, ALL16K), BF16),
            pltpu.VMEM((C64, ALL16K), BF16),
            pltpu.VMEM((T16, K144, R256), BF16),
            pltpu.VMEM((C64, ALL16K), F32),
            pltpu.VMEM((384, C64), BF16),
            pltpu.VMEM((K144, C64), BF16),
        ] + [pltpu.VMEM((R256, R256), F32), pltpu.VMEM((H8, R256), F32)] * H8 + [
            pltpu.VMEM((H8, T16, R256), F32),
            pltpu.VMEM((H8, T16, R256), F32),
            pltpu.SemaphoreType.DMA((H8,)),
            pltpu.SemaphoreType.DMA((H8,)),
            pltpu.SemaphoreType.DMA((11,)),
            pltpu.SemaphoreType.DMA((11,)),
        ],
        compiler_params=pltpu.CompilerParams(collective_id=0, has_side_effects=True, vmem_limit_bytes=VMEM_LIMIT),
    )(msa, pair, mask, wpb, wri, brg, wro, wci)


def tail_kernel(qs_ref, kv_ref, mask_ref, e_buf, g_buf, z_hbm, bcg_ref, wco_ref, wti_ref, wto_ref, wom_ref, w_ref, b_ref,
                e3_ref, out_ref,
                second, stat, logit_s, z_buf,
                w_co, w_ti, w_to, w_om, ab_s, ab,
                a_half, b_full, m_full, turn_s, a_tmp, a_s, acc, p_hi0, p_lo0, p_hi1, p_lo1, w_tmp, w_t, inv_s,
                load_sem, stat_send, stat_recv, send_sem, recv_sem):
    me, batch, mate, cross = place()
    z_load = pltpu.make_async_copy(z_hbm, z_buf, load_sem)
    z_load.start()
    barrier = pltpu.get_barrier_semaphore()
    for peer in (mate, cross):
        pl.semaphore_signal(barrier, inc=1, device_id=(batch, peer), device_id_type=MESH)

    def pass_on(src, dst, slot, peer):
        copy = pltpu.make_async_remote_copy(
            src_ref=src, dst_ref=dst, send_sem=stat_send.at[slot], recv_sem=stat_recv.at[slot],
            device_id=(batch, peer), device_id_type=MESH)
        copy.start()
        return copy

    w_co[...] = dot(dot_t(eye(C64), wco_ref[...]).astype(BF16),
                    (swap8(iota((C64, C64), 1)) == iota((C64, C64), 0)).astype(BF16)).astype(BF16)
    w_ti[...] = dot_t(eye(R256), wti_ref[...]).astype(BF16)
    w_to[...] = wto_ref[...]
    w_om[...] = dot_t(eye(C64), wom_ref[...]).astype(BF16)
    for c in range(O32):
        w_tmp[c * 40:c * 40 + O32, :] = w_ref[c * O32:(c + 1) * O32, :].astype(F32)
    for k in range(FOUR):
        for d in range(H8):
            w_t[k, :, d * O32:(d + 1) * O32] = jnp.transpose(w_tmp[pl.ds(k * H8 + d, O32, stride=40), :]).astype(BF16)

    total = qs_ref[...]
    population = total[C64:72] + 1e-10
    q_bar = [(total[d * H8:(d + 1) * H8] / population).astype(BF16).astype(F32) for d in range(H8)]

    def scores(s, top):
        kv = kv_ref[s]
        value = q_bar[0] * kv[0:1]
        for d in range(1, H8):
            value += q_bar[d] * kv[d:d + 1]
        value = jnp.where(mask_ref[pl.ds(s, 1), :] > 0, value * (H8 ** -0.5), MASK_FILL)
        logit_s[s] = value
        return jnp.maximum(top, value)

    top = lax.fori_loop(0, C64, scores, jnp.full((H8, R256), -3e38, F32), unroll=H8)

    def gather(s, sums):
        kv = kv_ref[s]
        weight = jnp.exp(logit_s[s] - top)
        return (sums[0] + weight,) + tuple(sums[d + 1] + weight * kv[H8 + d:9 + d] for d in range(H8))

    sums = lax.fori_loop(0, C64, gather, (jnp.zeros((H8, R256), F32),) * 9, unroll=H8)
    stat[0:H8, :] = top
    for n in range(9):
        stat[H8 + n * H8:T16 + n * H8, :] = sums[n]
    m_full[rows64(me), :] = mask_ref[...].astype(F32).astype(BF16)
    m_view = m_full.at[rows64(me), :]
    pl.semaphore_wait(barrier, TWO)
    stat_mate = pass_on(stat, second.at[0], TWO, mate)
    mask_cross = pass_on(m_view, m_view, FOUR, cross)
    mask_mate = pass_on(m_view, m_view, 5, mate)

    def merge(left, right, dst):
        best = jnp.maximum(left[0:H8, :], right[0:H8, :])
        scale = [jnp.exp(side[0:H8, :] - best) for side in (left, right)]
        dst[0:H8, :] = best
        for at in range(H8, 80, H8):
            dst[at:at + H8, :] = left[at:at + H8, :] * scale[0] + right[at:at + H8, :] * scale[1]

    stat_mate.wait_recv()
    merge(stat, second.at[0], second.at[1])
    stat_cross = pass_on(second.at[1], second.at[TWO], THREE, cross)
    far_mask = m_full.at[rows64(cross), :]
    mask_cross.wait_recv()
    mask_relay = pass_on(far_mask, far_mask, 6, mate)
    stat_cross.wait_recv()
    merge(second.at[1], second.at[TWO], second.at[THREE])
    den = second[THREE, H8:T16, :]
    column_out = jnp.concatenate([second[THREE, T16 + d * H8:24 + d * H8, :] / den for d in range(H8)], axis=0)
    col = jnp.concatenate([column_out] * H8, axis=1)
    gate_bias = column(bcg_ref[...], swap8, C64)

    def send(src, dst, slot, peer):
        return pltpu.make_async_remote_copy(
            src_ref=src, dst_ref=dst, send_sem=send_sem.at[slot], recv_sem=recv_sem.at[slot],
            device_id=(batch, peer), device_id_type=MESH)

    def lanes_of(device):
        return pl.ds(pl.multiple_of((device // TWO) * L128, L128), L128)

    def rows16(device, block):
        return pl.ds(pl.multiple_of(device * C64 + block * T16, T16), T16)

    def b_piece(k, src_rows, dst_rows, slot, peer):
        return send(ab.at[pl.ds(O32 + k * H8, H8), src_rows, :], b_full.at[pl.ds(k * H8, H8), dst_rows, :], slot, peer)

    whole = pl.ds(0, C64)

    def a_cross(n):
        return send(ab.at[pl.ds(0, O32), rows16(0, n), lanes_of(cross)], a_half.at[:, rows16(me, n), :], n, cross)

    def late_cross(k):
        return b_piece(k, whole, rows64(me), FOUR + k, cross)

    def b_mate(k):
        return b_piece(k, whole, rows64(me), H8 + k, mate)

    def b_relay(k):
        far_b = b_full.at[pl.ds(k * H8, H8), rows64(cross), :]
        return send(far_b, far_b, 12 + k, mate)

    a_mate = send(ab.at[pl.ds(0, O32), :, lanes_of(me)], a_half.at[:, rows64(me), :], T16, mate)
    far_a = a_half.at[:, rows64(cross), :]
    a_relay = send(far_a, far_a, 17, mate)


    def sixteen(block, done):
        def half(part, carry):
            where = block * TWO + part
            lanes = pl.ds(pl.multiple_of(where * W2K, W2K), W2K)
            gate = jax.nn.sigmoid(g_buf[:, lanes].astype(F32) + gate_bias)
            gated = (gate * col).astype(BF16)
            e_two = (e_buf[:, lanes].astype(F32) + dot(w_co[...], gated)).astype(BF16).astype(F32)
            hidden = jnp.maximum(dot(w_ti[...], norm_cols(e_two)), 0.0).astype(BF16)
            e_three = (e_two + dot(w_to[...], hidden)).astype(BF16).astype(F32)
            for t in range(H8):
                e3_ref[where * H8 + t] = e_three[:, t * R256:(t + 1) * R256].astype(BF16)
            proj = dot(w_om[...], norm_cols(e_three)).astype(BF16).astype(F32)
            keep = mask_ref[pl.ds(pl.multiple_of(where * H8, H8), H8), :].astype(F32)
            for t in range(H8):
                at = pl.ds(pl.multiple_of((part * H8 + t) * 72, H8), C64)
                for lane in range(TWO):
                    cut = slice(lane * L128, (lane + 1) * L128)
                    ab_s[lane, at, :] = proj[:, t * R256 + lane * L128:t * R256 + (lane + 1) * L128] * keep[t:t + 1, cut]
            return carry

        lax.fori_loop(0, TWO, half, 0)
        for f in range(C64):
            for lane in range(TWO):
                ab[f, rows16(0, block), lane * L128:(lane + 1) * L128] = (
                    ab_s[lane, pl.ds(f, T16, stride=72), :].astype(BF16))
            if f == 31:
                a_cross(block).start()
        return done

    lax.fori_loop(0, FOUR, sixteen, 0)
    a_mate.start()
    for k in range(FOUR):
        late_cross(k).start()
        b_mate(k).start()

    a_half[:, rows64(me), :] = ab[0:O32, :, lanes_of(me)]
    b_full[:, rows64(me), :] = ab[O32:C64, :, :]
    mask_mate.wait_recv()
    mask_relay.wait_recv()
    keep_all = m_full[...]
    inv_s[...] = 1.0 / (dot(jnp.transpose(keep_all.astype(F32)).astype(BF16), keep_all) + 1e-3)
    z_load.wait()
    e_bias = b_ref[...].astype(F32)

    for n in range(FOUR):
        a_cross(n).wait_recv()
    a_relay.start()
    a_mate.wait_recv()
    a_relay.wait_recv()
    offset = pl.multiple_of(lax.rem(me, TWO) * C64, C64)

    def turn(c, carry):
        turn_s[...] = jnp.transpose(a_half[c].astype(F32))
        mine = turn_s[pl.ds(offset, C64), :]
        for lane in range(TWO):
            a_tmp[lane, pl.ds(pl.multiple_of(c * 72, H8), C64), :] = mine[:, lane * L128:(lane + 1) * L128]
        return carry

    lax.fori_loop(0, O32, turn, 0)
    for i in range(C64):
        for lane in range(TWO):
            a_s[i * O32:(i + 1) * O32, lane * L128:(lane + 1) * L128] = a_tmp[lane, pl.ds(i, O32, stride=72), :].astype(BF16)

    late_cross(0).wait_recv()
    b_relay(0).start()
    slots = ((p_hi0, p_lo0), (p_hi1, p_lo1))

    def outer(slot, index, d):
        p_hi, p_lo = slots[slot]
        k, n = index // H8, lax.rem(index, H8)
        value = dot(a_s[pl.ds(pl.multiple_of(n * R256, R256), R256), :], b_full[k * H8 + d])
        high = value.astype(BF16)
        low = (value - high.astype(F32)).astype(BF16)
        for i in range(H8):
            p_hi[i, d * O32:(d + 1) * O32, :] = high[i * O32:(i + 1) * O32]
            p_lo[i, d * O32:(d + 1) * O32, :] = low[i * O32:(i + 1) * O32]

    def project(slot, index, i):
        p_hi, p_lo = slots[slot]
        index = jnp.maximum(index, 0)
        k, at = index // H8, lax.rem(index, H8) * H8 + i
        part = dot(w_t[k], p_hi[i]) + dot(w_t[k], p_lo[i])
        acc[at] = jnp.where(k == 0, part, acc[at] + part)

    def settle(index, i):
        at = jnp.maximum(index - 24, 0) * H8 + i
        update = acc[at] * inv_s[pl.ds(me * C64 + at, 1), :]
        out_ref[at] = (z_buf[at].astype(F32) + jnp.transpose(update) + e_bias).astype(BF16)

    def pair(last, t, carry):
        k = t // TWO

        @pl.when(lax.rem(t, TWO) == 0)
        def _():
            b_mate(k).wait_recv()
            b_relay(k).wait_recv()

        if not last:
            @pl.when(lax.rem(t, TWO) == 1)
            def _():
                late_cross(k + 1).wait_recv()
                b_relay(k + 1).start()

        for step in range(FOUR):
            index, slot = FOUR * t + step, step % TWO
            for n in range(H8):
                outer(slot, index, n)
                project(1 - slot, index - 1, n)
                if last:
                    settle(index - TWO, n)
        return carry

    lax.fori_loop(0, 6, functools.partial(pair, False), 0)
    lax.fori_loop(6, H8, functools.partial(pair, True), 0)
    for n in range(H8):
        project(1, 31, n)
        settle(30, n)
    for n in range(H8):
        settle(31, n)
    for copy in (stat_mate, stat_cross, mask_cross, mask_mate, mask_relay, a_mate, a_relay):
        copy.wait_send()
    for n in range(FOUR):
        a_cross(n).wait_send()
        late_cross(n).wait_send()
        b_mate(n).wait_send()
        b_relay(n).wait_send()


def tail_stage(qs, kv, mask, e1, g1, pair, bcg, wco, wti, wto, wom, weight, bias):
    any_spec = pl.BlockSpec(memory_space=pl.ANY)
    vmem = pl.BlockSpec(memory_space=pltpu.VMEM)
    return pl.pallas_call(
        tail_kernel,
        name='tail_stage',
        out_shape=(jax.ShapeDtypeStruct((C64, C64, R256), BF16), jax.ShapeDtypeStruct((C64, R256, L128), BF16)),
        in_specs=[vmem] * 5 + [any_spec] + [vmem] * 7,
        out_specs=(vmem, vmem),
        scratch_shapes=[
            pltpu.VMEM((FOUR, 80, R256), F32),
            pltpu.VMEM((80, R256), F32),
            pltpu.VMEM((C64, H8, R256), F32),
            pltpu.VMEM((C64, R256, L128), BF16),
            pltpu.VMEM((C64, C64), BF16),
            pltpu.VMEM((R256, C64), BF16),
            pltpu.VMEM((C64, R256), BF16),
            pltpu.VMEM((C64, C64), BF16),
            pltpu.VMEM((TWO, 1152, L128), F32),
            pltpu.VMEM((C64, C64, R256), BF16),
            pltpu.VMEM((O32, R256, L128), BF16),
            pltpu.VMEM((O32, R256, R256), BF16),
            pltpu.VMEM((R256, R256), BF16),
            pltpu.VMEM((L128, R256), F32),
            pltpu.VMEM((TWO, 2304, L128), F32),
            pltpu.VMEM((W2K, R256), BF16),
            pltpu.VMEM((C64, L128, R256), F32),
        ] + [pltpu.VMEM((H8, R256, R256), BF16)] * FOUR + [
            pltpu.VMEM((1280, L128), F32),
            pltpu.VMEM((FOUR, L128, R256), BF16),
            pltpu.VMEM((R256, R256), F32),
            pltpu.SemaphoreType.DMA(()),
            pltpu.SemaphoreType.DMA((7,)),
            pltpu.SemaphoreType.DMA((7,)),
            pltpu.SemaphoreType.DMA((18,)),
            pltpu.SemaphoreType.DMA((18,)),
        ],
        compiler_params=pltpu.CompilerParams(collective_id=1, has_side_effects=True, vmem_limit_bytes=TAIL_LIMIT),
    )(qs, kv, mask, e1, g1, pair, bcg, wco, wti, wto, wom, weight, bias)


def solution(mesh):
    row_spec = P(('batch', 'seq'))
    rep_spec = P()

    def local_block(msa, mask, pair, w_pair_bias, w_row_in, b_row_gate, w_row_out, w_col_in, b_col_gate, w_col_out, w_trans_in, w_trans_out, w_opm_in, w_opm_out, b_opm_out):
        pinned = [pltpu.with_memory_space_constraint(value, pltpu.HBM) for value in (
            jnp.swapaxes(msa, 1, TWO), pair, mask, w_pair_bias.T, w_row_in, b_row_gate.reshape(1, C64), w_row_out, w_col_in)]
        e1, g1, kv, qs = row_stage(*pinned)
        e3, pair_out = tail_stage(qs, kv, mask, e1, g1, pair, b_col_gate.reshape(1, C64), w_col_out, w_trans_in, w_trans_out.T, w_opm_in, w_opm_out.reshape(1024, L128), b_opm_out.reshape(1, L128))
        return jnp.swapaxes(e3, 1, TWO), pair_out

    return jax.shard_map(local_block, mesh=mesh, in_specs=(row_spec, row_spec, row_spec) + (rep_spec,) * 12, out_specs=(row_spec, row_spec), check_vma=False)
```
